32 devices in a mesh: dp: 2 (over x), tp: 16 (over y, z, core).
Axes of the slice: x: 2, y: 2, z: 4, core: 2. Of those that a mesh axis runs over, the one named last changes fastest.
Arguments:
- x: bfloat16 [13312, 2560], P(('dp', 'tp')), parts along dimension 0
- dy: bfloat16 [13312, 2560], P(('dp', 'tp')), parts along dimension 0
- gate: bfloat16 [13312, 10240], P('dp', 'tp'), parts along dimension 0
- up: bfloat16 [13312, 10240], P('dp', 'tp'), parts along dimension 0
- w_gate: bfloat16 [2560, 10240], P(None, 'tp')
- w_up: bfloat16 [2560, 10240], P(None, 'tp')
- w_down: bfloat16 [10240, 2560], P('tp')
Outputs:
- output 1: bfloat16 [13312, 2560], P(('dp', 'tp')), parts along dimension 0
- output 2: bfloat16 [5120, 10240], P('dp', 'tp'), parts along dimension 0
- output 3: bfloat16 [5120, 10240], P('dp', 'tp'), parts along dimension 0
- output 4: bfloat16 [20480, 2560], P(('dp', 'tp')), parts along dimension 0
There are 2 independent parts. The reference program is written for one: setup_inputs(seed, part) draws one part's arguments, and reference() takes and returns one part's arrays. A program takes and returns all parts, laid end to end along the dimension named above; an argument that names none is the same for every part.
All inputs are finite; a program needn't handle non-finite values.
Results may differ from the reference program's by a relative error of at most 0.012.
Values are sent between devices in bfloat16 or wider.
A program may use at most 2 GiB of HBM per device.

```python
import jax
import jax.numpy as jnp

ROWS = 6656
D = 2560
FF = 10240


def act(gate, up):
    return jax.nn.gelu(gate) * up


def setup_inputs(seed: int = 0, part: int = 0) -> dict:
    kx, ky, ka, kb, kg, ku, kd = jax.random.split(jax.random.key(seed), 7)
    kx, ky, ka, kb = (jax.random.fold_in(k, part) for k in (kx, ky, ka, kb))
    drawn = {
        "x": jax.random.normal(kx, (ROWS, D), jnp.float32),
        "dy": jax.random.normal(ky, (ROWS, D), jnp.float32),
        "gate": jax.random.normal(ka, (ROWS, FF), jnp.float32),
        "up": jax.random.normal(kb, (ROWS, FF), jnp.float32),
        "w_gate": jax.random.normal(kg, (D, FF), jnp.float32) * D**-0.5,
        "w_up": jax.random.normal(ku, (D, FF), jnp.float32) * D**-0.5,
        "w_down": jax.random.normal(kd, (FF, D), jnp.float32) * FF**-0.5,
    }
    return {k: v.astype(jnp.bfloat16) for k, v in drawn.items()}


def reference(x, dy, gate, up, w_gate, w_up, w_down):
    hidden, back = jax.vjp(act, gate.astype(jnp.float32), up.astype(jnp.float32))
    d_hidden = jnp.dot(dy, w_down.T, preferred_element_type=jnp.float32)
    d_gate, d_up = (g.astype(jnp.bfloat16) for g in back(d_hidden))
    dx = jnp.dot(d_gate, w_gate.T, preferred_element_type=jnp.float32) + jnp.dot(d_up, w_up.T, preferred_element_type=jnp.float32)
    dw_gate = jnp.dot(x.T, d_gate, preferred_element_type=jnp.float32)
    dw_up = jnp.dot(x.T, d_up, preferred_element_type=jnp.float32)
    dw_down = jnp.dot(hidden.astype(jnp.bfloat16).T, dy, preferred_element_type=jnp.float32)
    return tuple(g.astype(jnp.bfloat16) for g in (dx, dw_gate, dw_up, dw_down))
```

```python
import jax
import jax.numpy as jnp
from jax import lax
from jax.experimental import pallas as pl
from jax.experimental.pallas import tpu as pltpu
from jax.sharding import PartitionSpec as P

MESH = pl.DeviceIdType.MESH
F32, BF16 = jnp.float32, jnp.bfloat16

H = 2
SLOTS = 10
P_, D_, Y_, W_ = 0, 1, 2, 3
DY, X = 0, 1
ROLES = ("M", "C")

SENDS = {
    "M": {
        P_: {0: (DY, "00M"), 1: (DY, "01M"), 2: (DY, "01C"), 3: (X, "00M"), 4: (X, "01M"), 5: (X, "01C")},
        D_: {0: (DY, "00M"), 1: (DY, "00C"), 2: (DY, "10M"), 3: (X, "00M"), 4: (X, "00C"), 5: (X, "10M")},
        Y_: {0: (DY, "00M"), 1: (DY, "00C"), 2: (DY, "01C"), 3: (X, "00M"), 4: (X, "00C"), 6: (X, "01C")},
    },
    "C": {
        P_: {0: (DY, "00C"), 1: (X, "00C")},
        Y_: {0: (DY, "00C"), 1: (DY, "00M"), 2: (DY, "01M"), 3: (DY, "01C"),
             4: (X, "00C"), 5: (X, "00M"), 6: (X, "01M"), 7: (X, "01C")},
    },
}
RECEIVES = {
    "M": {
        0: [(DY, "00C"), (DY, "10M"), (DY, "01M")], 1: [(X, "00C"), (DY, "10C"), (DY, "01C")], 2: [(DY, "11C"), (DY, "11M")],
        3: [(X, "10M"), (X, "01M")], 4: [(X, "10C"), (X, "01C")], 5: [(X, "11M")], 6: [(X, "11C")],
    },
    "C": {
        0: [(DY, "00M"), (DY, "10C")], 1: [(DY, "01M"), (DY, "10M")], 2: [(DY, "01C"), (DY, "11M")],
        3: [(DY, "11C"), (X, "00M")], 4: [(X, "10C"), (X, "01M")], 5: [(X, "10M"), (X, "01C")], 6: [(X, "11M")], 7: [(X, "11C")],
    },
}
SUMS = {
    "M": {
        5: [("11M", (P_,), Y_, 0)],
        6: [("11C", (P_,), D_, 0)],
        7: [("01C", (P_,), D_, 1), ("10C", (P_, D_), Y_, 1)],
        8: [("01M", (P_, Y_), D_, 1), ("10M", (P_,), Y_, 1), ("00C", (D_, Y_), P_, 0)],
        9: [("00M", (P_, D_, Y_), None, 0)],
    },
    "C": {
        2: [("10C", (), P_, 0)], 3: [("10M", (), P_, 1)], 4: [("11M", (), P_, 1)], 5: [("11C", (), P_, 1)],
        6: [("01C", (), P_, 1)], 7: [("01M", (), P_, 1)], 8: [("00M", (), P_, 1)], 9: [("00C", (P_,), None, 0)],
    },
}
TOKENS = {
    "M": {
        DY: [["00M"], ["00C", "10M", "01M"], ["10C", "01C"], ["11M", "11C"]],
        X: [["00M", "00C"], ["10M", "01M"], ["01C", "10C"], ["11M", "11C"]],
    },
    "C": {
        DY: [["00C"], ["00M", "10C"], ["01M", "10M"], ["01C", "11M"], ["11C"]],
        X: [["00C", "00M"], ["10C", "01M"], ["01C", "10M"], ["11M", "11C"]],
    },
}
X_FROM = {"M": 9, "C": 11}


def pack(unit):
    return int(unit[0]) + 2 * int(unit[1]) + 4 * (unit[2] == "M")


def select(key, table):
    out = jnp.int32(0)
    for k, v in table.items():
        out = jnp.where(key == k, jnp.int32(v), out)
    return out


def token_tables():
    count, what = {}, {}
    for r, role in enumerate(ROLES):
        for array in (DY, X):
            for g, units in enumerate(TOKENS[role][array]):
                for h in range(H):
                    if array == DY:
                        s = h if g == 0 else (g - 1) * H + h + H + 1
                    else:
                        s = X_FROM[role] + g * H + h
                    count[r * 100 + s] = len(units)
                    for k, unit in enumerate(units):
                        what[(r * 100 + s) * 10 + k] = pack(unit) + 8 * h + 16 * array
    return count, what


def sum_tables():
    count, what = {}, {}
    for r, role in enumerate(ROLES):
        for slot, entries in SUMS[role].items():
            count[r * 100 + slot] = len(entries)
            for k, (unit, links, out, before) in enumerate(entries):
                mask = sum(1 << link for link in links)
                code = pack(unit) + 8 * mask + 64 * (3 if out is None else out) + 256 * before
                what[(r * 100 + slot) * 10 + k] = code
    return count, what


def kernel(
    x, dy, gate, up, w_gate, w_up, w_down,
    dx, dw_gate, dw_up, dw_down, full, parts,
    wg, wu, wd, acc, dg, du, tok, gb, ub, dh, hid, total, ext, out, outw,
    ag_recv, ag_send, rs_recv, rs_send, w_send, w_sem, tok_sem, g_sem, u_sem, e_sem, st_sem,
):
    block, depth = dy.shape
    width = gate.shape[1]
    rows = block // H
    tile = 512
    own_in = {DY: dy, X: x}

    tp = lax.axis_index("tp")
    core, chip = tp % 2, tp // 2
    y, z = chip // 4, chip % 4
    half = z // 2
    middle = ((z + 1) % 4) // 2
    is_m, is_c = middle == 1, middle == 0
    role = 1 - middle

    def chip_of(yy, hh, mm):
        return yy * 4 + mm + hh * (3 - 2 * mm)

    def chip_at(unit):
        yy = 1 - y if unit[0] == "1" else y
        hh = 1 - half if unit[1] == "1" else half
        return chip_of(yy, hh, 1 if unit[2] == "M" else 0)

    def chip_packed(code):
        ry, rh, mm = code % 2, (code // 2) % 2, (code // 4) % 2
        return chip_of(y + ry - 2 * y * ry, half + rh - 2 * half * rh, mm)

    partner = tp + 1 - 2 * core
    at_link = {
        P_: chip_of(y, half, 1 - middle) * 2 + core,
        D_: chip_of(y, 1 - half, middle) * 2 + core,
        Y_: chip_of(1 - y, half, middle) * 2 + core,
        W_: partner,
    }

    def piece(h):
        return pl.ds(pl.multiple_of(h * rows, rows), rows)

    def remote(src, dst, send, recv, to):
        return pltpu.make_async_remote_copy(
            src_ref=src, dst_ref=dst, send_sem=send, recv_sem=recv, device_id={"tp": to}, device_id_type=MESH
        )


    def gather(link, array, unit, own, h):
        c = chip_at(unit)
        to = full.at[array, c * 2 + core, piece(h)]
        return remote(
            own_in[array].at[piece(h)] if own else to, to, ag_send.at[link, array, c, h], ag_recv.at[array, c * 2 + core, h],
            at_link[link],
        )

    def arrived(array, unit, h):
        c = chip_at(unit)
        to = full.at[array, c * 2 + core, piece(h)]
        remote(to, to, ag_send.at[W_, array, c, h], ag_recv.at[array, c * 2 + core, h], partner).wait_recv()

    def communicate(slot, name, h):
        for array, unit in RECEIVES[name].get(slot - 1, []):
            arrived(array, unit, h)
        for link in (P_, D_, Y_):
            entry = SENDS[name].get(link, {}).get(slot)
            if entry:
                gather(link, *entry, entry[1] == "00" + name, h).start()
        if slot in (0, 1):
            gather(W_, slot, "00" + name, True, h).start()
        for array, unit in RECEIVES[name].get(slot - 1, []):
            gather(W_, array, unit, False, h).start()


    sum_count, sum_what = sum_tables()

    def dx_term(index, plane):
        span = pl.ds(pl.multiple_of(plane * rows, rows), rows)

        def column(n, _):
            cols = pl.ds(pl.multiple_of(n * tile, tile), tile)
            total[:, cols] = lax.dot_general(
                dg[index, span, :], wg[cols, :], (((1,), (1,)), ((), ())), preferred_element_type=F32
            ) + lax.dot_general(du[index, span, :], wu[cols, :], (((1,), (1,)), ((), ())), preferred_element_type=F32)
            return 0

        lax.fori_loop(0, depth // tile, column, 0)

    def by_rows(step, n_rows, fn):
        def body(i, _):
            fn(pl.ds(pl.multiple_of(i * step, step), step))
            return 0

        lax.fori_loop(0, n_rows // step, body, 0)

    def term_in(kind, c, h):
        return pltpu.make_async_copy(parts.at[kind, c, piece(h)], ext.at[kind], e_sem.at[kind])

    def send_term(link, c, h, to):
        return remote(out.at[link, h], parts.at[link, c, piece(h)], rs_send.at[link, h], rs_recv.at[link, c, h], to)

    def reduce_one(code, h):
        c = chip_packed(code)
        mask, link, before = (code // 8) % 8, (code // 64) % 4, code // 256
        bits = [mask % 2 == 1, (mask // 2) % 2 == 1, mask // 4 == 1]
        for kind in (P_, D_, Y_, W_):

            def fetch(kind=kind):
                remote(ext.at[kind], parts.at[kind, c, piece(h)], w_send.at[0], rs_recv.at[kind, c, h], partner).wait_recv()
                term_in(kind, c, h).start()

            fetch() if kind == W_ else pl.when(bits[kind])(fetch)
        dx_term(c * H + h, core)
        for kind in (P_, D_, Y_):

            @pl.when(bits[kind])
            def _(kind=kind):
                term_in(kind, c, h).wait()

                def add(r):
                    total[r, :] += ext[kind, r, :].astype(F32)

                by_rows(16, rows, add)

        term_in(W_, c, h).wait()

        @pl.when(link == 3)
        def _():
            def finish(r):
                ext[P_, r, :] = (total[r, :] + ext[W_, r, :].astype(F32)).astype(BF16)

            by_rows(16, rows, finish)
            done = pltpu.make_async_copy(ext.at[P_], dx.at[piece(h)], e_sem.at[P_])
            done.start()
            done.wait()

        @pl.when(link != 3)
        def _():
            to = jnp.where(link == P_, at_link[P_], jnp.where(link == D_, at_link[D_], at_link[Y_]))

            @pl.when(before == 1)
            def _():
                send_term(link, c, h, to).wait_send()

            def round_(r):
                out[link, h, r, :] = (total[r, :] + ext[W_, r, :].astype(F32)).astype(BF16)

            by_rows(16, rows, round_)
            send_term(link, c, h, to).start()

    def term_to_partner(code, h, b):
        c = chip_packed(code)
        return remote(outw.at[b], parts.at[W_, c, piece(h)], w_send.at[b], rs_recv.at[W_, c, h], partner)

    def partner_one(key, k, h):
        code = select(key * 10 + k, sum_what)
        b = k % 2
        dx_term(chip_packed(code) * H + h, 1 - core)

        @pl.when(k >= 2)
        def _():
            term_to_partner(code, h, b).wait_send()

        def round_(r):
            outw[b, r, :] = total[r, :].astype(BF16)

        by_rows(16, rows, round_)
        term_to_partner(code, h, b).start()


    tok_count, tok_what = token_tables()
    nj, ni = depth // 128, width // 128

    def tok_in(code, b, start):
        c, h, array = chip_packed(code), (code // 8) % 2, code // 16
        mine = c == chip
        for plane in range(2):
            blk = c * 2 + plane
            dst = tok.at[b, plane * rows : (plane + 1) * rows]
            src = full.at[array, blk, piece(h)]
            sem = tok_sem.at[b, plane]
            spread = pl.ds(pl.multiple_of(blk * block + h * rows, rows), rows)
            g_in = pltpu.make_async_copy(gate.at[spread], gb.at[b, plane * rows : (plane + 1) * rows], g_sem.at[b, plane])
            u_in = pltpu.make_async_copy(up.at[spread], ub.at[b, plane * rows : (plane + 1) * rows], u_sem.at[b, plane])
            if not start:
                pltpu.make_async_copy(src, dst, sem).wait()

                @pl.when(array == DY)
                def _(g_in=g_in, u_in=u_in):
                    g_in.wait()
                    u_in.wait()

                continue

            @pl.when(array == DY)
            def _(g_in=g_in, u_in=u_in):
                g_in.start()
                u_in.start()

            local = mine & (core == plane)

            @pl.when(core != plane)
            def _(src=src, sem=sem, blk=blk):
                remote(src, src, w_send.at[0], ag_recv.at[array, blk, h], partner).wait_recv()

            @pl.when(jnp.logical_not(local))
            def _(src=src, dst=dst, sem=sem):
                pltpu.make_async_copy(src, dst, sem).start()

            for a in (DY, X):

                @pl.when(local & (array == a))
                def _(a=a, dst=dst, sem=sem):
                    pltpu.make_async_copy(own_in[a].at[piece(h)], dst, sem).start()

    def zero(i):
        def body(k, _):
            acc[i, k] = jnp.zeros((128, 128), F32)
            return 0

        lax.fori_loop(0, ni * nj, body, 0)

    def work_dy(code, b):
        index = chip_packed(code) * H + (code // 8) % 2
        dh[...] = lax.dot_general(tok[b], wd[...], (((1,), (1,)), ((), ())), preferred_element_type=F32)

        def pointwise(r):
            g, u, d = gb[b, r, :].astype(F32), ub[b, r, :].astype(F32), dh[r, :]
            g2 = g * g
            t = jnp.tanh(g * (0.7978845608028654 + (0.7978845608028654 * 0.044715) * g2))
            cdf = 0.5 + 0.5 * t
            act = g * cdf
            slope = cdf + (0.5 * g) * (1.0 - t * t) * (0.7978845608028654 + (3 * 0.7978845608028654 * 0.044715) * g2)
            du[index, r, :] = (d * act).astype(BF16)
            dg[index, r, :] = ((d * u) * slope).astype(BF16)
            hid[r, :] = (act * u).astype(BF16)

        by_rows(16, 2 * rows, pointwise)

        def column(n, _):
            cols = pl.ds(pl.multiple_of(n * tile, tile), tile)
            new = lax.dot_general(hid[...], tok[b, :, cols], (((0,), (0,)), ((), ())), preferred_element_type=F32)
            for i in range(ni):
                for j in range(tile // 128):
                    k = i * nj + n * (tile // 128) + j
                    acc[0, k] += new[i * 128 : (i + 1) * 128, j * 128 : (j + 1) * 128]
            return 0

        lax.fori_loop(0, depth // tile, column, 0)

    def work_x(code, b):
        index = chip_packed(code) * H + (code // 8) % 2

        def column(n, _):
            cols = pl.ds(pl.multiple_of(n * tile, tile), tile)
            xt = tok[b, :, cols]
            for a, d in enumerate((dg, du)):
                new = lax.dot_general(xt, d[index], (((0,), (0,)), ((), ())), preferred_element_type=F32)
                for i in range(tile // 128):
                    for j in range(ni):
                        k = (n * (tile // 128) + i) * ni + j
                        acc[a, k] += new[i * 128 : (i + 1) * 128, j * 128 : (j + 1) * 128]
            return 0

        lax.fori_loop(0, depth // tile, column, 0)

    def finish_down():
        for i in range(ni):
            b = i % 2
            put = pltpu.make_async_copy(tok.at[b, 0:128], dw_down.at[pl.ds(i * 128, 128)], st_sem.at[0, b])
            if i >= 2:
                put.wait()
            for j in range(nj):
                tok[b, 0:128, j * 128 : (j + 1) * 128] = acc[0, i * nj + j].astype(BF16)
            put.start()
        for i in range(max(ni - 2, 0), ni):
            pltpu.make_async_copy(tok.at[i % 2, 0:128], dw_down.at[pl.ds(i * 128, 128)], st_sem.at[0, i % 2]).wait()

    def finish_gate_up():
        def put(a, i, b):
            to = (dw_gate, dw_up)[a].at[pl.ds(pl.multiple_of(i * 128, 128), 128)]
            return pltpu.make_async_copy((gb, ub)[a].at[b, 0:128], to, st_sem.at[a, b])

        def body(i, _):
            b = i % 2
            for a in range(2):

                @pl.when(i >= 2)
                def _(a=a):
                    put(a, i, b).wait()

                for j in range(ni):
                    (gb, ub)[a][b, 0:128, j * 128 : (j + 1) * 128] = acc[a, i * ni + j].astype(BF16)
                put(a, i, b).start()
            return 0

        lax.fori_loop(0, nj, body, 0)
        for a in range(2):
            for b in range(2):
                put(a, 0, b).wait()


    loads = [pltpu.make_async_copy(s, d, w_sem.at[i]) for i, (s, d) in enumerate(((w_down, wd), (w_gate, wg), (w_up, wu)))]
    for load in loads:
        load.start()

    barrier = pltpu.get_barrier_semaphore()
    for link in (P_, Y_, W_):
        pl.semaphore_signal(barrier, inc=1, device_id={"tp": at_link[link]}, device_id_type=MESH)

    @pl.when(is_m)
    def _():
        pl.semaphore_signal(barrier, inc=1, device_id={"tp": at_link[D_]}, device_id_type=MESH)
        pl.semaphore_wait(barrier, 4)

    @pl.when(is_c)
    def _():
        pl.semaphore_wait(barrier, 3)

    zero(0)
    x_from = jnp.where(is_m, X_FROM["M"], X_FROM["C"])

    def step(s, _):
        slot, h = s // H, s % H
        for name, here in (("M", is_m), ("C", is_c)):
            for t in range(SLOTS):
                if t - 1 in RECEIVES[name] or any(t in v for v in SENDS[name].values()):

                    @pl.when(here & (slot == t))
                    def _(t=t, name=name):
                        communicate(t, name, h)

        @pl.when(s == x_from)
        def _():
            finish_down()
            zero(0)
            zero(1)

        key = role * 100 + s
        n_tok = select(key, tok_count)

        @pl.when(n_tok > 0)
        def _():
            tok_in(select(key * 10, tok_what), 0, True)

        @pl.when(s == 0)
        def _():
            for load in loads:
                load.wait()

        sum_key = role * 100 + slot

        def sums(k, _):
            reduce_one(select(sum_key * 10 + k, sum_what), h)
            return 0

        lax.fori_loop(0, select(sum_key, sum_count), sums, 0)

        def tokens(k, _):
            code, b = select(key * 10 + k, tok_what), k % 2

            @pl.when(k + 1 < n_tok)
            def _():
                tok_in(select(key * 10 + k + 1, tok_what), 1 - b, True)

            tok_in(code, b, False)

            @pl.when(code // 16 == DY)
            def _():
                work_dy(code, b)

            @pl.when(code // 16 == X)
            def _():
                work_x(code, b)

            return 0

        lax.fori_loop(0, n_tok, tokens, 0)

        next_key = role * 100 + (s + 1) // H
        next_h = (s + 1) % H
        n_next = select(next_key, sum_count)

        def partners(k, _):
            partner_one(next_key, k, next_h)
            return 0

        lax.fori_loop(0, n_next, partners, 0)
        for b in range(2):

            @pl.when(n_next > b)
            def _(b=b):
                term_to_partner(0, 0, b).wait_send()

        @pl.when(s == H * 9)
        def _():
            finish_gate_up()

        return 0

    lax.fori_loop(0, SLOTS * H, step, 0)

    for name, here in (("M", is_m), ("C", is_c)):

        @pl.when(here)
        def _(name=name):
            def drain(h, _):
                for link, entries in SENDS[name].items():
                    for array, unit in entries.values():
                        gather(link, array, unit, False, h).wait_send()
                for array in (DY, X):
                    gather(W_, array, "00" + name, False, h).wait_send()
                for entries in RECEIVES[name].values():
                    for array, unit in entries:
                        gather(W_, array, unit, False, h).wait_send()
                for link in {out_ for entries in SUMS[name].values() for _, _, out_, _ in entries if out_ is not None}:
                    send_term(link, chip, h, partner).wait_send()
                return 0

            lax.fori_loop(0, H, drain, 0)


def solution(mesh):
    def step(x, dy, gate, up, w_gate, w_up, w_down):
        block, depth = dy.shape
        tokens, width = gate.shape
        rows = block // H
        blocks = tokens // block
        anywhere = pl.BlockSpec(memory_space=pl.ANY)
        dma, flops = pltpu.SemaphoreType.DMA, 12 * tokens * depth * width
        outs = pl.pallas_call(
            kernel,
            out_shape=[
                jax.ShapeDtypeStruct((block, depth), BF16),
                jax.ShapeDtypeStruct((depth, width), BF16),
                jax.ShapeDtypeStruct((depth, width), BF16),
                jax.ShapeDtypeStruct((width, depth), BF16),
                jax.ShapeDtypeStruct((2, blocks, block, depth), BF16),
                jax.ShapeDtypeStruct((4, blocks // 2, block, depth), BF16),
            ],
            in_specs=[anywhere] * 7,
            out_specs=[anywhere] * 6,
            scratch_shapes=[
                pltpu.VMEM((depth, width), BF16),
                pltpu.VMEM((depth, width), BF16),
                pltpu.VMEM((width, depth), BF16),
                pltpu.VMEM((2, (depth // 128) * (width // 128), 128, 128), F32),
                pltpu.VMEM((blocks // 2 * H, 2 * rows, width), BF16),
                pltpu.VMEM((blocks // 2 * H, 2 * rows, width), BF16),
                pltpu.VMEM((2, 2 * rows, depth), BF16),
                pltpu.VMEM((2, 2 * rows, width), BF16),
                pltpu.VMEM((2, 2 * rows, width), BF16),
                pltpu.VMEM((2 * rows, width), F32),
                pltpu.VMEM((2 * rows, width), BF16),
                pltpu.VMEM((rows, depth), F32),
                pltpu.VMEM((4, rows, depth), BF16),
                pltpu.VMEM((3, H, rows, depth), BF16),
                pltpu.VMEM((2, rows, depth), BF16),
                dma((2, blocks, H)),
                dma((4, 2, blocks // 2, H)),
                dma((4, blocks // 2, H)),
                dma((3, H)),
                dma((2,)),
                dma((3,)),
                dma((2, 2)),
                dma((2, 2)),
                dma((2, 2)),
                dma((4,)),
                dma((2, 2)),
            ],
            compiler_params=pltpu.CompilerParams(collective_id=0, has_side_effects=True, vmem_limit_bytes=67043328),
            cost_estimate=pl.CostEstimate(flops=flops, bytes_accessed=12 * tokens * depth, transcendentals=tokens * width),
            name="mlp_backward",
        )(x, dy, gate, up, w_gate, w_up, w_down)
        return tuple(outs[:4])

    rows_, cols_ = P(("dp", "tp"), None), P("dp", "tp")
    return jax.shard_map(
        step,
        mesh=mesh,
        in_specs=(rows_, rows_, cols_, cols_, P(None, "tp"), P(None, "tp"), P("tp", None)),
        out_specs=(rows_, cols_, cols_, rows_),
        check_vma=False,
    )
```

```python
import jax
import jax.numpy as jnp
from jax import lax
from jax.experimental import pallas as pl
from jax.experimental.pallas import tpu as pltpu
from jax.sharding import PartitionSpec as P

MESH = pl.DeviceIdType.MESH
F32, BF16 = jnp.float32, jnp.bfloat16

P_, D_, Y_, W_ = 0, 1, 2, 3
DY, X = 0, 1
ROLES = "MC"
LINKS = {"a": ("C", "C", Y_), "b": ("M", "C", P_), "c": ("C", "M", P_), "d": ("M", "M", D_), "e": ("M", "M", Y_)}

START = {
    "a": {
        0: "d00C0", 2: "d00C1", 4: "d00M1", 6: "d01C1", 8: "d00M0", 10: "d01C0", 12: "d01M0", 14: "d01M1",
        16: "s10M0", 18: "x00M1", 20: "x00M0", 22: "x01C0", 24: "x01M0", 26: "x01C1", 28: "x00C1", 30: "s10M1",
        32: "x00C0",
    },
    "b": {
        0: "d00M1", 2: "d01M1", 4: "d01C1", 6: "d00M0", 8: "d01C0", 10: "d01M0", 12: "s10M0", 14: "x00M1",
        16: "x01M1", 18: "x00M0", 20: "x01C0", 22: "x01M0", 24: "x01C1", 26: "s10M1", 28: "x11M1", 30: "s00C0",
        32: "s00C1",
    },
    "c": {
        0: "d00C1", 2: "d00C0", 4: "x00C0", 6: "s10C0", 8: "s10C1", 10: "s01C1", 12: "s11C1", 14: "x00C1",
        16: "s01M0", 18: "s11C0", 20: "s11M0", 22: "s01C0", 24: "s00M0", 26: "s11M1", 28: "s01M1", 30: "x10C1",
        33: "s00M1",
    },
    "d": {
        0: "d00M1", 2: "d00C1", 4: "d10M0", 6: "d00C0", 8: "d00M0", 10: "x00M1", 12: "d10M1", 14: "s01C1",
        16: "s11C1", 18: "x00C0", 20: "x00M0", 22: "x00C1", 24: "x10M1", 26: "s01C0", 28: "s01M0", 30: "x10M0",
        33: "s01M1",
    },
    "e": {
        0: "d00M1", 2: "d00M0", 4: "d00C0", 6: "d00C1", 8: "d01C0", 10: "d01C1", 12: "s10C0", 14: "x00M1",
        16: "x00M0", 18: "x00C0", 20: "x01C0", 22: "s11C0", 24: "s11M0", 26: "x01C1", 28: "s10C1", 30: "s11M1",
    },
}
TOKENS = {
    "M": {
        0: ["d00M0"], 1: ["d00M1"], 4: ["d10M1", "d00C1"], 5: ["d01M1"],
        6: ["d10M0", "d01C1"], 7: ["d00C0"], 8: ["d10C0", "d11M0"], 10: ["d01C0", "d10C1"],
        12: ["d11C0", "d01M0"], 14: ["d11C1"], 16: ["d11M1"], 17: ["x00M1", "x00M0"],
        18: ["x00C0", "x01M1"], 19: ["x10M1", "x00C1"], 20: ["x10M0"], 22: ["x01C0", "x10C0"],
        24: ["x01M0", "x11C0"], 26: ["x01C1"], 28: ["x11M1"], 30: ["x11C1"],
        34: ["x10C1", "x11M0"],
    },
    "C": {
        0: ["d00C0"], 1: ["d00C1"], 4: ["d10C0", "d00M1"], 6: ["d10C1", "d01M1"],
        8: ["d01C1", "d10M1"], 10: ["d11C1", "d00M0"], 12: ["d10M0", "d01C0"], 14: ["d01M0", "d11C0"],
        16: ["d11M0"], 18: ["d11M1"], 19: ["x00C0", "x00C1"], 20: ["x00M1", "x01M1"],
        22: ["x10M1", "x00M0"], 24: ["x01C0", "x10M0"], 26: ["x01M0", "x11C0"], 28: ["x11M0", "x01C1"],
        30: ["x11C1"], 32: ["x11M1", "x10C1"], 36: ["x10C0"],
    },
}
X_FROM = {"M": 17, "C": 19}
LAST = {"M": (31, 36), "C": (33, 35)}
STEPS = 37
RING = 8


def seen_by_receiver(unit, link):
    flip = {"0": "1", "1": "0"}
    if link == Y_:
        return flip[unit[0]] + unit[1:]
    return unit[0] + flip[unit[1]] + unit[2] if link == D_ else unit


def pack(unit):
    return int(unit[0]) + 2 * int(unit[1]) + 4 * (unit[2] == "M")


def select(key, table):
    out = jnp.int32(0)
    for k, v in table.items():
        out = jnp.where(key == k, jnp.int32(v), out)
    return out


def plan():
    send, recv = ({P_: {}, D_: {}, Y_: {}} for _ in range(2))
    sums, terms = {"M": {}, "C": {}}, {}
    for name, entries in START.items():
        sender, receiver, link = LINKS[name]
        for n, (t, what) in enumerate(sorted(entries.items())):
            kind, unit, h = what[0], what[1:4], int(what[4])
            there = seen_by_receiver(unit, link)
            if kind == "s":
                count = sum(w[0] == "s" for s, w in entries.items() if s < t)
                sums[sender].setdefault(t, []).append((unit, h, link, count % 2, count >= 2))
                terms.setdefault((receiver, there, h), []).append(link)
                continue
            for k in range(2):
                code = 1 + "dx".index(kind) + 16 * (2 * h + k)
                send[link][ROLES.index(sender) * 100 + t + k] = code + 2 * pack(unit)
                recv[link][ROLES.index(receiver) * 100 + t + k + 2] = code + 2 * pack(there)
    for role in ROLES:
        for h in range(2):
            sums[role].setdefault(LAST[role][h], []).append(("00" + role, h, 3, 0, 0))
    sum_count, sum_what, tok_count, tok_what = {}, {}, {}, {}
    for r, role in enumerate(ROLES):
        for t, entries in sums[role].items():
            sum_count[r * 100 + t] = len(entries)
            for k, (unit, h, link, parity, before) in enumerate(entries):
                mask = sum(1 << i for i in terms.get((role, unit, h), []))
                sum_what[(r * 100 + t) * 10 + k] = pack(unit) + 8 * h + 16 * mask + 128 * link + 512 * parity + 1024 * before
        last = max(TOKENS[role])
        for t, entries in TOKENS[role].items():
            tok_count[r * 100 + t] = len(entries)
            for k, what in enumerate(entries):
                code = pack(what[1:4]) + 8 * int(what[4]) + 16 * "dx".index(what[0])
                tok_what[(r * 100 + t) * 10 + k] = code + 32 * (t == last and k == len(entries) - 1)
    return send, recv, sum_count, sum_what, tok_count, tok_what


def kernel(
    x, dy, gate, up, w_gate, w_up, w_down,
    dx, dw_gate, dw_up, dw_down, full, parts,
    wg, wu, wd, acc, dg, du, tok, gb, ub, dh, hid, total, ext, out, outw,
    ag_recv, ag_send, w_recv, w_send, rs_recv, rs_send, p_send, l_sem, tok_sem, g_sem, u_sem, e_sem, st_sem,
):
    block, depth = dy.shape
    width = gate.shape[1]
    rows, quarter = block // 2, block // 4
    tile = 512
    nj, ni = depth // 128, width // 128
    own_in = {DY: dy, X: x}
    send_what, recv_what, sum_count, sum_what, tok_count, tok_what = plan()

    tp = lax.axis_index("tp")
    core, chip = tp % 2, tp // 2
    y, z = chip // 4, chip % 4
    half = z // 2
    middle = ((z + 1) % 4) // 2
    is_m, is_c = middle == 1, middle == 0
    role = 1 - middle

    def chip_of(yy, hh, mm):
        return yy * 4 + mm + hh * (3 - 2 * mm)

    def chip_packed(code):
        ry, rh, mm = code % 2, (code // 2) % 2, (code // 4) % 2
        return chip_of(y + ry - 2 * y * ry, half + rh - 2 * half * rh, mm)

    partner = tp + 1 - 2 * core
    at_link = {
        P_: chip_of(y, half, 1 - middle) * 2 + core,
        D_: chip_of(y, 1 - half, middle) * 2 + core,
        Y_: chip_of(1 - y, half, middle) * 2 + core,
    }

    def span(h):
        return pl.ds(pl.multiple_of(h * rows, rows), rows)

    def remote(src, dst, send, recv, to):
        return pltpu.make_async_remote_copy(
            src_ref=src, dst_ref=dst, send_sem=send, recv_sem=recv, device_id={"tp": to}, device_id_type=MESH
        )

    def by_rows(step, n_rows, fn):
        def body(i, _):
            fn(pl.ds(pl.multiple_of(i * step, step), step))
            return 0

        lax.fori_loop(0, n_rows // step, body, 0)


    def on_link(link, code, s, src=None):
        code = code - 1
        array, c, p = code % 2, chip_packed(code // 2), code // 16
        piece = pl.ds(pl.multiple_of(p * quarter, quarter), quarter)
        to = full.at[array, c * 2 + core, piece]
        return remote(to if src is None else src.at[piece], to, ag_send.at[link, s % RING], ag_recv.at[array, c, p], at_link[link])

    def to_partner(array, c, h, src=None):
        to = full.at[array, c * 2 + core, span(h)]
        return remote(to if src is None else src.at[span(h)], to, w_send.at[array, c, h], w_recv.at[array, c, h], partner)

    def settle(s):
        for link in (P_, D_, Y_):

            @pl.when(select(role * 100 + s, send_what[link]) > 0)
            def _(link=link):
                on_link(link, jnp.int32(1), s).wait_send()

    def communicate(s):
        key = role * 100 + s
        come = {link: select(key, recv_what[link]) for link in (P_, D_, Y_)}
        for link, code in come.items():

            @pl.when(code > 0)
            def _(link=link, code=code):
                on_link(link, code, s).wait_recv()

        settle(s - RING)
        for link in (P_, D_, Y_):
            code = select(key, send_what[link])
            mine = chip_packed((code - 1) // 2) == chip

            @pl.when((code > 0) & jnp.logical_not(mine))
            def _(link=link, code=code):
                on_link(link, code, s).start()

            for array in (DY, X):

                @pl.when((code > 0) & mine & ((code - 1) % 2 == array))
                def _(link=link, code=code, array=array):
                    on_link(link, code, s, own_in[array]).start()

        for link, code in come.items():

            @pl.when((code > 0) & (((code - 1) // 16) % 2 == 1))
            def _(code=code):
                to_partner((code - 1) % 2, chip_packed((code - 1) // 2), (code - 1) // 32).start()

        for array, when in ((DY, 0), (X, 2)):

            @pl.when(s == when)
            def _(array=array):
                for h in range(2):
                    to_partner(array, chip, h, own_in[array]).start()


    def dx_term(code, plane):
        index = chip_packed(code) * 2 + (code // 8) % 2
        here = span(plane)

        def column(n, _):
            cols = pl.ds(pl.multiple_of(n * tile, tile), tile)
            total[:, cols] = lax.dot_general(
                dg[index, here, :], wg[cols, :], (((1,), (1,)), ((), ())), preferred_element_type=F32
            ) + lax.dot_general(du[index, here, :], wu[cols, :], (((1,), (1,)), ((), ())), preferred_element_type=F32)
            return 0

        lax.fori_loop(0, depth // tile, column, 0)

    def reduce_one(code):
        c, h = chip_packed(code), (code // 8) % 2
        mask, link, parity, before = (code // 16) % 8, (code // 128) % 4, (code // 512) % 2, code // 1024
        bits = {P_: mask % 2 == 1, D_: (mask // 2) % 2 == 1, Y_: mask // 4 == 1}

        def term_in(kind):
            return pltpu.make_async_copy(parts.at[kind, c, span(h)], ext.at[kind], e_sem.at[kind])

        def fetch(kind):
            remote(ext.at[kind], parts.at[kind, c, span(h)], p_send.at[0], rs_recv.at[kind, c, h], partner).wait_recv()
            term_in(kind).start()

        def send_term(to):
            return remote(out.at[link, parity], parts.at[link, c, span(h)], rs_send.at[link, parity], rs_recv.at[link, c, h], to)

        fetch(W_)
        for kind in (P_, D_, Y_):

            @pl.when(bits[kind] & (link != 3))
            def _(kind=kind):
                fetch(kind)

        dx_term(code, core)
        for kind in (P_, D_, Y_):

            @pl.when(bits[kind] & (link == 3))
            def _(kind=kind):
                fetch(kind)

        for kind in (P_, D_, Y_):

            @pl.when(bits[kind])
            def _(kind=kind):
                term_in(kind).wait()

                def add(r):
                    total[r, :] += ext[kind, r, :].astype(F32)

                by_rows(16, rows, add)

        term_in(W_).wait()

        @pl.when(link == 3)
        def _():
            def finish(r):
                ext[P_, r, :] = (total[r, :] + ext[W_, r, :].astype(F32)).astype(BF16)

            by_rows(16, rows, finish)
            done = pltpu.make_async_copy(ext.at[P_], dx.at[span(h)], e_sem.at[P_])
            done.start()
            done.wait()

        @pl.when(link != 3)
        def _():
            to = jnp.where(link == P_, at_link[P_], jnp.where(link == D_, at_link[D_], at_link[Y_]))

            @pl.when(before == 1)
            def _():
                send_term(to).wait_send()

            def round_(r):
                out[link, parity, r, :] = (total[r, :] + ext[W_, r, :].astype(F32)).astype(BF16)

            by_rows(16, rows, round_)
            send_term(to).start()

    def term_to_partner(code, b):
        c, h = chip_packed(code), (code // 8) % 2
        return remote(outw.at[b], parts.at[W_, c, span(h)], p_send.at[b], rs_recv.at[W_, c, h], partner)

    def partner_one(code, k):
        b = k % 2
        dx_term(code, 1 - core)

        @pl.when(k >= 2)
        def _():
            term_to_partner(code, b).wait_send()

        def round_(r):
            outw[b, r, :] = total[r, :].astype(BF16)

        by_rows(16, rows, round_)
        term_to_partner(code, b).start()


    def tok_in(code, b, start):
        c, h, array = chip_packed(code), (code // 8) % 2, (code // 16) % 2
        mine = c == chip
        for plane in range(2):
            blk = c * 2 + plane
            here = slice(plane * rows, (plane + 1) * rows)
            dst, src, sem = tok.at[b, here], full.at[array, blk, span(h)], tok_sem.at[b, plane]
            spread = pl.ds(pl.multiple_of(blk * block + h * rows, rows), rows)
            pair = (
                pltpu.make_async_copy(gate.at[spread], gb.at[b, here], g_sem.at[b, plane]),
                pltpu.make_async_copy(up.at[spread], ub.at[b, here], u_sem.at[b, plane]),
            )
            if not start:
                pltpu.make_async_copy(src, dst, sem).wait()

                @pl.when(array == DY)
                def _(pair=pair):
                    for copy in pair:
                        copy.wait()

                continue

            @pl.when(array == DY)
            def _(pair=pair):
                for copy in pair:
                    copy.start()

            local = mine & (core == plane)

            @pl.when(core != plane)
            def _(src=src):
                remote(src, src, p_send.at[0], w_recv.at[array, c, h], partner).wait_recv()

            @pl.when(jnp.logical_not(local))
            def _(src=src, dst=dst, sem=sem):
                pltpu.make_async_copy(src, dst, sem).start()

            for a in (DY, X):

                @pl.when(local & (array == a))
                def _(a=a, dst=dst, sem=sem):
                    pltpu.make_async_copy(own_in[a].at[span(h)], dst, sem).start()

    def work_dy(code, b):
        index = chip_packed(code) * 2 + (code // 8) % 2
        dh[...] = lax.dot_general(tok[b], wd[...], (((1,), (1,)), ((), ())), preferred_element_type=F32)

        def pointwise(r):
            g, u, d = gb[b, r, :].astype(F32), ub[b, r, :].astype(F32), dh[r, :]
            g2 = g * g
            t = jnp.tanh(g * (0.7978845608028654 + (0.7978845608028654 * 0.044715) * g2))
            cdf = 0.5 + 0.5 * t
            act = g * cdf
            slope = cdf + (0.5 * g) * (1.0 - t * t) * (0.7978845608028654 + (3 * 0.7978845608028654 * 0.044715) * g2)
            du[index, r, :] = (d * act).astype(BF16)
            dg[index, r, :] = ((d * u) * slope).astype(BF16)
            hid[r, :] = (act * u).astype(BF16)

        by_rows(16, 2 * rows, pointwise)

        def column(n, _):
            cols = pl.ds(pl.multiple_of(n * tile, tile), tile)
            new = lax.dot_general(hid[...], tok[b, :, cols], (((0,), (0,)), ((), ())), preferred_element_type=F32)
            for i in range(ni):
                for j in range(tile // 128):
                    k = i * nj + n * (tile // 128) + j
                    acc[0, k] += new[i * 128 : (i + 1) * 128, j * 128 : (j + 1) * 128]
            return 0

        lax.fori_loop(0, depth // tile, column, 0)

    places = 2 * (2 * rows // 128)

    def put(a, i):
        b = i % places
        here = (b // (places // 2), pl.ds(pl.multiple_of((b % (places // 2)) * 128, 128), 128))
        to = (dw_gate, dw_up)[a].at[pl.ds(pl.multiple_of(i * 128, 128), 128)]
        return here, pltpu.make_async_copy((gb, ub)[a].at[here], to, st_sem.at[a, b])

    def work_x(code, b):
        index = chip_packed(code) * 2 + (code // 8) % 2
        last = code // 32 == 1

        def column(n, _):
            cols = pl.ds(pl.multiple_of(n * tile, tile), tile)
            xt = tok[b, :, cols]
            for a, d in enumerate((dg, du)):
                new = lax.dot_general(xt, d[index], (((0,), (0,)), ((), ())), preferred_element_type=F32)
                for i in range(tile // 128):
                    for j in range(ni):
                        k = (n * (tile // 128) + i) * ni + j
                        acc[a, k] += new[i * 128 : (i + 1) * 128, j * 128 : (j + 1) * 128]

            @pl.when(last)
            def _():
                for i in range(tile // 128):
                    for a in range(2):
                        k = n * (tile // 128) + i
                        here, copy = put(a, k)

                        @pl.when(k >= places)
                        def _(copy=copy):
                            copy.wait()

                        for j in range(ni):
                            (gb, ub)[a][(*here, slice(j * 128, (j + 1) * 128))] = acc[a, k * ni + j].astype(BF16)
                        copy.start()

            return 0

        lax.fori_loop(0, depth // tile, column, 0)

        @pl.when(last)
        def _():
            for a in range(2):
                for i in range(max(nj - places, 0), nj):
                    put(a, i)[1].wait()

    def finish_down():
        copies = []
        for i in range(ni):
            at = (i * 128) // (2 * rows // 128 * 128)
            here = pl.ds(i * 128 - at * (2 * rows // 128 * 128), 128)
            copy = pltpu.make_async_copy(tok.at[at % 2, here], dw_down.at[pl.ds(i * 128, 128)], st_sem.at[0, at % 2 * (places // 2) + i % (places // 2)])
            if at >= 2:
                copies[i - places].wait()
            for j in range(nj):
                tok[at % 2, here, j * 128 : (j + 1) * 128] = acc[0, i * nj + j].astype(BF16)
                acc[0, i * nj + j] = jnp.zeros((128, 128), F32)
            copy.start()
            copies.append(copy)
        for copy in copies[max(ni - places, 0) :]:
            copy.wait()

    def clear(i):
        def body(k, _):
            acc[i, k] = jnp.zeros((128, 128), F32)
            return 0

        lax.fori_loop(0, ni * nj, body, 0)


    loads = [pltpu.make_async_copy(s, d, l_sem.at[i]) for i, (s, d) in enumerate(((w_down, wd), (w_gate, wg), (w_up, wu)))]
    for load in loads:
        load.start()

    barrier = pltpu.get_barrier_semaphore()
    for to in (at_link[P_], at_link[Y_], partner):
        pl.semaphore_signal(barrier, inc=1, device_id={"tp": to}, device_id_type=MESH)

    @pl.when(is_m)
    def _():
        pl.semaphore_signal(barrier, inc=1, device_id={"tp": at_link[D_]}, device_id_type=MESH)
        pl.semaphore_wait(barrier, 4)

    @pl.when(is_c)
    def _():
        pl.semaphore_wait(barrier, 3)

    x_from = jnp.where(is_m, X_FROM["M"], X_FROM["C"])

    def step(s, _):
        communicate(s)

        @pl.when(s == x_from)
        def _():
            finish_down()

        key = role * 100 + s
        n_tok = select(key, tok_count)

        @pl.when(n_tok > 0)
        def _():
            tok_in(select(key * 10, tok_what), 0, True)

        @pl.when(s == 0)
        def _():
            clear(0)
            clear(1)
            for load in loads:
                load.wait()

        def sums(k, _):
            reduce_one(select(key * 10 + k, sum_what))
            return 0

        lax.fori_loop(0, select(key, sum_count), sums, 0)

        def tokens(k, _):
            code, b = select(key * 10 + k, tok_what), k % 2

            @pl.when(k + 1 < n_tok)
            def _():
                tok_in(select(key * 10 + k + 1, tok_what), 1 - b, True)

            tok_in(code, b, False)

            @pl.when((code // 16) % 2 == DY)
            def _():
                work_dy(code, b)

            @pl.when((code // 16) % 2 == X)
            def _():
                work_x(code, b)

            return 0

        lax.fori_loop(0, n_tok, tokens, 0)

        n_next = select(key + 1, sum_count)

        def partners(k, _):
            partner_one(select((key + 1) * 10 + k, sum_what), k)
            return 0

        lax.fori_loop(0, n_next, partners, 0)
        for b in range(2):

            @pl.when(n_next > b)
            def _(b=b):
                term_to_partner(0, b).wait_send()

        return 0

    lax.fori_loop(0, STEPS, step, 0)

    def rest(s, _):
        settle(s)
        return 0

    lax.fori_loop(STEPS - RING, STEPS, rest, 0)
    for link in (P_, D_, Y_):

        @pl.when(is_m | (link != D_))
        def _(link=link):
            for parity in range(2):
                half_block = parts.at[link, 0, span(0)]
                remote(out.at[link, parity], half_block, rs_send.at[link, parity], rs_recv.at[link, 0, 0], partner).wait_send()

    def left(i, _):
        to_partner(i // 16, (i // 2) % 8, i % 2).wait_send()
        return 0

    lax.fori_loop(0, 32, left, 0)


def solution(mesh):
    def step(x, dy, gate, up, w_gate, w_up, w_down):
        block, depth = dy.shape
        tokens, width = gate.shape
        rows, chips = block // 2, tokens // block // 2
        places = 2 * (2 * rows // 128)
        anywhere = pl.BlockSpec(memory_space=pl.ANY)
        dma, flops = pltpu.SemaphoreType.DMA, 12 * tokens * depth * width
        outs = pl.pallas_call(
            kernel,
            out_shape=[
                jax.ShapeDtypeStruct((block, depth), BF16),
                jax.ShapeDtypeStruct((depth, width), BF16),
                jax.ShapeDtypeStruct((depth, width), BF16),
                jax.ShapeDtypeStruct((width, depth), BF16),
                jax.ShapeDtypeStruct((2, 2 * chips, block, depth), BF16),
                jax.ShapeDtypeStruct((4, chips, block, depth), BF16),
            ],
            in_specs=[anywhere] * 7,
            out_specs=[anywhere] * 6,
            scratch_shapes=[
                pltpu.VMEM((depth, width), BF16),
                pltpu.VMEM((depth, width), BF16),
                pltpu.VMEM((width, depth), BF16),
                pltpu.VMEM((2, (depth // 128) * (width // 128), 128, 128), F32),
                pltpu.VMEM((2 * chips, 2 * rows, width), BF16),
                pltpu.VMEM((2 * chips, 2 * rows, width), BF16),
                pltpu.VMEM((2, 2 * rows, depth), BF16),
                pltpu.VMEM((2, 2 * rows, width), BF16),
                pltpu.VMEM((2, 2 * rows, width), BF16),
                pltpu.VMEM((2 * rows, width), F32),
                pltpu.VMEM((2 * rows, width), BF16),
                pltpu.VMEM((rows, depth), F32),
                pltpu.VMEM((4, rows, depth), BF16),
                pltpu.VMEM((3, 2, rows, depth), BF16),
                pltpu.VMEM((2, rows, depth), BF16),
                dma((2, chips, 4)),
                dma((3, RING)),
                dma((2, chips, 2)),
                dma((2, chips, 2)),
                dma((4, chips, 2)),
                dma((3, 2)),
                dma((2,)),
                dma((3,)),
                dma((2, 2)),
                dma((2, 2)),
                dma((2, 2)),
                dma((4,)),
                dma((2, places)),
            ],
            compiler_params=pltpu.CompilerParams(collective_id=0, has_side_effects=True, vmem_limit_bytes=67043328),
            cost_estimate=pl.CostEstimate(flops=flops, bytes_accessed=12 * tokens * depth, transcendentals=tokens * width),
            name="mlp_backward",
        )(x, dy, gate, up, w_gate, w_up, w_down)
        return tuple(outs[:4])

    rows_, cols_ = P(("dp", "tp"), None), P("dp", "tp")
    return jax.shard_map(
        step,
        mesh=mesh,
        in_specs=(rows_, rows_, cols_, cols_, P(None, "tp"), P(None, "tp"), P("tp", None)),
        out_specs=(rows_, cols_, cols_, rows_),
        check_vma=False,
    )
```

```python
import jax
import jax.numpy as jnp
from jax import lax
from jax.experimental import pallas as pl
from jax.experimental.pallas import tpu as pltpu
from jax.sharding import PartitionSpec as P

MESH = pl.DeviceIdType.MESH
F32, BF16 = jnp.float32, jnp.bfloat16

P_, D_, Y_, W_ = 0, 1, 2, 3
DY, X = 0, 1
ROLES = "MC"
LINKS = {"a": ("C", "C", Y_), "b": ("M", "C", P_), "c": ("C", "M", P_), "d": ("M", "M", D_), "e": ("M", "M", Y_)}

START = {
    "a": [
        "d00C1", "d00M1", "d01M0", "d01C0", "d00C0", "d01C1", "d01M1", "d00M0", "x01C1", "x00C1", "x01M0", "x01M1",
        "x01C0", "s10M0", "s10M1", "x00C0", "x00M1",
    ],
    "b": [
        "d00M1", "d01M0", "d01C0", "s10M0", "d01C1", "d01M1", "d00M0", "x01C1", "s10M1", "x01M0", "x01M1", "x01C0",
        "x00M1", "x10M0", "x00M0", "s00C0", "s00C1",
    ],
    "c": [
        "d00C0", "d00C1", "x00C1", "s10C1", "x00C0", "s01C0", "s11M0", "s10C0", "s11C1", "s11C0", "x10C1", "s01C1",
        "s11M1", "s01M0", "s01M1", "s00M0", "s00M1",
    ],
    "d": [
        "d00M0", "d00C0", "d00C1", "d10M0", "d00M1", "d10M1", "x00C1", "s01C0", "x00M0", "x00M1", "x00C0", "s11C0",
        "x10M1", "x10M0", "s01C1", "s01M0", "s01M1",
    ],
    "e": [
        "d00M0", "d00M1", "d00C1", "d01C1", "d01C0", "s10C1", "d00C0", "x00M1", "s11M0", "x00C0", "s11C1", "x01C0",
        "x00M0", "s10C0", "s11M1", "x01C1",
    ],
}
TOKENS = {
    "M": [
        "0d00M0", "1d00M1", "4d10M0", "4d01M0", "5d00C0", "6d01C0", "6d10M1", "7d00C1", "8d10C1", "8d01C1", "10d11M0", "10d11C1",
        "12d11C0", "12d01M1", "14d11M1", "16d10C0", "17x00M0", "17x00M1", "18x00C1", "18x00C0", "19x01C1", "19x10M1", "20x01M0", "22x10C0",
        "22x01M1", "24x10C1", "24x01C0", "26x11C0", "28x10M0", "28x11M1", "30x11M0", "35x11C1",
    ],
    "C": [
        "0d00C0", "1d00C1", "4d10C1", "4d00M1", "6d01M0", "6d10M1", "8d01C0", "8d11M0", "10d11C0", "12d10C0", "12d01C1", "14d11C1",
        "14d01M1", "16d11M1", "16d00M0", "18d10M0", "19x00C0", "19x00C1", "20x01C1", "20x11C1", "22x10C1", "22x01M0", "24x11M0", "24x01M1",
        "26x11M1", "26x01C0", "28x11C0", "28x00M1", "30x10M0", "32x00M0", "34x10C0", "36x10M1",
    ],
}
X_FROM = {"M": 17, "C": 19}
LAST = {"M": (33, 35), "C": (33, 35)}
WAITS_LAST = {"M": True, "C": False}
STEPS = 37
RING = 8


def seen_by_receiver(unit, link):
    flip = {"0": "1", "1": "0"}
    if link == Y_:
        return flip[unit[0]] + unit[1:]
    return unit[0] + flip[unit[1]] + unit[2] if link == D_ else unit


def pack(unit):
    return int(unit[0]) + 2 * int(unit[1]) + 4 * (unit[2] == "M")


def select(key, table):
    out = jnp.int32(0)
    for k, v in table.items():
        out = jnp.where(key == k, jnp.int32(v), out)
    return out


def plan():
    send, recv = ({P_: {}, D_: {}, Y_: {}} for _ in range(2))
    sums, terms = {"M": {}, "C": {}}, {}
    for name, entries in START.items():
        sender, receiver, link = LINKS[name]
        t = count = 0
        for what in entries:
            if what[0] == "+":
                t += int(what)
                continue
            kind, unit, h = what[0], what[1:4], int(what[4])
            there = seen_by_receiver(unit, link)
            if kind == "s":
                sums[sender].setdefault(t, []).append((unit, h, link, count % 2, count >= 2, 0))
                terms.setdefault((receiver, there, h), []).append(link)
                count += 1
            for k in range(0 if kind == "s" else 2):
                code = 1 + "dx".index(kind) + 16 * (2 * h + k)
                send[link][ROLES.index(sender) * 100 + t + k] = code + 2 * pack(unit)
                recv[link][ROLES.index(receiver) * 100 + t + k + 2] = code + 2 * pack(there)
            t += 2
    for role in ROLES:
        for h in range(2):
            early = LAST[role][h] == max(LAST[role])
            sums[role].setdefault(LAST[role][h], []).insert(0, ("00" + role, h, 3, 0, 0, early))
    sum_count, sum_what, tok_count, tok_what = {}, {}, {}, {}
    for r, role in enumerate(ROLES):
        for t, entries in sums[role].items():
            sum_count[r * 100 + t] = len(entries)
            for k, (unit, h, link, parity, before, early) in enumerate(entries):
                code = pack(unit) + 8 * h + 16 * sum(1 << i for i in terms.get((role, unit, h), []))
                sum_what[(r * 100 + t) * 10 + k] = code + 128 * link + 512 * parity + 1024 * before + 2048 * early
        for what in TOKENS[role]:
            t, kind, unit, h = int(what[:-5]), what[-5], what[-4:-1], int(what[-1])
            k = tok_count.get(r * 100 + t, 0)
            tok_count[r * 100 + t] = k + 1
            code = pack(unit) + 8 * h + 16 * "dx".index(kind)
            tok_what[(r * 100 + t) * 10 + k] = code + 32 * (what is TOKENS[role][-1])
    return send, recv, sum_count, sum_what, tok_count, tok_what


def kernel(
    x, dy, gate, up, w_gate, w_up, w_down,
    dx, wg, wu, wd, full, parts,
    acc, dg, du, tok, gb, ub, dh, hid, total, ext, out, outw,
    ag_recv, ag_send, w_recv, w_send, rs_recv, rs_send, p_send, l_sem, tok_sem, g_sem, u_sem, e_sem,
):
    block, depth = dy.shape
    width = gate.shape[1]
    rows, quarter = block // 2, block // 4
    tile = 512
    nj, ni = depth // 128, width // 128
    own_in = {DY: dy, X: x}
    send_what, recv_what, sum_count, sum_what, tok_count, tok_what = plan()

    tp = lax.axis_index("tp")
    core, chip = tp % 2, tp // 2
    y, z = chip // 4, chip % 4
    half = z // 2
    middle = ((z + 1) % 4) // 2
    is_m, is_c = middle == 1, middle == 0
    role = 1 - middle

    def chip_of(yy, hh, mm):
        return yy * 4 + mm + hh * (3 - 2 * mm)

    def chip_packed(code):
        ry, rh, mm = code % 2, (code // 2) % 2, (code // 4) % 2
        return chip_of(y + ry - 2 * y * ry, half + rh - 2 * half * rh, mm)

    partner = tp + 1 - 2 * core
    at_link = {
        P_: chip_of(y, half, 1 - middle) * 2 + core,
        D_: chip_of(y, 1 - half, middle) * 2 + core,
        Y_: chip_of(1 - y, half, middle) * 2 + core,
    }

    def span(h):
        return pl.ds(pl.multiple_of(h * rows, rows), rows)

    def remote(src, dst, send, recv, to):
        return pltpu.make_async_remote_copy(
            src_ref=src, dst_ref=dst, send_sem=send, recv_sem=recv, device_id={"tp": to}, device_id_type=MESH
        )

    def by_rows(step, n_rows, fn):
        def body(i, _):
            fn(pl.ds(pl.multiple_of(i * step, step), step))
            return 0

        lax.fori_loop(0, n_rows // step, body, 0)


    def on_link(link, code, s, src=None):
        code = code - 1
        array, c, p = code % 2, chip_packed(code // 2), code // 16
        piece = pl.ds(pl.multiple_of(p * quarter, quarter), quarter)
        to = full.at[array, c * 2 + core, piece]
        return remote(to if src is None else src.at[piece], to, ag_send.at[link, s % RING], ag_recv.at[array, c, p], at_link[link])

    def to_partner(array, c, h, src=None):
        to = full.at[array, c * 2 + core, span(h)]
        return remote(to if src is None else src.at[span(h)], to, w_send.at[array, c, h], w_recv.at[array, c, h], partner)

    def settle(s):
        for link in (P_, D_, Y_):

            @pl.when(select(role * 100 + s, send_what[link]) > 0)
            def _(link=link):
                on_link(link, jnp.int32(1), s).wait_send()

    def communicate(s):
        key = role * 100 + s
        come = {link: select(key, recv_what[link]) for link in (P_, D_, Y_)}
        for link, code in come.items():

            @pl.when(code > 0)
            def _(link=link, code=code):
                on_link(link, code, s).wait_recv()

        settle(s - RING)
        for link in (P_, D_, Y_):
            code = select(key, send_what[link])
            mine = chip_packed((code - 1) // 2) == chip

            @pl.when((code > 0) & jnp.logical_not(mine))
            def _(link=link, code=code):
                on_link(link, code, s).start()

            for array in (DY, X):

                @pl.when((code > 0) & mine & ((code - 1) % 2 == array))
                def _(link=link, code=code, array=array):
                    on_link(link, code, s, own_in[array]).start()

        for link, code in come.items():

            @pl.when((code > 0) & (((code - 1) // 16) % 2 == 1))
            def _(code=code):
                to_partner((code - 1) % 2, chip_packed((code - 1) // 2), (code - 1) // 32).start()

        for array, when in ((DY, 0), (X, 2)):

            @pl.when(s == when)
            def _(array=array):
                for h in range(2):
                    to_partner(array, chip, h, own_in[array]).start()


    def dx_term(code, plane):
        index = chip_packed(code) * 2 + (code // 8) % 2
        here = span(plane)

        def column(n, _):
            cols = pl.ds(pl.multiple_of(n * tile, tile), tile)
            total[:, cols] = lax.dot_general(
                dg[index, here, :], wg[cols, :], (((1,), (1,)), ((), ())), preferred_element_type=F32
            ) + lax.dot_general(du[index, here, :], wu[cols, :], (((1,), (1,)), ((), ())), preferred_element_type=F32)
            return 0

        lax.fori_loop(0, depth // tile, column, 0)

    def reduce_one(code):
        c, h = chip_packed(code), (code // 8) % 2
        mask, link, parity, before = (code // 16) % 8, (code // 128) % 4, (code // 512) % 2, (code // 1024) % 2
        bits = {P_: mask % 2 == 1, D_: (mask // 2) % 2 == 1, Y_: mask // 4 == 1}

        def term_in(kind):
            return pltpu.make_async_copy(parts.at[kind, c, span(h)], ext.at[kind], e_sem.at[kind])

        def fetch(kind):
            remote(ext.at[kind], parts.at[kind, c, span(h)], p_send.at[0], rs_recv.at[kind, c, h], partner).wait_recv()
            term_in(kind).start()

        def send_term(to):
            return remote(out.at[link, parity], parts.at[link, c, span(h)], rs_send.at[link, parity], rs_recv.at[link, c, h], to)

        fetch(W_)
        for kind in (P_, D_, Y_):

            @pl.when(bits[kind] & (link != 3))
            def _(kind=kind):
                fetch(kind)

        @pl.when(code < 2048)
        def _():
            dx_term(code, core)

        for kind in (P_, D_, Y_):

            @pl.when(bits[kind] & (link == 3))
            def _(kind=kind):
                fetch(kind)

        for kind in (P_, D_, Y_):

            @pl.when(bits[kind])
            def _(kind=kind):
                term_in(kind).wait()

                def add(r):
                    total[r, :] += ext[kind, r, :].astype(F32)

                by_rows(16, rows, add)

        term_in(W_).wait()

        @pl.when(link == 3)
        def _():
            def finish(r):
                to = pl.ds(pl.multiple_of(h * rows + r.start, 16), 16)
                dx[to, :] = (total[r, :] + ext[W_, r, :].astype(F32)).astype(BF16)

            by_rows(16, rows, finish)

        @pl.when(link != 3)
        def _():
            to = jnp.where(link == P_, at_link[P_], jnp.where(link == D_, at_link[D_], at_link[Y_]))

            @pl.when(before == 1)
            def _():
                send_term(to).wait_send()

            def round_(r):
                out[link, parity, r, :] = (total[r, :] + ext[W_, r, :].astype(F32)).astype(BF16)

            by_rows(16, rows, round_)
            send_term(to).start()

    def term_to_partner(code, b):
        c, h = chip_packed(code), (code // 8) % 2
        return remote(outw.at[b], parts.at[W_, c, span(h)], p_send.at[b], rs_recv.at[W_, c, h], partner)

    def partner_one(code, k):
        b = k % 2
        dx_term(code, 1 - core)

        @pl.when(k >= 2)
        def _():
            term_to_partner(code, b).wait_send()

        def round_(r):
            outw[b, r, :] = total[r, :].astype(BF16)

        by_rows(16, rows, round_)
        term_to_partner(code, b).start()


    def last_in(code, b, plane):
        c, h = chip_packed(code), (code // 8) % 2
        src = full.at[X, c * 2 + plane, span(h)]
        return pltpu.make_async_copy(src, tok.at[b, span(plane)], tok_sem.at[b, plane])

    def tok_in(code, b, start):
        @pl.when(code < 32)
        def _():
            pair_in(code, b, start)

        @pl.when(code >= 32)
        def _():
            copy = last_in(code, b, core)
            copy.start() if start else copy.wait()

    def pair_in(code, b, start):
        c, h, array = chip_packed(code), (code // 8) % 2, (code // 16) % 2
        mine = c == chip
        for plane in range(2):
            blk = c * 2 + plane
            here = slice(plane * rows, (plane + 1) * rows)
            dst, src, sem = tok.at[b, here], full.at[array, blk, span(h)], tok_sem.at[b, plane]
            spread = pl.ds(pl.multiple_of(blk * block + h * rows, rows), rows)
            pair = (
                pltpu.make_async_copy(gate.at[spread], gb.at[b, here], g_sem.at[b, plane]),
                pltpu.make_async_copy(up.at[spread], ub.at[b, here], u_sem.at[b, plane]),
            )
            if not start:
                pltpu.make_async_copy(src, dst, sem).wait()

                @pl.when(array == DY)
                def _(pair=pair):
                    for copy in pair:
                        copy.wait()

                continue

            @pl.when(array == DY)
            def _(pair=pair):
                for copy in pair:
                    copy.start()

            local = mine & (core == plane)

            @pl.when(core != plane)
            def _(src=src):
                remote(src, src, p_send.at[0], w_recv.at[array, c, h], partner).wait_recv()

            @pl.when(jnp.logical_not(local))
            def _(src=src, dst=dst, sem=sem):
                pltpu.make_async_copy(src, dst, sem).start()

            for a in (DY, X):

                @pl.when(local & (array == a))
                def _(a=a, dst=dst, sem=sem):
                    pltpu.make_async_copy(own_in[a].at[span(h)], dst, sem).start()

    def work_dy(code, b):
        index = chip_packed(code) * 2 + (code // 8) % 2
        dh[...] = lax.dot_general(tok[b], wd[...], (((1,), (1,)), ((), ())), preferred_element_type=F32)

        def pointwise(r):
            g, u, d = gb[b, r, :].astype(F32), ub[b, r, :].astype(F32), dh[r, :]
            g2 = g * g
            t = jnp.tanh(g * (0.7978845608028654 + (0.7978845608028654 * 0.044715) * g2))
            cdf = 0.5 + 0.5 * t
            act = g * cdf
            slope = cdf + (0.5 * g) * (1.0 - t * t) * (0.7978845608028654 + (3 * 0.7978845608028654 * 0.044715) * g2)
            du[index, r, :] = (d * act).astype(BF16)
            dg[index, r, :] = ((d * u) * slope).astype(BF16)
            hid[r, :] = (act * u).astype(BF16)

        by_rows(16, 2 * rows, pointwise)

        def column(n, _):
            cols = pl.ds(pl.multiple_of(n * tile, tile), tile)
            new = lax.dot_general(hid[...], tok[b, :, cols], (((0,), (0,)), ((), ())), preferred_element_type=F32)
            for i in range(ni):
                for j in range(tile // 128):
                    k = i * nj + n * (tile // 128) + j
                    acc[0, k] += new[i * 128 : (i + 1) * 128, j * 128 : (j + 1) * 128]
            return 0

        lax.fori_loop(0, depth // tile, column, 0)

    def x_columns(index, b, here, results):
        def column(n, _):
            cols = pl.ds(pl.multiple_of(n * tile, tile), tile)
            xt = tok[b, here, cols]
            for a, d in enumerate((dg, du)):
                new = lax.dot_general(xt, d[index, here, :], (((0,), (0,)), ((), ())), preferred_element_type=F32)
                for i in range(tile // 128):
                    for j in range(ni):
                        k = (n * (tile // 128) + i) * ni + j
                        one = acc[a, k] + new[i * 128 : (i + 1) * 128, j * 128 : (j + 1) * 128]
                        if results:
                            to = pl.ds(pl.multiple_of(n * tile + i * 128, 128), 128)
                            (wg, wu)[a][to, j * 128 : (j + 1) * 128] = one.astype(BF16)
                        else:
                            acc[a, k] = one
            return 0

        lax.fori_loop(0, depth // tile, column, 0)

    def work_x(code, b):
        x_columns(chip_packed(code) * 2 + (code // 8) % 2, b, slice(None), False)

    def last_x(code, b):
        c, h = chip_packed(code), (code // 8) % 2
        x_columns(c * 2 + h, b, span(core), False)
        there = full.at[X, c * 2 + 1 - core, span(h)]
        remote(there, there, p_send.at[0], w_recv.at[X, c, h], partner).wait_recv()
        copy = last_in(code, b, 1 - core)
        copy.start()
        copy.wait()
        x_columns(c * 2 + h, b, span(1 - core), True)

    def finish_down():
        for i in range(ni):
            for j in range(nj):
                wd[i * 128 : (i + 1) * 128, j * 128 : (j + 1) * 128] = acc[0, i * nj + j].astype(BF16)
                acc[0, i * nj + j] = jnp.zeros((128, 128), F32)

    def clear(i):
        def body(k, _):
            acc[i, k] = jnp.zeros((128, 128), F32)
            return 0

        lax.fori_loop(0, ni * nj, body, 0)


    loads = [pltpu.make_async_copy(s, d, l_sem.at[i]) for i, (s, d) in enumerate(((w_down, wd), (w_gate, wg), (w_up, wu)))]
    for load in loads:
        load.start()

    barrier = pltpu.get_barrier_semaphore()
    for to in (at_link[P_], at_link[Y_], partner):
        pl.semaphore_signal(barrier, inc=1, device_id={"tp": to}, device_id_type=MESH)

    @pl.when(is_m)
    def _():
        pl.semaphore_signal(barrier, inc=1, device_id={"tp": at_link[D_]}, device_id_type=MESH)
        pl.semaphore_wait(barrier, 4)

    @pl.when(is_c)
    def _():
        pl.semaphore_wait(barrier, 3)

    x_from = jnp.where(is_m, X_FROM["M"], X_FROM["C"])

    last_sum = jnp.where(is_m, max(LAST["M"]), max(LAST["C"]))

    def step(s, _):
        @pl.when(s == last_sum)
        def _():
            dx_term(select((role * 100 + s) * 10, sum_what), core)

        communicate(s)

        @pl.when(s == x_from)
        def _():
            finish_down()

        key = role * 100 + s
        n_tok = select(key, tok_count)

        @pl.when(n_tok > 0)
        def _():
            tok_in(select(key * 10, tok_what), 0, True)

        @pl.when(s == 0)
        def _():
            clear(0)
            clear(1)
            for load in loads:
                load.wait()

        def sums(k, _):
            reduce_one(select(key * 10 + k, sum_what))
            return 0

        def tokens(k, _):
            code, b = select(key * 10 + k, tok_what), k % 2

            @pl.when(k + 1 < n_tok)
            def _():
                tok_in(select(key * 10 + k + 1, tok_what), 1 - b, True)

            tok_in(code, b, False)

            @pl.when((code // 16) % 2 == DY)
            def _():
                work_dy(code, b)

            @pl.when(code // 16 == X)
            def _():
                work_x(code, b)

            @pl.when(code >= 32)
            def _():
                last_x(code, b)

            return 0

        n_sum = select(key, sum_count)
        tokens_first = (s == last_sum) & jnp.where(is_m, WAITS_LAST["M"], WAITS_LAST["C"])

        def phase(p, _):
            now = (p == 0) != tokens_first
            lax.fori_loop(0, jnp.where(now, n_sum, 0), sums, 0)
            lax.fori_loop(0, jnp.where(now, 0, n_tok), tokens, 0)
            return 0

        lax.fori_loop(0, 2, phase, 0)

        n_next = select(key + 1, sum_count)

        def partners(k, _):
            partner_one(select((key + 1) * 10 + k, sum_what), k)
            return 0

        lax.fori_loop(0, n_next, partners, 0)
        for b in range(2):

            @pl.when(n_next > b)
            def _(b=b):
                term_to_partner(0, b).wait_send()

        return 0

    lax.fori_loop(0, STEPS, step, 0)

    def rest(s, _):
        settle(s)
        return 0

    lax.fori_loop(STEPS - RING, STEPS, rest, 0)
    for link in (P_, D_, Y_):

        @pl.when(is_m | (link != D_))
        def _(link=link):
            for parity in range(2):
                half_block = parts.at[link, 0, span(0)]
                remote(out.at[link, parity], half_block, rs_send.at[link, parity], rs_recv.at[link, 0, 0], partner).wait_send()

    def left(i, _):
        to_partner(i // 16, (i // 2) % 8, i % 2).wait_send()
        return 0

    lax.fori_loop(0, 32, left, 0)


def store(*refs):
    results, places, sem = refs[:4], refs[4:8], refs[8]
    copies = []
    for i, (result, place) in enumerate(zip(results, places)):
        n = result.shape[0] // 4
        for k in range(4):
            here = pl.ds(k * n, n)
            copies.append(pltpu.make_async_copy(result.at[here], place.at[here], sem.at[i, k]))
    for copy in copies:
        copy.start()
    for copy in copies:
        copy.wait()


def solution(mesh):
    def step(x, dy, gate, up, w_gate, w_up, w_down):
        block, depth = dy.shape
        tokens, width = gate.shape
        rows, chips = block // 2, tokens // block // 2
        anywhere = pl.BlockSpec(memory_space=pl.ANY)
        dma, flops = pltpu.SemaphoreType.DMA, 12 * tokens * depth * width
        outs = pl.pallas_call(
            kernel,
            out_shape=[
                pltpu.VMEM((block, depth), BF16),
                pltpu.VMEM((depth, width), BF16),
                pltpu.VMEM((depth, width), BF16),
                pltpu.VMEM((width, depth), BF16),
                jax.ShapeDtypeStruct((2, 2 * chips, block, depth), BF16),
                jax.ShapeDtypeStruct((4, chips, block, depth), BF16),
            ],
            in_specs=[anywhere] * 7,
            out_specs=[pl.BlockSpec(memory_space=pltpu.VMEM)] * 4 + [anywhere] * 2,
            scratch_shapes=[
                pltpu.VMEM((2, (depth // 128) * (width // 128), 128, 128), F32),
                pltpu.VMEM((2 * chips, 2 * rows, width), BF16),
                pltpu.VMEM((2 * chips, 2 * rows, width), BF16),
                pltpu.VMEM((2, 2 * rows, depth), BF16),
                pltpu.VMEM((2, 2 * rows, width), BF16),
                pltpu.VMEM((2, 2 * rows, width), BF16),
                pltpu.VMEM((2 * rows, width), F32),
                pltpu.VMEM((2 * rows, width), BF16),
                pltpu.VMEM((rows, depth), F32),
                pltpu.VMEM((4, rows, depth), BF16),
                pltpu.VMEM((3, 2, rows, depth), BF16),
                pltpu.VMEM((2, rows, depth), BF16),
                dma((2, chips, 4)),
                dma((3, RING)),
                dma((2, chips, 2)),
                dma((2, chips, 2)),
                dma((4, chips, 2)),
                dma((3, 2)),
                dma((2,)),
                dma((3,)),
                dma((2, 2)),
                dma((2, 2)),
                dma((2, 2)),
                dma((4,)),
            ],
            compiler_params=pltpu.CompilerParams(collective_id=0, has_side_effects=True, vmem_limit_bytes=55050000),
            cost_estimate=pl.CostEstimate(flops=flops, bytes_accessed=12 * tokens * depth, transcendentals=tokens * width),
            name="mlp_backward",
        )(x, dy, gate, up, w_gate, w_up, w_down)
        results = outs[:4]
        return pl.pallas_call(
            store,
            out_shape=[jax.ShapeDtypeStruct(r.shape, BF16) for r in results],
            in_specs=[pl.BlockSpec(memory_space=pltpu.VMEM)] * 4,
            out_specs=[anywhere] * 4,
            scratch_shapes=[dma((4, 4))],
            compiler_params=pltpu.CompilerParams(vmem_limit_bytes=2**20),
            name="store",
        )(*results)

    rows_, cols_ = P(("dp", "tp"), None), P("dp", "tp")
    return jax.shard_map(
        step,
        mesh=mesh,
        in_specs=(rows_, rows_, cols_, cols_, P(None, "tp"), P(None, "tp"), P("tp", None)),
        out_specs=(rows_, cols_, cols_, rows_),
        check_vma=False,
    )
```

```python
import jax
import jax.numpy as jnp
from jax import lax
from jax.experimental import pallas as pl
from jax.experimental.pallas import tpu as pltpu
from jax.sharding import PartitionSpec as P

MESH = pl.DeviceIdType.MESH
F32, BF16 = jnp.float32, jnp.bfloat16

P_, D_, Y_, W_ = 0, 1, 2, 3
DY, X = 0, 1
ROLES = "MC"
LINKS = {"a": ("C", "C", Y_), "b": ("M", "C", P_), "c": ("C", "M", P_), "d": ("M", "M", D_), "e": ("M", "M", Y_)}

START = {
    "a": [
        "d00C0", "d00C1", "d00M0", "d01C0", "d01M0", "d01M1", "d00M1", "d01C1", "s10M0", "x01M1", "x00C0", "x00C1",
        "x01C1", "x00M1", "s10M1", "x01M0", "x01C0",
    ],
    "b": [
        "d00M0", "d01M0", "d01C0", "s10M0", "d01M1", "d00M1", "d01C1", "s10M1", "x01M1", "x10M0", "x01C0", "x01C1",
        "x00M1", "x00M0", "x01M0", "s00C0", "s00C1",
    ],
    "c": [
        "d00C0", "d00C1", "x00C0", "s10C0", "s10C1", "s01C0", "s11C0", "s01M0", "x00C1", "s01C1", "s11C1", "s11M0",
        "x10C1", "s11M1", "s01M1", "s00M0", "s00M1",
    ],
    "d": [
        "d00M0", "d00C0", "d10M0", "d00M1", "d10M1", "d00C1", "x00M0", "x00M1", "x10M0", "x00C0", "x00C1", "s01C1",
        "s11C1", "s01C0", "x10M1", "s01M0", "+1", "s01M1",
    ],
    "e": [
        "d00M0", "d00C0", "d00C1", "d00M1", "d01C0", "s10C0", "d01C1", "x00M0", "s11C0", "x00M1", "x01C0", "x01C1",
        "x00C0", "s11M0", "s10C1", "s11M1",
    ],
}
TOKENS = {
    "M": [
        "0d00M0", "1d00M1", "4d10M0", "4d00C0", "5d01M0", "6d10C0", "6d01C0", "7d00C1", "8d11M0", "8d10C1", "10d10M1", "10d01M1",
        "12d11C0", "12d11M1", "14d01C1", "16d11C1", "17x00M0", "17x00M1", "18x00C0", "18x01M0", "19x01M1", "19x10M0", "20x00C1", "20x11M0",
        "22x10M1", "22x01C0", "24x01C1", "24x11C0", "26x11C1", "28x10C0", "28x10C1", "32x11M1",
    ],
    "C": [
        "0d00C0", "1d00C1", "4d10C0", "4d00M0", "6d10C1", "6d01M0", "8d01C0", "8d10M0", "10d11C0", "12d11M0", "12d01M1", "14d11M1",
        "14d00M1", "16d01C1", "16d10M1", "18d11C1", "19x00C0", "19x00C1", "20x01M1", "22x11M1", "22x10M0", "24x10C0", "24x01C0", "26x01C1",
        "26x10C1", "28x11C1", "28x00M1", "30x10M1", "30x00M0", "32x01M0", "34x11M0", "36x11C0",
    ],
}
X_FROM = {"M": 17, "C": 19}
LAST = {"M": (33, 36), "C": (33, 35)}
STEPS = 37
RING = 8


def seen_by_receiver(unit, link):
    flip = {"0": "1", "1": "0"}
    if link == Y_:
        return flip[unit[0]] + unit[1:]
    return unit[0] + flip[unit[1]] + unit[2] if link == D_ else unit


def pack(unit):
    return int(unit[0]) + 2 * int(unit[1]) + 4 * (unit[2] == "M")


def select(key, table):
    out = jnp.int32(0)
    for k, v in table.items():
        out = jnp.where(key == k, jnp.int32(v), out)
    return out


def plan():
    send, recv = ({P_: {}, D_: {}, Y_: {}} for _ in range(2))
    sums, terms = {"M": {}, "C": {}}, {}
    for name, entries in START.items():
        sender, receiver, link = LINKS[name]
        t = count = 0
        for what in entries:
            if what[0] == "+":
                t += int(what)
                continue
            kind, unit, h = what[0], what[1:4], int(what[4])
            there = seen_by_receiver(unit, link)
            if kind == "s":
                sums[sender].setdefault(t, []).append((unit, h, link, count % 2, count >= 2, 0))
                terms.setdefault((receiver, there, h), []).append(link)
                count += 1
            for k in range(0 if kind == "s" else 2):
                code = 1 + "dx".index(kind) + 16 * (2 * h + k)
                send[link][ROLES.index(sender) * 100 + t + k] = code + 2 * pack(unit)
                recv[link][ROLES.index(receiver) * 100 + t + k + 2] = code + 2 * pack(there)
            t += 2
    for role in ROLES:
        for h in range(2):
            early = LAST[role][h] == max(LAST[role])
            sums[role].setdefault(LAST[role][h], []).insert(0, ("00" + role, h, 3, 0, 0, early))
    sum_count, sum_what, tok_count, tok_what = {}, {}, {}, {}
    for r, role in enumerate(ROLES):
        for t, entries in sums[role].items():
            sum_count[r * 100 + t] = len(entries)
            for k, (unit, h, link, parity, before, early) in enumerate(entries):
                code = pack(unit) + 8 * h + 16 * sum(1 << i for i in terms.get((role, unit, h), []))
                sum_what[(r * 100 + t) * 10 + k] = code + 128 * link + 512 * parity + 1024 * before + 2048 * early
        for what in TOKENS[role]:
            t, kind, unit, h = int(what[:-5]), what[-5], what[-4:-1], int(what[-1])
            k = tok_count.get(r * 100 + t, 0)
            tok_count[r * 100 + t] = k + 1
            code = pack(unit) + 8 * h + 16 * "dx".index(kind)
            tok_what[(r * 100 + t) * 10 + k] = code + 32 * (what is TOKENS[role][-1])
    return send, recv, sum_count, sum_what, tok_count, tok_what


def last_code(role):
    what = TOKENS[role][-1]
    return pack(what[-4:-1]) + 8 * int(what[-1])


def kernel(
    x, dy, gate, up, w_gate, w_up, w_down,
    dx, wd, acc, dg_last, du_last, full, parts,
    wg, wu, dg, du, tok, gb, ub, dh, total, ext, out, outw,
    ag_recv, ag_send, w_recv, w_send, rs_recv, rs_send, p_send, l_sem, tok_sem, g_sem, u_sem, e_sem,
):
    block, depth = dy.shape
    width = gate.shape[1]
    rows, quarter = block // 2, block // 4
    tile = 512
    nj, ni = depth // 128, width // 128
    own_in = {DY: dy, X: x}
    send_what, recv_what, sum_count, sum_what, tok_count, tok_what = plan()

    tp = lax.axis_index("tp")
    core, chip = tp % 2, tp // 2
    y, z = chip // 4, chip % 4
    half = z // 2
    middle = ((z + 1) % 4) // 2
    is_m, is_c = middle == 1, middle == 0
    role = 1 - middle

    def chip_of(yy, hh, mm):
        return yy * 4 + mm + hh * (3 - 2 * mm)

    def chip_packed(code):
        ry, rh, mm = code % 2, (code // 2) % 2, (code // 4) % 2
        return chip_of(y + ry - 2 * y * ry, half + rh - 2 * half * rh, mm)

    partner = tp + 1 - 2 * core
    at_link = {
        P_: chip_of(y, half, 1 - middle) * 2 + core,
        D_: chip_of(y, 1 - half, middle) * 2 + core,
        Y_: chip_of(1 - y, half, middle) * 2 + core,
    }

    def span(h):
        return pl.ds(pl.multiple_of(h * rows, rows), rows)

    def quarter_at(p):
        return pl.ds(pl.multiple_of(p * quarter, quarter), quarter)

    def remote(src, dst, send, recv, to):
        return pltpu.make_async_remote_copy(
            src_ref=src, dst_ref=dst, send_sem=send, recv_sem=recv, device_id={"tp": to}, device_id_type=MESH
        )

    def by_rows(step, n_rows, fn):
        def body(i, _):
            fn(pl.ds(pl.multiple_of(i * step, step), step))
            return 0

        lax.fori_loop(0, n_rows // step, body, 0)


    def on_link(link, code, s, src=None):
        code = code - 1
        array, c, p = code % 2, chip_packed(code // 2), code // 16
        piece = quarter_at(p)
        to = full.at[array, c * 2 + core, piece]
        return remote(to if src is None else src.at[piece], to, ag_send.at[link, s % RING], ag_recv.at[array, c, p], at_link[link])

    def to_partner(array, c, p, src=None):
        piece = quarter_at(p)
        to = full.at[array, c * 2 + core, piece]
        return remote(to if src is None else src.at[piece], to, w_send.at[array, c, p], w_recv.at[array, c, p], partner)

    def from_partner(array, c, h):
        for k in range(2):
            there = full.at[array, c * 2 + 1 - core, quarter_at(2 * h + k)]
            remote(there, there, p_send.at[0], w_recv.at[array, c, 2 * h + k], partner).wait_recv()

    def settle(s):
        for link in (P_, D_, Y_):

            @pl.when(select(role * 100 + s, send_what[link]) > 0)
            def _(link=link):
                on_link(link, jnp.int32(1), s).wait_send()

    def communicate(s):
        key = role * 100 + s
        come = {link: select(key, recv_what[link]) for link in (P_, D_, Y_)}
        for link, code in come.items():

            @pl.when(code > 0)
            def _(link=link, code=code):
                on_link(link, code, s).wait_recv()

        settle(s - RING)
        for link in (P_, D_, Y_):
            code = select(key, send_what[link])
            mine = chip_packed((code - 1) // 2) == chip

            @pl.when((code > 0) & jnp.logical_not(mine))
            def _(link=link, code=code):
                on_link(link, code, s).start()

            for array in (DY, X):

                @pl.when((code > 0) & mine & ((code - 1) % 2 == array))
                def _(link=link, code=code, array=array):
                    on_link(link, code, s, own_in[array]).start()

        for link, code in come.items():

            @pl.when(code > 0)
            def _(code=code):
                to_partner((code - 1) % 2, chip_packed((code - 1) // 2), (code - 1) // 16).start()

        for array, when in ((DY, 0), (X, 2)):

            @pl.when(s == when)
            def _(array=array):
                for p in range(4):
                    to_partner(array, chip, p, own_in[array]).start()


    def dx_term(code, plane):
        index = chip_packed(code) * 2 + (code // 8) % 2
        here = span(plane)

        def column(n, _):
            cols = pl.ds(pl.multiple_of(n * tile, tile), tile)
            total[:, cols] = lax.dot_general(
                dg[index, here, :], wg[cols, :], (((1,), (1,)), ((), ())), preferred_element_type=F32
            ) + lax.dot_general(du[index, here, :], wu[cols, :], (((1,), (1,)), ((), ())), preferred_element_type=F32)
            return 0

        lax.fori_loop(0, depth // tile, column, 0)

    def reduce_one(code):
        c, h = chip_packed(code), (code // 8) % 2
        mask, link, parity, before = (code // 16) % 8, (code // 128) % 4, (code // 512) % 2, (code // 1024) % 2
        bits = {P_: mask % 2 == 1, D_: (mask // 2) % 2 == 1, Y_: mask // 4 == 1}

        def term_in(kind):
            return pltpu.make_async_copy(parts.at[kind, c, span(h)], ext.at[kind], e_sem.at[kind])

        def fetch(kind):
            remote(ext.at[kind], parts.at[kind, c, span(h)], p_send.at[0], rs_recv.at[kind, c, h], partner).wait_recv()
            term_in(kind).start()

        def send_term(to):
            return remote(out.at[link, parity], parts.at[link, c, span(h)], rs_send.at[link, parity], rs_recv.at[link, c, h], to)

        fetch(W_)
        for kind in (P_, D_, Y_):

            @pl.when(bits[kind] & (link != 3))
            def _(kind=kind):
                fetch(kind)

        @pl.when(code < 2048)
        def _():
            dx_term(code, core)

        for kind in (P_, D_, Y_):

            @pl.when(bits[kind] & (link == 3))
            def _(kind=kind):
                fetch(kind)

        for kind in (P_, D_, Y_):

            @pl.when(bits[kind])
            def _(kind=kind):
                term_in(kind).wait()

                def add(r):
                    total[r, :] += ext[kind, r, :].astype(F32)

                by_rows(16, rows, add)

        term_in(W_).wait()

        @pl.when(link == 3)
        def _():
            def finish(r):
                to = pl.ds(pl.multiple_of(h * rows + r.start, 16), 16)
                dx[to, :] = (total[r, :] + ext[W_, r, :].astype(F32)).astype(BF16)

            by_rows(16, rows, finish)

        @pl.when(link != 3)
        def _():
            to = jnp.where(link == P_, at_link[P_], jnp.where(link == D_, at_link[D_], at_link[Y_]))

            @pl.when(before == 1)
            def _():
                send_term(to).wait_send()

            def round_(r):
                out[link, parity, r, :] = (total[r, :] + ext[W_, r, :].astype(F32)).astype(BF16)

            by_rows(16, rows, round_)
            send_term(to).start()

    def term_to_partner(code, b):
        c, h = chip_packed(code), (code // 8) % 2
        return remote(outw.at[b], parts.at[W_, c, span(h)], p_send.at[b], rs_recv.at[W_, c, h], partner)

    def partner_one(code, k):
        b = k % 2
        dx_term(code, 1 - core)

        @pl.when(k >= 2)
        def _():
            term_to_partner(code, b).wait_send()

        def round_(r):
            outw[b, r, :] = total[r, :].astype(BF16)

        by_rows(16, rows, round_)
        term_to_partner(code, b).start()


    def last_in(code, b):
        c, h = chip_packed(code), (code // 8) % 2
        src = full.at[X, c * 2 + core, span(h)]
        return pltpu.make_async_copy(src, tok.at[b, span(core)], tok_sem.at[b, core])

    def tok_in(code, b, start):
        @pl.when(code < 32)
        def _():
            pair_in(code, b, start)

        @pl.when(code >= 32)
        def _():
            copy = last_in(code, b)
            copy.start() if start else copy.wait()

    def pair_in(code, b, start):
        c, h, array = chip_packed(code), (code // 8) % 2, (code // 16) % 2
        mine = c == chip
        for plane in range(2):
            blk = c * 2 + plane
            here = slice(plane * rows, (plane + 1) * rows)
            dst, src, sem = tok.at[b, here], full.at[array, blk, span(h)], tok_sem.at[b, plane]
            spread = pl.ds(pl.multiple_of(blk * block + h * rows, rows), rows)
            pair = (
                pltpu.make_async_copy(gate.at[spread], gb.at[b, here], g_sem.at[b, plane]),
                pltpu.make_async_copy(up.at[spread], ub.at[b, here], u_sem.at[b, plane]),
            )
            if not start:
                pltpu.make_async_copy(src, dst, sem).wait()

                @pl.when(array == DY)
                def _(pair=pair):
                    for copy in pair:
                        copy.wait()

                continue

            @pl.when(array == DY)
            def _(pair=pair):
                for copy in pair:
                    copy.start()

            local = mine & (core == plane)

            @pl.when(core != plane)
            def _():
                from_partner(array, c, h)

            @pl.when(jnp.logical_not(local))
            def _(src=src, dst=dst, sem=sem):
                pltpu.make_async_copy(src, dst, sem).start()

            for a in (DY, X):

                @pl.when(local & (array == a))
                def _(a=a, dst=dst, sem=sem):
                    pltpu.make_async_copy(own_in[a].at[span(h)], dst, sem).start()

    def work_dy(code, b):
        index = chip_packed(code) * 2 + (code // 8) % 2
        dh[...] = lax.dot_general(tok[b], wd[...], (((1,), (1,)), ((), ())), preferred_element_type=F32)

        def pointwise(r):
            g, u, d = gb[b, r, :].astype(F32), ub[b, r, :].astype(F32), dh[r, :]
            g2 = g * g
            t = jnp.tanh(g * (0.7978845608028654 + (0.7978845608028654 * 0.044715) * g2))
            cdf = 0.5 + 0.5 * t
            act = g * cdf
            slope = cdf + (0.5 * g) * (1.0 - t * t) * (0.7978845608028654 + (3 * 0.7978845608028654 * 0.044715) * g2)
            du[index, r, :] = (d * act).astype(BF16)
            dg[index, r, :] = ((d * u) * slope).astype(BF16)
            gb[b, r, :] = (act * u).astype(BF16)

        by_rows(16, 2 * rows, pointwise)

        def column(n, _):
            cols = pl.ds(pl.multiple_of(n * tile, tile), tile)
            new = lax.dot_general(gb[b], tok[b, :, cols], (((0,), (0,)), ((), ())), preferred_element_type=F32)
            for i in range(ni):
                for j in range(tile // 128):
                    k = i * nj + n * (tile // 128) + j
                    acc[0, k] += new[i * 128 : (i + 1) * 128, j * 128 : (j + 1) * 128]
            return 0

        lax.fori_loop(0, depth // tile, column, 0)

    def x_columns(index, b, here):
        def column(n, _):
            cols = pl.ds(pl.multiple_of(n * tile, tile), tile)
            xt = tok[b, here, cols]
            for a, d in enumerate((dg, du)):
                new = lax.dot_general(xt, d[index, here, :], (((0,), (0,)), ((), ())), preferred_element_type=F32)
                for i in range(tile // 128):
                    for j in range(ni):
                        k = (n * (tile // 128) + i) * ni + j
                        acc[a, k] += new[i * 128 : (i + 1) * 128, j * 128 : (j + 1) * 128]
            return 0

        lax.fori_loop(0, depth // tile, column, 0)

    def work_x(code, b):
        x_columns(chip_packed(code) * 2 + (code // 8) % 2, b, slice(None))

    def last_x(code, b):
        c, h = chip_packed(code), (code // 8) % 2
        x_columns(c * 2 + h, b, span(core))

        def keep(r):
            there = pl.ds(pl.multiple_of((1 - core) * rows + r.start, 16), 16)
            dg_last[r, :] = dg[c * 2 + h, there, :]
            du_last[r, :] = du[c * 2 + h, there, :]

        by_rows(16, rows, keep)
        from_partner(X, c, h)

    def finish_down():
        for i in range(ni):
            for j in range(nj):
                wd[i * 128 : (i + 1) * 128, j * 128 : (j + 1) * 128] = acc[0, i * nj + j].astype(BF16)
                acc[0, i * nj + j] = jnp.zeros((128, 128), F32)

    def clear(i):
        def body(k, _):
            acc[i, k] = jnp.zeros((128, 128), F32)
            return 0

        lax.fori_loop(0, ni * nj, body, 0)


    loads = [pltpu.make_async_copy(s, d, l_sem.at[i]) for i, (s, d) in enumerate(((w_down, wd), (w_gate, wg), (w_up, wu)))]
    for load in loads:
        load.start()

    barrier = pltpu.get_barrier_semaphore()
    for to in (at_link[P_], at_link[Y_], partner):
        pl.semaphore_signal(barrier, inc=1, device_id={"tp": to}, device_id_type=MESH)

    @pl.when(is_m)
    def _():
        pl.semaphore_signal(barrier, inc=1, device_id={"tp": at_link[D_]}, device_id_type=MESH)
        pl.semaphore_wait(barrier, 4)

    @pl.when(is_c)
    def _():
        pl.semaphore_wait(barrier, 3)

    x_from = jnp.where(is_m, X_FROM["M"], X_FROM["C"])

    last_sum = jnp.where(is_m, max(LAST["M"]), max(LAST["C"]))

    def step(s, _):
        @pl.when(s == last_sum)
        def _():
            dx_term(select((role * 100 + s) * 10, sum_what), core)

        communicate(s)

        @pl.when(s == x_from)
        def _():
            finish_down()

        key = role * 100 + s
        n_tok = select(key, tok_count)

        @pl.when(n_tok > 0)
        def _():
            tok_in(select(key * 10, tok_what), 0, True)

        @pl.when(s == 0)
        def _():
            clear(0)
            clear(1)
            for load in loads:
                load.wait()

        def sums(k, _):
            reduce_one(select(key * 10 + k, sum_what))
            return 0

        def tokens(k, _):
            code, b = select(key * 10 + k, tok_what), k % 2

            @pl.when(k + 1 < n_tok)
            def _():
                tok_in(select(key * 10 + k + 1, tok_what), 1 - b, True)

            tok_in(code, b, False)

            @pl.when((code // 16) % 2 == DY)
            def _():
                work_dy(code, b)

            @pl.when(code // 16 == X)
            def _():
                work_x(code, b)

            @pl.when(code >= 32)
            def _():
                last_x(code, b)

            return 0

        lax.fori_loop(0, select(key, sum_count), sums, 0)
        lax.fori_loop(0, n_tok, tokens, 0)

        n_next = select(key + 1, sum_count)

        def partners(k, _):
            partner_one(select((key + 1) * 10 + k, sum_what), k)
            return 0

        lax.fori_loop(0, n_next, partners, 0)
        for b in range(2):

            @pl.when(n_next > b)
            def _(b=b):
                term_to_partner(0, b).wait_send()

        return 0

    lax.fori_loop(0, STEPS, step, 0)

    def rest(s, _):
        settle(s)
        return 0

    lax.fori_loop(STEPS - RING, STEPS, rest, 0)
    for link in (P_, D_, Y_):

        @pl.when(is_m | (link != D_))
        def _(link=link):
            for parity in range(2):
                half_block = parts.at[link, 0, span(0)]
                remote(out.at[link, parity], half_block, rs_send.at[link, parity], rs_recv.at[link, 0, 0], partner).wait_send()

    def left(i, _):
        to_partner(i // 32, (i // 4) % 8, i % 4).wait_send()
        return 0

    lax.fori_loop(0, 64, left, 0)


def finish(dx, wd, acc, dg, du, full, to_x, to_gate, to_up, to_down, rows_in, done, x_sem, d_sem, g_sem):
    depth, width = to_gate.shape
    rows, tile, ni = rows_in.shape[0], 512, width // 128
    tp = lax.axis_index("tp")
    core, y, z = tp % 2, tp // 8, (tp // 2) % 4
    half, middle = z // 2, ((z + 1) % 4) // 2
    code = jnp.where(middle == 1, last_code("M"), last_code("C"))
    ry, rh, mm, h = code % 2, (code // 2) % 2, (code // 4) % 2, code // 8
    yy, hh = y + ry - 2 * y * ry, half + rh - 2 * half * rh
    chip = yy * 4 + mm + hh * (3 - 2 * mm)
    load = pltpu.make_async_copy(full.at[X, chip * 2 + 1 - core, pl.ds(pl.multiple_of(h * rows, rows), rows)], rows_in, x_sem.at[0])
    load.start()
    copies = []
    for i, (result, place) in enumerate(((dx, to_x), (wd, to_down))):
        n = result.shape[0] // 4
        for k in range(4):
            here = pl.ds(k * n, n)
            copies.append(pltpu.make_async_copy(result.at[here], place.at[here], d_sem.at[i, k]))
    for copy in copies:
        copy.start()
    load.wait()

    def store(a, n):
        here = pl.ds(pl.multiple_of(n * tile, tile), tile)
        return pltpu.make_async_copy(done.at[a, here], (to_gate, to_up)[a].at[here], g_sem.at[a, n])

    def column(n, _):
        xt = rows_in[:, pl.ds(pl.multiple_of(n * tile, tile), tile)]
        for a, d in enumerate((dg, du)):
            new = lax.dot_general(xt, d[...], (((0,), (0,)), ((), ())), preferred_element_type=F32)
            for i in range(tile // 128):
                to = pl.ds(pl.multiple_of(n * tile + i * 128, 128), 128)
                for j in range(ni):
                    k = (n * (tile // 128) + i) * ni + j
                    one = acc[a, k] + new[i * 128 : (i + 1) * 128, j * 128 : (j + 1) * 128]
                    done[a, to, j * 128 : (j + 1) * 128] = one.astype(BF16)
            store(a, n).start()
        return 0

    lax.fori_loop(0, depth // tile, column, 0)
    for copy in copies:
        copy.wait()
    for n in range(depth // tile):
        for a in range(2):
            store(a, n).wait()


def solution(mesh):
    def step(x, dy, gate, up, w_gate, w_up, w_down):
        block, depth = dy.shape
        tokens, width = gate.shape
        rows, chips = block // 2, tokens // block // 2
        anywhere, inside = pl.BlockSpec(memory_space=pl.ANY), pl.BlockSpec(memory_space=pltpu.VMEM)
        dma, flops = pltpu.SemaphoreType.DMA, 12 * tokens * depth * width
        outs = pl.pallas_call(
            kernel,
            out_shape=[
                pltpu.VMEM((block, depth), BF16),
                pltpu.VMEM((width, depth), BF16),
                pltpu.VMEM((2, (depth // 128) * (width // 128), 128, 128), F32),
                pltpu.VMEM((rows, width), BF16),
                pltpu.VMEM((rows, width), BF16),
                jax.ShapeDtypeStruct((2, 2 * chips, block, depth), BF16),
                jax.ShapeDtypeStruct((4, chips, block, depth), BF16),
            ],
            in_specs=[anywhere] * 7,
            out_specs=[inside] * 5 + [anywhere] * 2,
            scratch_shapes=[
                pltpu.VMEM((depth, width), BF16),
                pltpu.VMEM((depth, width), BF16),
                pltpu.VMEM((2 * chips, 2 * rows, width), BF16),
                pltpu.VMEM((2 * chips, 2 * rows, width), BF16),
                pltpu.VMEM((2, 2 * rows, depth), BF16),
                pltpu.VMEM((2, 2 * rows, width), BF16),
                pltpu.VMEM((2, 2 * rows, width), BF16),
                pltpu.VMEM((2 * rows, width), F32),
                pltpu.VMEM((rows, depth), F32),
                pltpu.VMEM((4, rows, depth), BF16),
                pltpu.VMEM((3, 2, rows, depth), BF16),
                pltpu.VMEM((2, rows, depth), BF16),
                dma((2, chips, 4)),
                dma((3, RING)),
                dma((2, chips, 4)),
                dma((2, chips, 4)),
                dma((4, chips, 2)),
                dma((3, 2)),
                dma((2,)),
                dma((3,)),
                dma((2, 2)),
                dma((2, 2)),
                dma((2, 2)),
                dma((4,)),
            ],
            compiler_params=pltpu.CompilerParams(collective_id=0, has_side_effects=True, vmem_limit_bytes=47950000),
            cost_estimate=pl.CostEstimate(flops=flops, bytes_accessed=12 * tokens * depth, transcendentals=tokens * width),
            name="mlp_backward",
        )(x, dy, gate, up, w_gate, w_up, w_down)
        return pl.pallas_call(
            finish,
            out_shape=[jax.ShapeDtypeStruct(a.shape, BF16) for a in (dy, w_gate, w_up, w_down)],
            in_specs=[inside] * 5 + [anywhere],
            out_specs=[anywhere] * 4,
            scratch_shapes=[
                pltpu.VMEM((rows, depth), BF16),
                pltpu.VMEM((2, depth, width), BF16),
                dma((1,)),
                dma((2, 4)),
                dma((2, depth // 512)),
            ],
            compiler_params=pltpu.CompilerParams(vmem_limit_bytes=2**24),
            name="finish",
        )(*outs[:6])

    rows_, cols_ = P(("dp", "tp"), None), P("dp", "tp")
    return jax.shard_map(
        step,
        mesh=mesh,
        in_specs=(rows_, rows_, cols_, cols_, P(None, "tp"), P(None, "tp"), P("tp", None)),
        out_specs=(rows_, cols_, cols_, rows_),
        check_vma=False,
    )
```

```python
import jax
import jax.numpy as jnp
from jax import lax
from jax.experimental import pallas as pl
from jax.experimental.pallas import tpu as pltpu
from jax.sharding import PartitionSpec as P

MESH = pl.DeviceIdType.MESH
F32, BF16 = jnp.float32, jnp.bfloat16

P_, D_, Y_, W_ = 0, 1, 2, 3
DY, X = 0, 1
ROLES = "MC"
LINKS = {"a": ("C", "C", Y_), "b": ("M", "C", P_), "c": ("C", "M", P_), "d": ("M", "M", D_), "e": ("M", "M", Y_)}

START = {
    "a": [
        "d00C0", "x00C0", "d01M1", "d01C0", "d00M1", "d01C1", "d01M0", "d00C1", "d00M0", "s10M1", "x00C1", "x01C1",
        "x00M0", "x01C0", "s10M0", "x01M0", "x01M1",
    ],
    "b": [
        "d00M1", "d01M1", "d01C0", "d00M0", "d01C1", "d01M0", "x00M1", "s10M1", "x01M1", "s10M0", "x01C1", "x00M0",
        "x01C0", "x10M1", "x01M0", "s00C1", "s00C0",
    ],
    "c": [
        "d00C0", "x00C1", "d00C1", "s10C0", "x00C0", "s11M1", "s11C0", "s01C1", "s11C1", "s01M0", "s10C1", "s11M0",
        "s01C0", "s01M1", "s00M1", "x10C1", "s00M0",
    ],
    "d": [
        "d00M1", "d00C0", "x10M0", "d00C1", "d00M0", "d10M1", "x00C1", "x00M1", "d10M0", "s01C1", "s11C1", "x00C0",
        "x10M1", "x00M0", "s01C0", "s01M1", "s01M0",
    ],
    "e": [
        "x00M0", "d00C0", "d01C0", "d00C1", "d00M1", "d01C1", "d00M0", "x01C1", "s11C0", "s11M1", "s10C0", "x00M1",
        "x01C0", "s10C1", "s11M0", "x00C0",
    ],
}
TOKENS = {
    "M": [
        "0d00M0", "1d00M1", "4d01M1", "4d00C0", "6d10C0", "6d01C0", "8d11C0", "8d00C1", "10d01C1", "10d10C1", "12d10M1", "12d01M0",
        "14d11M1", "14d11C1", "16d10M0", "20d11M0", "21x00M0", "21x00M1", "22x10M0", "22x00C1", "23x11M0", "23x00C0", "24x01C1", "24x01M1",
        "25x11C1", "26x01C0", "26x10M1", "28x11C0", "28x11M1", "30x01M0", "34x10C1", "34x10C0",
    ],
    "C": [
        "0d00C0", "1d00C1", "4d10C0", "4d00M1", "6d01M1", "8d11M1", "8d01C0", "10d11C0", "10d00M0", "12d01C1", "12d10M1", "14d11C1",
        "14d01M0", "16d11M0", "18d10C1", "20d10M0", "21x00C0", "21x00C1", "22x10C0", "22x00M1", "23x01M1", "24x10C1", "24x01C1", "26x00M0",
        "26x11C1", "28x01C0", "28x10M0", "30x10M1", "30x11C0", "32x01M0", "34x11M0", "36x11M1",
    ],
}
X_FROM = {"M": 21, "C": 21}
LAST = {"M": (35, 33), "C": (35, 33)}
STEPS = 37


def seen_by_receiver(unit, link):
    flip = {"0": "1", "1": "0"}
    if link == Y_:
        return flip[unit[0]] + unit[1:]
    return unit[0] + flip[unit[1]] + unit[2] if link == D_ else unit


def pack(unit):
    return int(unit[0]) + 2 * int(unit[1]) + 4 * (unit[2] == "M")


def select(key, table):
    out = jnp.int32(0)
    for k, v in table.items():
        out = jnp.where(key == k, jnp.int32(v), out)
    return out


def plan():
    send, recv = ({P_: {}, D_: {}, Y_: {}} for _ in range(2))
    sums, terms = {"M": {}, "C": {}}, {}
    for name, entries in START.items():
        sender, receiver, link = LINKS[name]
        t = count = 0
        for what in entries:
            if what[0] == "+":
                t += int(what)
                continue
            kind, unit, h = what[0], what[1:4], int(what[4])
            there = seen_by_receiver(unit, link)
            if kind == "s":
                sums[sender].setdefault(t, []).append((unit, h, link, count % 2, count >= 2, 0))
                terms.setdefault((receiver, there, h), []).append(link)
                count += 1
            for k in range(0 if kind == "s" else 2):
                code = 1 + "dx".index(kind) + 16 * (2 * h + k)
                send[link][ROLES.index(sender) * 100 + t + k] = code + 2 * pack(unit)
                recv[link][ROLES.index(receiver) * 100 + t + k + 2] = code + 2 * pack(there)
            t += 2
    for role in ROLES:
        for h in range(2):
            early = h == (LAST[role][1] >= LAST[role][0])
            sums[role].setdefault(LAST[role][h], []).insert(0, ("00" + role, h, 3, 0, 0, early))
    sum_count, sum_what, tok_count, tok_what = {}, {}, {}, {}
    for r, role in enumerate(ROLES):
        for t, entries in sums[role].items():
            sum_count[r * 100 + t] = len(entries)
            for k, (unit, h, link, parity, before, early) in enumerate(entries):
                code = pack(unit) + 8 * h + 16 * sum(1 << i for i in terms.get((role, unit, h), []))
                sum_what[(r * 100 + t) * 10 + k] = code + 128 * link + 512 * parity + 1024 * before + 2048 * early
        for what in TOKENS[role]:
            t, kind, unit, h = int(what[:-5]), what[-5], what[-4:-1], int(what[-1])
            k = tok_count.get(r * 100 + t, 0)
            tok_count[r * 100 + t] = k + 1
            code = pack(unit) + 8 * h + 16 * "dx".index(kind)
            tok_what[(r * 100 + t) * 10 + k] = code + 32 * (what is TOKENS[role][-1])
    return send, recv, sum_count, sum_what, tok_count, tok_what


def last_code(role):
    what = TOKENS[role][-1]
    return pack(what[-4:-1]) + 8 * int(what[-1])


def kernel(
    x, dy, gate, up, w_gate, w_up, w_down,
    dx, wd, acc, d_last, last_rows, full, parts,
    w, d, tok, gb, ub, dh, total, ext, out, outw,
    ag_recv, ag_send, w_recv, w_send, rs_recv, rs_send, p_send, l_send, l_sem, tok_sem, g_sem, u_sem, e_sem,
):
    block, depth = dy.shape
    width = gate.shape[1]
    rows, quarter = block // 2, block // 4
    tile = 512
    nj, ni = depth // 128, width // 128
    own_in = {DY: dy, X: x}
    send_what, recv_what, sum_count, sum_what, tok_count, tok_what = plan()

    tp = lax.axis_index("tp")
    core, chip = tp % 2, tp // 2
    y, z = chip // 4, chip % 4
    half = z // 2
    middle = ((z + 1) % 4) // 2
    is_m, is_c = middle == 1, middle == 0
    role = 1 - middle

    def chip_of(yy, hh, mm):
        return yy * 4 + mm + hh * (3 - 2 * mm)

    def chip_packed(code):
        ry, rh, mm = code % 2, (code // 2) % 2, (code // 4) % 2
        return chip_of(y + ry - 2 * y * ry, half + rh - 2 * half * rh, mm)

    partner = tp + 1 - 2 * core
    at_link = {
        P_: chip_of(y, half, 1 - middle) * 2 + core,
        D_: chip_of(y, 1 - half, middle) * 2 + core,
        Y_: chip_of(1 - y, half, middle) * 2 + core,
    }

    def span(h):
        return pl.ds(pl.multiple_of(h * rows, rows), rows)

    def quarter_at(p):
        return pl.ds(pl.multiple_of(p * quarter, quarter), quarter)

    def remote(src, dst, send, recv, to):
        return pltpu.make_async_remote_copy(
            src_ref=src, dst_ref=dst, send_sem=send, recv_sem=recv, device_id={"tp": to}, device_id_type=MESH
        )

    def by_rows(step, n_rows, fn):
        def body(i, _):
            fn(pl.ds(pl.multiple_of(i * step, step), step))
            return 0

        lax.fori_loop(0, n_rows // step, body, 0)


    def on_link(link, code, src=None):
        code = code - 1
        array, c, p = code % 2, chip_packed(code // 2), code // 16
        piece = quarter_at(p)
        to = full.at[array, c * 2 + core, piece]
        return remote(to if src is None else src.at[piece], to, ag_send.at[link], ag_recv.at[array, c, p], at_link[link])

    def to_partner(array, c, p, src=None):
        piece = quarter_at(p)
        to = full.at[array, c * 2 + core, piece]
        return remote(to if src is None else src.at[piece], to, w_send.at[array], w_recv.at[array, c, p], partner)

    last = jnp.where(is_m, last_code("M"), last_code("C"))

    def last_to_partner():
        c, h = chip_packed(last), last // 8
        here = full.at[X, c * 2 + core, span(h)]
        return remote(here, last_rows, l_send, w_recv.at[X, c, 2 * h + 1], partner)

    def from_partner(array, c, h):
        for k in range(2):
            there = full.at[array, c * 2 + 1 - core, quarter_at(2 * h + k)]
            remote(there, there, p_send, w_recv.at[array, c, 2 * h + k], partner).wait_recv()

    def communicate(s):
        key = role * 100 + s
        come = {link: select(key, recv_what[link]) for link in (P_, D_, Y_)}
        for link, code in come.items():

            @pl.when(code > 0)
            def _(link=link, code=code):
                on_link(link, code).wait_recv()

        for link in (P_, D_, Y_):
            code = select(key, send_what[link])
            mine = chip_packed((code - 1) // 2) == chip

            @pl.when((code > 0) & jnp.logical_not(mine))
            def _(link=link, code=code):
                on_link(link, code).start()

            for array in (DY, X):

                @pl.when((code > 0) & mine & ((code - 1) % 2 == array))
                def _(link=link, code=code, array=array):
                    on_link(link, code, own_in[array]).start()

        for link, code in come.items():

            ends = ((code - 1) % 16 == X + 2 * (last % 8)) & ((code - 1) // 32 == last // 8)

            @pl.when((code > 0) & jnp.logical_not(ends))
            def _(code=code):
                to_partner((code - 1) % 2, chip_packed((code - 1) // 2), (code - 1) // 16).start()

            @pl.when(ends & ((code - 1) // 16 % 2 == 1))
            def _():
                last_to_partner().start()

        for array, when in ((DY, 0), (X, 2)):

            @pl.when(s == when)
            def _(array=array):
                for p in range(4):
                    to_partner(array, chip, p, own_in[array]).start()


    def dx_term(code, plane):
        index = chip_packed(code) * 2 + (code // 8) % 2
        here = span(plane)

        def column(n, _):
            cols = pl.ds(pl.multiple_of(n * tile, tile), tile)
            total[:, cols] = lax.dot_general(
                d[index, here, :], w[cols, :], (((1,), (1,)), ((), ())), preferred_element_type=F32
            )
            return 0

        lax.fori_loop(0, depth // tile, column, 0)

    def reduce_one(code):
        c, h = chip_packed(code), (code // 8) % 2
        mask, link, parity, before = (code // 16) % 8, (code // 128) % 4, (code // 512) % 2, (code // 1024) % 2
        bits = {P_: mask % 2 == 1, D_: (mask // 2) % 2 == 1, Y_: mask // 4 == 1}

        def term_in(kind):
            return pltpu.make_async_copy(parts.at[kind, c, span(h)], ext.at[kind], e_sem.at[kind])

        def fetch(kind):
            remote(ext.at[kind], parts.at[kind, c, span(h)], p_send, rs_recv.at[kind, c, h], partner).wait_recv()
            term_in(kind).start()

        def send_term(to):
            return remote(out.at[link, parity], parts.at[link, c, span(h)], rs_send.at[link, parity], rs_recv.at[link, c, h], to)

        fetch(W_)
        for kind in (P_, D_, Y_):

            @pl.when(bits[kind] & (link != 3))
            def _(kind=kind):
                fetch(kind)

        @pl.when(code < 2048)
        def _():
            dx_term(code, core)

        for kind in (P_, D_, Y_):

            @pl.when(bits[kind] & (link == 3))
            def _(kind=kind):
                fetch(kind)

        for kind in (P_, D_, Y_):

            @pl.when(bits[kind])
            def _(kind=kind):
                term_in(kind).wait()

                def add(r):
                    total[r, :] += ext[kind, r, :].astype(F32)

                by_rows(16, rows, add)

        term_in(W_).wait()

        @pl.when(link == 3)
        def _():
            def finish(r):
                to = pl.ds(pl.multiple_of(h * rows + r.start, 16), 16)
                dx[to, :] = (total[r, :] + ext[W_, r, :].astype(F32)).astype(BF16)

            by_rows(16, rows, finish)

        @pl.when(link != 3)
        def _():
            to = jnp.where(link == P_, at_link[P_], jnp.where(link == D_, at_link[D_], at_link[Y_]))

            @pl.when(before == 1)
            def _():
                send_term(to).wait_send()

            def round_(r):
                out[link, parity, r, :] = (total[r, :] + ext[W_, r, :].astype(F32)).astype(BF16)

            by_rows(16, rows, round_)
            send_term(to).start()

    def term_to_partner(code):
        c, h = chip_packed(code), (code // 8) % 2
        return remote(outw, parts.at[W_, c, span(h)], p_send, rs_recv.at[W_, c, h], partner)

    def partner_one(code, first):
        dx_term(code, 1 - core)

        @pl.when(jnp.logical_not(first))
        def _():
            term_to_partner(code).wait_send()

        def round_(r):
            outw[r, :] = total[r, :].astype(BF16)

        by_rows(16, rows, round_)
        term_to_partner(code).start()


    def last_in(code, b):
        c, h = chip_packed(code), (code // 8) % 2
        src = full.at[X, c * 2 + core, span(h)]
        return pltpu.make_async_copy(src, tok.at[b, span(core)], tok_sem.at[b, core])

    def tok_in(code, b, start):
        @pl.when(code < 32)
        def _():
            pair_in(code, b, start)

        @pl.when(code >= 32)
        def _():
            copy = last_in(code, b)
            copy.start() if start else copy.wait()

    def pair_in(code, b, start):
        c, h, array = chip_packed(code), (code // 8) % 2, (code // 16) % 2
        mine = c == chip
        for plane in range(2):
            blk = c * 2 + plane
            here = slice(plane * rows, (plane + 1) * rows)
            dst, src, sem = tok.at[b, here], full.at[array, blk, span(h)], tok_sem.at[b, plane]
            spread = pl.ds(pl.multiple_of(blk * block + h * rows, rows), rows)
            pair = (
                pltpu.make_async_copy(gate.at[spread], gb.at[b, here], g_sem.at[b, plane]),
                pltpu.make_async_copy(up.at[spread], ub.at[b, here], u_sem.at[b, plane]),
            )
            if not start:
                pltpu.make_async_copy(src, dst, sem).wait()

                @pl.when(array == DY)
                def _(pair=pair):
                    for copy in pair:
                        copy.wait()

                continue

            @pl.when(array == DY)
            def _(pair=pair):
                for copy in pair:
                    copy.start()

            local = mine & (core == plane)

            @pl.when(core != plane)
            def _():
                from_partner(array, c, h)

            @pl.when(jnp.logical_not(local))
            def _(src=src, dst=dst, sem=sem):
                pltpu.make_async_copy(src, dst, sem).start()

            for a in (DY, X):

                @pl.when(local & (array == a))
                def _(a=a, dst=dst, sem=sem):
                    pltpu.make_async_copy(own_in[a].at[span(h)], dst, sem).start()

    def work_dy(code, b):
        index = chip_packed(code) * 2 + (code // 8) % 2
        dh[...] = lax.dot_general(tok[b], wd[...], (((1,), (1,)), ((), ())), preferred_element_type=F32)

        def pointwise(r):
            g, u, dhid = gb[b, r, :].astype(F32), ub[b, r, :].astype(F32), dh[r, :]
            g2 = g * g
            t = jnp.tanh(g * (0.7978845608028654 + (0.7978845608028654 * 0.044715) * g2))
            cdf = 0.5 + 0.5 * t
            act = g * cdf
            slope = cdf + (0.5 * g) * (1.0 - t * t) * (0.7978845608028654 + (3 * 0.7978845608028654 * 0.044715) * g2)
            d[index, r, width:] = (dhid * act).astype(BF16)
            d[index, r, :width] = ((dhid * u) * slope).astype(BF16)
            gb[b, r, :] = (act * u).astype(BF16)

        by_rows(16, 2 * rows, pointwise)

        def column(n, _):
            cols = pl.ds(pl.multiple_of(n * tile, tile), tile)
            new = lax.dot_general(gb[b], tok[b, :, cols], (((0,), (0,)), ((), ())), preferred_element_type=F32)
            for i in range(ni):
                for j in range(tile // 128):
                    k = i * nj + n * (tile // 128) + j
                    acc[0, k] += new[i * 128 : (i + 1) * 128, j * 128 : (j + 1) * 128]
            return 0

        lax.fori_loop(0, depth // tile, column, 0)

    def x_columns(index, b, here):
        def column(n, _):
            cols = pl.ds(pl.multiple_of(n * tile, tile), tile)
            xt = tok[b, here, cols]
            new = lax.dot_general(xt, d[index, here, :], (((0,), (0,)), ((), ())), preferred_element_type=F32)
            for i in range(tile // 128):
                for j in range(2 * ni):
                    k = (n * (tile // 128) + i) * ni + j % ni
                    acc[j // ni, k] += new[i * 128 : (i + 1) * 128, j * 128 : (j + 1) * 128]
            return 0

        lax.fori_loop(0, depth // tile, column, 0)

    def work_x(code, b):
        x_columns(chip_packed(code) * 2 + (code // 8) % 2, b, slice(None))

    def last_x(code, b):
        c, h = chip_packed(code), (code // 8) % 2
        x_columns(c * 2 + h, b, span(core))

        def keep(r):
            there = pl.ds(pl.multiple_of((1 - core) * rows + r.start, 16), 16)
            d_last[r, :] = d[c * 2 + h, there, :]

        by_rows(16, rows, keep)
        last_to_partner().wait_recv()

    def finish_down():
        for i in range(ni):
            for j in range(nj):
                wd[i * 128 : (i + 1) * 128, j * 128 : (j + 1) * 128] = acc[0, i * nj + j].astype(BF16)
                acc[0, i * nj + j] = jnp.zeros((128, 128), F32)

    def clear(i):
        def body(k, _):
            acc[i, k] = jnp.zeros((128, 128), F32)
            return 0

        lax.fori_loop(0, ni * nj, body, 0)


    pairs = (w_down, wd), (w_gate, w.at[:, :width]), (w_up, w.at[:, width:])
    loads = [pltpu.make_async_copy(s, d, l_sem.at[i]) for i, (s, d) in enumerate(pairs)]
    for load in loads:
        load.start()

    barrier = pltpu.get_barrier_semaphore()
    for to in (at_link[P_], at_link[Y_], partner):
        pl.semaphore_signal(barrier, inc=1, device_id={"tp": to}, device_id_type=MESH)

    @pl.when(is_m)
    def _():
        pl.semaphore_signal(barrier, inc=1, device_id={"tp": at_link[D_]}, device_id_type=MESH)
        pl.semaphore_wait(barrier, 4)

    @pl.when(is_c)
    def _():
        pl.semaphore_wait(barrier, 3)

    x_from = jnp.where(is_m, X_FROM["M"], X_FROM["C"])

    first_sum = jnp.where(is_m, min(k for k in sum_count if k < 100), min(k for k in sum_count if k >= 100) - 100)
    last_sum = jnp.where(is_m, max(LAST["M"]), max(LAST["C"]))

    def step(s, _):
        @pl.when(s == last_sum)
        def _():
            dx_term(select((role * 100 + s) * 10, sum_what), core)

        communicate(s)

        @pl.when(s == x_from)
        def _():
            finish_down()

        key = role * 100 + s
        n_tok = select(key, tok_count)

        @pl.when(n_tok > 0)
        def _():
            tok_in(select(key * 10, tok_what), 0, True)

        @pl.when(s == 0)
        def _():
            clear(0)
            clear(1)
            for load in loads:
                load.wait()

        def sums(k, _):
            reduce_one(select(key * 10 + k, sum_what))
            return 0

        def tokens(k, _):
            code, b = select(key * 10 + k, tok_what), k % 2

            @pl.when(k + 1 < n_tok)
            def _():
                tok_in(select(key * 10 + k + 1, tok_what), 1 - b, True)

            tok_in(code, b, False)

            @pl.when((code // 16) % 2 == DY)
            def _():
                work_dy(code, b)

            @pl.when(code // 16 == X)
            def _():
                work_x(code, b)

            @pl.when(code >= 32)
            def _():
                last_x(code, b)

            return 0

        lax.fori_loop(0, select(key, sum_count), sums, 0)
        lax.fori_loop(0, n_tok, tokens, 0)

        n_next = select(key + 1, sum_count)

        def partners(k, _):
            partner_one(select((key + 1) * 10 + k, sum_what), (k == 0) & (s + 1 == first_sum))
            return 0

        lax.fori_loop(0, n_next, partners, 0)

        return 0

    lax.fori_loop(0, STEPS, step, 0)

    def pieces_left(sem, n):
        some = full.at[0, pl.ds(0, n // 2), pl.ds(0, rows)]
        remote(some, some, sem, ag_recv.at[0, 0, 0], partner).wait_send()

    for r, here in enumerate((is_m, is_c)):

        @pl.when(here)
        def _(r=r):
            for link in (P_, D_, Y_):
                n = sum(k // 100 == r for k in send_what[link])
                if n:
                    pieces_left(ag_send.at[link], n)
                    for parity in range(2):
                        half_block = parts.at[link, 0, span(0)]
                        remote(out.at[link, parity], half_block, rs_send.at[link, parity], rs_recv.at[link, 0, 0], partner).wait_send()

    for array in (DY, X):
        pieces_left(w_send.at[array], 32 if array == DY else 30)
    last_to_partner().wait_send()
    term_to_partner(0).wait_send()


def finish(dx, wd, acc, d, rows_in, to_x, to_gate, to_up, to_down, done, d_sem, g_sem):
    depth, width = to_gate.shape
    tile, ni = 512, width // 128
    copies = []
    for i, (result, place) in enumerate(((dx, to_x), (wd, to_down))):
        n = result.shape[0] // 4
        for k in range(4):
            here = pl.ds(k * n, n)
            copies.append(pltpu.make_async_copy(result.at[here], place.at[here], d_sem.at[i, k]))
    for copy in copies:
        copy.start()

    def store(a, n):
        here = pl.ds(pl.multiple_of(n * tile, tile), tile)
        return pltpu.make_async_copy(done.at[a, here], (to_gate, to_up)[a].at[here], g_sem.at[a, n])

    def column(n, _):
        xt = rows_in[:, pl.ds(pl.multiple_of(n * tile, tile), tile)]
        new = lax.dot_general(xt, d[...], (((0,), (0,)), ((), ())), preferred_element_type=F32)
        for i in range(tile // 128):
            to = pl.ds(pl.multiple_of(n * tile + i * 128, 128), 128)
            for j in range(2 * ni):
                k = (n * (tile // 128) + i) * ni + j % ni
                one = acc[j // ni, k] + new[i * 128 : (i + 1) * 128, j * 128 : (j + 1) * 128]
                done[j // ni, to, j % ni * 128 : (j % ni + 1) * 128] = one.astype(BF16)
        for a in range(2):
            store(a, n).start()
        return 0

    lax.fori_loop(0, depth // tile, column, 0)
    for copy in copies:
        copy.wait()
    for n in range(depth // tile):
        for a in range(2):
            store(a, n).wait()


def solution(mesh):
    def step(x, dy, gate, up, w_gate, w_up, w_down):
        block, depth = dy.shape
        tokens, width = gate.shape
        rows, chips = block // 2, tokens // block // 2
        anywhere, inside = pl.BlockSpec(memory_space=pl.ANY), pl.BlockSpec(memory_space=pltpu.VMEM)
        dma, flops = pltpu.SemaphoreType.DMA, 12 * tokens * depth * width
        outs = pl.pallas_call(
            kernel,
            out_shape=[
                pltpu.VMEM((block, depth), BF16),
                pltpu.VMEM((width, depth), BF16),
                pltpu.VMEM((2, (depth // 128) * (width // 128), 128, 128), F32),
                pltpu.VMEM((rows, 2 * width), BF16),
                pltpu.VMEM((rows, depth), BF16),
                jax.ShapeDtypeStruct((2, 2 * chips, block, depth), BF16),
                jax.ShapeDtypeStruct((4, chips, block, depth), BF16),
            ],
            in_specs=[anywhere] * 7,
            out_specs=[inside] * 5 + [anywhere] * 2,
            scratch_shapes=[
                pltpu.VMEM((depth, 2 * width), BF16),
                pltpu.VMEM((2 * chips, 2 * rows, 2 * width), BF16),
                pltpu.VMEM((2, 2 * rows, depth), BF16),
                pltpu.VMEM((2, 2 * rows, width), BF16),
                pltpu.VMEM((2, 2 * rows, width), BF16),
                pltpu.VMEM((2 * rows, width), F32),
                pltpu.VMEM((rows, depth), F32),
                pltpu.VMEM((4, rows, depth), BF16),
                pltpu.VMEM((3, 2, rows, depth), BF16),
                pltpu.VMEM((rows, depth), BF16),
                dma((2, chips, 4)),
                dma((3,)),
                dma((2, chips, 4)),
                dma((2,)),
                dma((4, chips, 2)),
                dma((3, 2)),
                dma(()),
                dma(()),
                dma((3,)),
                dma((2, 2)),
                dma((2, 2)),
                dma((2, 2)),
                dma((4,)),
            ],
            compiler_params=pltpu.CompilerParams(collective_id=0, has_side_effects=True, vmem_limit_bytes=46900000),
            cost_estimate=pl.CostEstimate(flops=flops, bytes_accessed=12 * tokens * depth, transcendentals=tokens * width),
            name="mlp_backward",
        )(x, dy, gate, up, w_gate, w_up, w_down)
        return pl.pallas_call(
            finish,
            out_shape=[jax.ShapeDtypeStruct(a.shape, BF16) for a in (dy, w_gate, w_up, w_down)],
            in_specs=[inside] * 5,
            out_specs=[anywhere] * 4,
            scratch_shapes=[
                pltpu.VMEM((2, depth, width), BF16),
                dma((2, 4)),
                dma((2, depth // 512)),
            ],
            compiler_params=pltpu.CompilerParams(vmem_limit_bytes=2**24),
            name="finish",
        )(*outs[:5])

    rows_, cols_ = P(("dp", "tp"), None), P("dp", "tp")
    return jax.shard_map(
        step,
        mesh=mesh,
        in_specs=(rows_, rows_, cols_, cols_, P(None, "tp"), P(None, "tp"), P("tp", None)),
        out_specs=(rows_, cols_, cols_, rows_),
        check_vma=False,
    )
```

```python
import jax
import jax.numpy as jnp
from jax import lax
from jax.experimental import pallas as pl
from jax.experimental.pallas import tpu as pltpu
from jax.sharding import PartitionSpec as P

MESH = pl.DeviceIdType.MESH
F32, BF16 = jnp.float32, jnp.bfloat16

P_, D_, Y_, W_ = 0, 1, 2, 3
DY, X = 0, 1
ROLES = "MC"
LINKS = {"a": ("C", "C", Y_), "b": ("M", "C", P_), "c": ("C", "M", P_), "d": ("M", "M", D_), "e": ("M", "M", Y_)}

START = {
    "a": [
        "d00C0", "d00M0", "d00M1", "d01C1", "d01M1", "d01M0", "x00C1", "s10M2", "d01C0", "d00C1", "s10M0", "x00C0",
        "x01C1", "x00M0", "x00M1", "x01M1", "x01C0",
    ],
    "b": [
        "d00M0", "d00M1", "d01C1", "d01M1", "d01M0", "s10M2", "x01M1", "d01C0", "s10M0", "x00M1", "x01C0", "x01C1",
        "x00M0", "x01M0", "x11M0", "s00C1", "s00C0",
    ],
    "c": [
        "d00C1", "d00C0", "x00C1", "s10C0", "x00C0", "s01C1", "s11C1", "s01M0", "x10C7", "s11M0", "s01C0", "s11C0",
        "s10C1", "s11M1", "s00M0", "s01M1", "s10M3", "s00M1",
    ],
    "d": [
        "d00M0", "d00C1", "d00M1", "d00C0", "d10M1", "x00M1", "d10M0", "s01C1", "s11C1", "x00C0", "x00C1", "x10M1",
        "x00M0", "x10M0", "s01C0", "s01M0", "s01M1",
    ],
    "e": [
        "d00M1", "d00C1", "d01C1", "d00C0", "d01C0", "d00M0", "x00M0", "s10C0", "x00C6", "x00C0", "x00M1", "s11M0",
        "x01C0", "s11C0", "s10C1", "s11M1", "x01C1", "s10M3",
    ],
}
TOKENS = {
    "M": [
        "0d00M0", "1d00M1", "4d10M1", "4d00C1", "5d01M0", "6d01C1", "6d10C1", "7d00C0", "8d11C1", "8d01M1", "10d10C0", "10d01C0",
        "12d11C0", "12d11M1", "14d10M0", "16d11M0", "17x00M0", "17x00M1", "18x00C1", "18x00C0", "19x01M1", "19x10M0", "20x10C1", "21x10C0",
        "22x01C0", "23x10M1", "24x01C1", "26x11M1", "27x11C0", "28x01M0", "30x11M0", "35x11C1",
    ],
    "C": [
        "0d00C0", "1d00C1", "4d10C0", "4d00M0", "6d10M0", "6d00M1", "8d01C1", "8d10M1", "10d11C1", "10d01M1", "12d01M0", "12d11M1",
        "14d11M0", "18d01C0", "20d11C0", "22d10C1", "23x00C0", "23x00C1", "24x01M1", "24x10C1", "25x00M1", "25x01C0", "26x01C1", "26x10C0",
        "28x00M0", "28x11C1", "30x01M0", "30x10M0", "32x10M1", "32x11M0", "34x11M1", "36x11C0",
    ],
}
X_FROM = {"M": 17, "C": 23}
LAST = {"M": (33, 35), "C": (35, 33)}
STEPS = 37


def seen_by_receiver(unit, link):
    flip = {"0": "1", "1": "0"}
    if link == Y_:
        return flip[unit[0]] + unit[1:]
    return unit[0] + flip[unit[1]] + unit[2] if link == D_ else unit


def pack(unit):
    return int(unit[0]) + 2 * int(unit[1]) + 4 * (unit[2] == "M")


def select(key, table):
    out = jnp.int32(0)
    for k, v in table.items():
        out = jnp.where(key == k, jnp.int32(v), out)
    return out


def plan():
    send, recv = ({P_: {}, D_: {}, Y_: {}} for _ in range(2))
    sums, terms, sent = {"M": {}, "C": {}}, {}, {}
    for name, entries in START.items():
        sender, receiver, link = LINKS[name]
        t = 0
        for what in entries:
            if what[0] == "+":
                t += int(what)
                continue
            kind, unit, part = what[0], what[1:4], int(what[4])
            there = seen_by_receiver(unit, link)
            if kind == "s":
                h, part = (1, part - 1) if part > 1 else (part, 0)
                before = sent.setdefault((sender, link), [])
                sums[sender].setdefault(t, []).append((unit, h, part, link, len(before) % 2, before[-2] + 1 if len(before) > 1 else 0, 0))
                before.append(part)
                terms.setdefault((receiver, there, h), []).append((link, part))
                t += 1 if part == 2 else 2
                continue
            for p in (2 * part, 2 * part + 1) if part < 2 else (part - 4,):
                code = 1 + "dx".index(kind) + 16 * p
                send[link][ROLES.index(sender) * 100 + t] = code + 2 * pack(unit)
                recv[link][ROLES.index(receiver) * 100 + t + 2] = code + 2 * pack(there)
                t += 1
    for role in ROLES:
        for h in range(2):
            early = h == (LAST[role][1] >= LAST[role][0])
            sums[role].setdefault(LAST[role][h], []).insert(0, ("00" + role, h, 0, 3, 0, 0, early))
    sum_count, sum_what, tok_count, tok_what = {}, {}, {}, {}
    for r, role in enumerate(ROLES):
        met = set()
        for t, entries in sorted(sums[role].items()):
            sum_count[r * 100 + t] = len(entries)
            for k, (unit, h, part, link, parity, before, early) in enumerate(entries):
                mine = [(i, p) for i, p in terms.get((role, unit, h), []) if part in (0, p)]
                odd = [(i, p) for i, p in mine if p]
                code = pack(unit) + 8 * h + 16 * sum(1 << i for i, _ in mine) + 128 * link + 512 * parity + 1024 * before
                code += 4096 * early + 8192 * part + 2**17 * ((unit, h) in met)
                if odd:
                    code += 2**15 * (odd[0][1] + 0) + 2**18 * odd[0][0]
                met.add((unit, h))
                sum_what[(r * 100 + t) * 10 + k] = code
        for what in TOKENS[role]:
            t, kind, unit, h = int(what[:-5]), what[-5], what[-4:-1], int(what[-1])
            k = tok_count.get(r * 100 + t, 0)
            tok_count[r * 100 + t] = k + 1
            code = pack(unit) + 8 * h + 16 * "dx".index(kind)
            tok_what[(r * 100 + t) * 10 + k] = code + 32 * (what is TOKENS[role][-1])
    return send, recv, sum_count, sum_what, tok_count, tok_what, sent


def last_code(role):
    what = TOKENS[role][-1]
    return pack(what[-4:-1]) + 8 * int(what[-1])


def kernel(
    x, dy, gate, up, w_gate, w_up, w_down,
    dx, wd, acc, d_last, last_rows, full, parts,
    w, d, tok, gb, ub, dh, total, ext, out, outw,
    ag_recv, ag_send, w_recv, w_send, rs_recv, rs_send, p_send, l_send, l_sem, tok_sem, g_sem, u_sem, e_sem,
):
    block, depth = dy.shape
    width = gate.shape[1]
    rows, quarter, blocks = block // 2, block // 4, full.shape[1] // 2
    tile = 512
    nj, ni = depth // 128, width // 128
    own_in = {DY: dy, X: x}
    send_what, recv_what, sum_count, sum_what, tok_count, tok_what, sent = plan()

    tp = lax.axis_index("tp")
    core, chip = tp % 2, tp // 2
    y, z = chip // 4, chip % 4
    half = z // 2
    middle = ((z + 1) % 4) // 2
    is_m, is_c = middle == 1, middle == 0
    role = 1 - middle

    def chip_of(yy, hh, mm):
        return yy * 4 + mm + hh * (3 - 2 * mm)

    def chip_packed(code):
        ry, rh, mm = code % 2, (code // 2) % 2, (code // 4) % 2
        return chip_of(y + ry - 2 * y * ry, half + rh - 2 * half * rh, mm)

    partner = tp + 1 - 2 * core
    at_link = {
        P_: chip_of(y, half, 1 - middle) * 2 + core,
        D_: chip_of(y, 1 - half, middle) * 2 + core,
        Y_: chip_of(1 - y, half, middle) * 2 + core,
    }

    def span(h):
        return pl.ds(pl.multiple_of(h * rows, rows), rows)

    def quarter_at(p):
        return pl.ds(pl.multiple_of(p * quarter, quarter), quarter)

    def remote(src, dst, send, recv, to):
        return pltpu.make_async_remote_copy(
            src_ref=src, dst_ref=dst, send_sem=send, recv_sem=recv, device_id={"tp": to}, device_id_type=MESH
        )

    def by_rows(step, n_rows, fn, start=0):
        def body(i, _):
            fn(pl.ds(pl.multiple_of(i * step, step), step))
            return 0

        lax.fori_loop(start // step, n_rows // step, body, 0)

    cut = rows * 3 // 4 // 16 * 16
    part_rows = ((0, rows), (0, cut), (cut, rows - cut))

    def bounds(part):
        return jnp.where(part == 2, cut, 0), jnp.where(part == 1, cut, rows)

    def in_part(part, fn):
        for i in range(3):

            @pl.when(part == i)
            def _(i=i):
                fn(*part_rows[i])


    def on_link(link, code, src=None):
        code = code - 1
        array, c, p = code % 2, chip_packed(code // 2), code // 16
        piece = quarter_at(p)
        to = full.at[array, c * 2 + core, piece]
        return remote(to if src is None else src.at[piece], to, ag_send.at[link], ag_recv.at[array, c, p], at_link[link])

    def to_partner(array, c, p, src=None):
        piece = quarter_at(p)
        to = full.at[array, c * 2 + core, piece]
        return remote(to if src is None else src.at[piece], to, w_send.at[array], w_recv.at[array, c, p], partner)

    last = jnp.where(is_m, last_code("M"), last_code("C"))

    def last_to_partner():
        c, h = chip_packed(last), last // 8
        here = full.at[X, c * 2 + core, span(h)]
        return remote(here, last_rows, l_send, w_recv.at[X, c, 2 * h + 1], partner)

    def from_partner(array, c, h):
        for k in range(2):
            there = full.at[array, c * 2 + 1 - core, quarter_at(2 * h + k)]
            remote(there, there, p_send, w_recv.at[array, c, 2 * h + k], partner).wait_recv()

    def communicate(s):
        key = role * 100 + s
        come = {link: select(key, recv_what[link]) for link in (P_, D_, Y_)}
        for link, code in come.items():

            @pl.when(code > 0)
            def _(link=link, code=code):
                on_link(link, code).wait_recv()

        for link in (P_, D_, Y_):
            code = select(key, send_what[link])
            mine = chip_packed((code - 1) // 2) == chip

            @pl.when((code > 0) & jnp.logical_not(mine))
            def _(link=link, code=code):
                on_link(link, code).start()

            for array in (DY, X):

                @pl.when((code > 0) & mine & ((code - 1) % 2 == array))
                def _(link=link, code=code, array=array):
                    on_link(link, code, own_in[array]).start()

        for link, code in come.items():

            ends = ((code - 1) % 16 == X + 2 * (last % 8)) & ((code - 1) // 32 == last // 8)

            @pl.when((code > 0) & jnp.logical_not(ends))
            def _(code=code):
                to_partner((code - 1) % 2, chip_packed((code - 1) // 2), (code - 1) // 16).start()

            @pl.when(ends & ((code - 1) // 16 % 2 == 1))
            def _():
                last_to_partner().start()

        for array, when in ((DY, 0), (X, 2)):

            @pl.when(s == when)
            def _(array=array):
                for p in range(4):
                    to_partner(array, chip, p, own_in[array]).start()


    def dx_term(code, plane):
        index = chip_packed(code) * 2 + (code // 8) % 2
        here = span(plane)

        def column(n, _):
            cols = pl.ds(pl.multiple_of(n * tile, tile), tile)
            total[:, cols] = lax.dot_general(
                d[index, here, :], w[cols, :], (((1,), (1,)), ((), ())), preferred_element_type=F32
            )
            return 0

        lax.fori_loop(0, depth // tile, column, 0)

    def reduce_one(code):
        c, h = chip_packed(code), (code // 8) % 2
        mask, link, parity, before = (code // 16) % 8, (code // 128) % 4, (code // 512) % 2, (code // 1024) % 4
        early, part, again = (code // 4096) % 2 == 1, (code // 8192) % 4, (code // 2**17) % 2 == 1
        odd_part, odd = (code // 2**15) % 4, code // 2**18
        bits = {P_: mask % 2 == 1, D_: (mask // 2) % 2 == 1, Y_: mask // 4 == 1}
        part_of = {P_: jnp.where(odd == P_, odd_part, 0), D_: jnp.int32(0), Y_: jnp.where(odd == Y_, odd_part, 0), W_: jnp.int32(0)}

        def there(lo, n):
            return pl.ds(pl.multiple_of(h * rows + lo, 16), n)

        def term_in(kind, lo, n):
            return pltpu.make_async_copy(parts.at[kind, c, there(lo, n)], ext.at[kind, pl.ds(lo, n)], e_sem.at[kind])

        def with_term(kind, fn):
            if kind in (P_, Y_):
                in_part(part_of[kind], fn)
            else:
                fn(0, rows)

        def arrived(kind):
            def wait(lo, n):
                here = ext.at[kind, pl.ds(lo, n)]
                remote(here, parts.at[kind, c, there(lo, n)], p_send, rs_recv.at[kind, c, h], partner).wait_recv()

            with_term(kind, wait)

        def fetch(kind):
            with_term(kind, lambda lo, n: term_in(kind, lo, n).start())

        def send_term(to, lo, n):
            return remote(
                out.at[link, parity, pl.ds(lo, n)], parts.at[link, c, there(lo, n)], rs_send.at[link, parity],
                rs_recv.at[link, c, h], to,
            )

        @pl.when(jnp.logical_not(again))
        def _():
            arrived(W_)

        fetch(W_)
        for kind in (P_, D_, Y_):

            @pl.when(bits[kind] & (link != 3))
            def _(kind=kind):
                arrived(kind)
                fetch(kind)

        @pl.when(jnp.logical_not(early))
        def _():
            dx_term(code, core)

        for kind in (P_, D_, Y_):

            @pl.when(bits[kind] & (link == 3))
            def _(kind=kind):
                arrived(kind)
                fetch(kind)

        for kind in (P_, D_, Y_):

            @pl.when(bits[kind])
            def _(kind=kind):
                with_term(kind, lambda lo, n: term_in(kind, lo, n).wait())

                def add(r):
                    total[r, :] += ext[kind, r, :].astype(F32)

                lo, hi = bounds(part_of[kind])
                by_rows(16, hi, add, lo)

        term_in(W_, 0, rows).wait()

        @pl.when(link == 3)
        def _():
            def finish(r):
                to = pl.ds(pl.multiple_of(h * rows + r.start, 16), 16)
                dx[to, :] = (total[r, :] + ext[W_, r, :].astype(F32)).astype(BF16)

            by_rows(16, rows, finish)

        @pl.when(link != 3)
        def _():
            to = jnp.where(link == P_, at_link[P_], jnp.where(link == D_, at_link[D_], at_link[Y_]))
            in_part(before - 1, lambda lo, n: send_term(to, lo, n).wait_send())

            def round_(r):
                out[link, parity, r, :] = (total[r, :] + ext[W_, r, :].astype(F32)).astype(BF16)

            lo, hi = bounds(part)
            by_rows(16, hi, round_, lo)
            in_part(part, lambda lo, n: send_term(to, lo, n).start())

    def term_to_partner(code):
        c, h = chip_packed(code), (code // 8) % 2
        return remote(outw, parts.at[W_, c, span(h)], p_send, rs_recv.at[W_, c, h], partner)

    def partner_one(code, first):
        dx_term(code, 1 - core)

        @pl.when(jnp.logical_not(first))
        def _():
            term_to_partner(code).wait_send()

        def round_(r):
            outw[r, :] = total[r, :].astype(BF16)

        by_rows(16, rows, round_)
        term_to_partner(code).start()


    def last_in(code, b):
        c, h = chip_packed(code), (code // 8) % 2
        src = full.at[X, c * 2 + core, span(h)]
        return pltpu.make_async_copy(src, tok.at[b, span(core)], tok_sem.at[b, core])

    def tok_in(code, b, start):
        @pl.when(code < 32)
        def _():
            pair_in(code, b, start)

        @pl.when(code >= 32)
        def _():
            copy = last_in(code, b)
            copy.start() if start else copy.wait()

    def pair_in(code, b, start):
        c, h, array = chip_packed(code), (code // 8) % 2, (code // 16) % 2
        mine = c == chip
        for plane in range(2):
            blk = c * 2 + plane
            here = slice(plane * rows, (plane + 1) * rows)
            dst, src, sem = tok.at[b, here], full.at[array, blk, span(h)], tok_sem.at[b, plane]
            spread = pl.ds(pl.multiple_of(blk * block + h * rows, rows), rows)
            pair = (
                pltpu.make_async_copy(gate.at[spread], gb.at[b, here], g_sem.at[b, plane]),
                pltpu.make_async_copy(up.at[spread], ub.at[b, here], u_sem.at[b, plane]),
            )
            if not start:
                pltpu.make_async_copy(src, dst, sem).wait()

                @pl.when(array == DY)
                def _(pair=pair):
                    for copy in pair:
                        copy.wait()

                continue

            @pl.when(array == DY)
            def _(pair=pair):
                for copy in pair:
                    copy.start()

            local = mine & (core == plane)

            @pl.when(core != plane)
            def _():
                from_partner(array, c, h)

            @pl.when(jnp.logical_not(local))
            def _(src=src, dst=dst, sem=sem):
                pltpu.make_async_copy(src, dst, sem).start()

            for a in (DY, X):

                @pl.when(local & (array == a))
                def _(a=a, dst=dst, sem=sem):
                    pltpu.make_async_copy(own_in[a].at[span(h)], dst, sem).start()

    def work_dy(code, b):
        index = chip_packed(code) * 2 + (code // 8) % 2
        dh[...] = lax.dot_general(tok[b], wd[...], (((1,), (1,)), ((), ())), preferred_element_type=F32)

        def pointwise(r):
            g, u, dhid = gb[b, r, :].astype(F32), ub[b, r, :].astype(F32), dh[r, :]
            g2 = g * g
            t = jnp.tanh(g * (0.7978845608028654 + (0.7978845608028654 * 0.044715) * g2))
            cdf = 0.5 + 0.5 * t
            act = g * cdf
            slope = cdf + (0.5 * g) * (1.0 - t * t) * (0.7978845608028654 + (3 * 0.7978845608028654 * 0.044715) * g2)
            d[index, r, width:] = (dhid * act).astype(BF16)
            d[index, r, :width] = ((dhid * u) * slope).astype(BF16)
            gb[b, r, :] = (act * u).astype(BF16)

        by_rows(16, 2 * rows, pointwise)

        def column(n, _):
            cols = pl.ds(pl.multiple_of(n * tile, tile), tile)
            new = lax.dot_general(gb[b], tok[b, :, cols], (((0,), (0,)), ((), ())), preferred_element_type=F32)
            for i in range(ni):
                for j in range(tile // 128):
                    k = i * nj + n * (tile // 128) + j
                    acc[0, k] += new[i * 128 : (i + 1) * 128, j * 128 : (j + 1) * 128]
            return 0

        lax.fori_loop(0, depth // tile, column, 0)

    def x_columns(index, b, here):
        def column(n, _):
            cols = pl.ds(pl.multiple_of(n * tile, tile), tile)
            xt = tok[b, here, cols]
            new = lax.dot_general(xt, d[index, here, :], (((0,), (0,)), ((), ())), preferred_element_type=F32)
            for i in range(tile // 128):
                for j in range(2 * ni):
                    k = (n * (tile // 128) + i) * ni + j % ni
                    acc[j // ni, k] += new[i * 128 : (i + 1) * 128, j * 128 : (j + 1) * 128]
            return 0

        lax.fori_loop(0, depth // tile, column, 0)

    def work_x(code, b):
        x_columns(chip_packed(code) * 2 + (code // 8) % 2, b, slice(None))

    def last_x(code, b):
        c, h = chip_packed(code), (code // 8) % 2
        x_columns(c * 2 + h, b, span(core))

        def keep(r):
            there = pl.ds(pl.multiple_of((1 - core) * rows + r.start, 16), 16)
            d_last[r, :] = d[c * 2 + h, there, :]

        by_rows(16, rows, keep)
        last_to_partner().wait_recv()

    def finish_down():
        for i in range(ni):
            for j in range(nj):
                wd[i * 128 : (i + 1) * 128, j * 128 : (j + 1) * 128] = acc[0, i * nj + j].astype(BF16)
                acc[0, i * nj + j] = jnp.zeros((128, 128), F32)

    def clear(i):
        def body(k, _):
            acc[i, k] = jnp.zeros((128, 128), F32)
            return 0

        lax.fori_loop(0, ni * nj, body, 0)


    pairs = (w_down, wd), (w_gate, w.at[:, :width]), (w_up, w.at[:, width:])
    loads = [pltpu.make_async_copy(s, d, l_sem.at[i]) for i, (s, d) in enumerate(pairs)]
    for load in loads:
        load.start()

    barrier = pltpu.get_barrier_semaphore()
    for to in (at_link[P_], at_link[Y_], partner):
        pl.semaphore_signal(barrier, inc=1, device_id={"tp": to}, device_id_type=MESH)

    @pl.when(is_m)
    def _():
        pl.semaphore_signal(barrier, inc=1, device_id={"tp": at_link[D_]}, device_id_type=MESH)
        pl.semaphore_wait(barrier, 4)

    @pl.when(is_c)
    def _():
        pl.semaphore_wait(barrier, 3)

    x_from = jnp.where(is_m, X_FROM["M"], X_FROM["C"])

    first_sum = jnp.where(is_m, min(k for k in sum_count if k < 100), min(k for k in sum_count if k >= 100) - 100)
    last_sum = jnp.where(is_m, max(LAST["M"]), max(LAST["C"]))

    def step(s, _):
        @pl.when(s == last_sum)
        def _():
            dx_term(select((role * 100 + s) * 10, sum_what), core)

        communicate(s)

        @pl.when(s == x_from)
        def _():
            finish_down()

        key = role * 100 + s
        n_tok = select(key, tok_count)

        @pl.when(n_tok > 0)
        def _():
            tok_in(select(key * 10, tok_what), 0, True)

        @pl.when(s == 0)
        def _():
            clear(0)
            clear(1)
            for load in loads:
                load.wait()

        def sums(k, _):
            reduce_one(select(key * 10 + k, sum_what))
            return 0

        def tokens(k, _):
            code, b = select(key * 10 + k, tok_what), k % 2

            @pl.when(k + 1 < n_tok)
            def _():
                tok_in(select(key * 10 + k + 1, tok_what), 1 - b, True)

            tok_in(code, b, False)

            @pl.when((code // 16) % 2 == DY)
            def _():
                work_dy(code, b)

            @pl.when(code // 16 == X)
            def _():
                work_x(code, b)

            @pl.when(code >= 32)
            def _():
                last_x(code, b)

            return 0

        n_sum, tokens_first = select(key, sum_count), is_m & (s == last_sum)

        def phase(p, _):
            now = (p == 0) != tokens_first
            lax.fori_loop(0, jnp.where(now, n_sum, 0), sums, 0)
            lax.fori_loop(0, jnp.where(now, 0, n_tok), tokens, 0)
            return 0

        lax.fori_loop(0, 2, phase, 0)

        n_next = select(key + 1, sum_count)

        def partners(k, _):
            code = select((key + 1) * 10 + k, sum_what)

            @pl.when((code // 2**17) % 2 == 0)
            def _():
                partner_one(code, (k == 0) & (s + 1 == first_sum))

            return 0

        lax.fori_loop(0, n_next, partners, 0)

        return 0

    lax.fori_loop(0, STEPS, step, 0)

    def pieces_left(sem, n):
        sizes = [(b, n * quarter // b) for b in range(1, 2 * blocks) if n * quarter % b == 0 and n * quarter // b <= block]
        b, m = min(sizes, key=lambda size: size[1] % 8 > 0)
        some = full.at[0, pl.ds(0, b), pl.ds(0, m)]
        remote(some, some, sem, ag_recv.at[0, 0, 0], partner).wait_send()

    for r, here in enumerate((is_m, is_c)):

        @pl.when(here)
        def _(r=r):
            for link in (P_, D_, Y_):
                n = sum(k // 100 == r for k in send_what[link])
                if n:
                    pieces_left(ag_send.at[link], n)
                    parts_sent = sent[ROLES[r], link]
                    for i in (len(parts_sent) - 2, len(parts_sent) - 1):
                        lo, m = part_rows[parts_sent[i]]
                        here, there = out.at[link, i % 2, pl.ds(lo, m)], parts.at[link, 0, pl.ds(lo, m)]
                        remote(here, there, rs_send.at[link, i % 2], rs_recv.at[link, 0, 0], partner).wait_send()

    for array in (DY, X):
        pieces_left(w_send.at[array], 32 if array == DY else 30)
    last_to_partner().wait_send()
    term_to_partner(0).wait_send()


def finish(dx, wd, acc, d, rows_in, to_x, to_gate, to_up, to_down, done, d_sem, g_sem):
    depth, width = to_gate.shape
    tile, ni = 512, width // 128
    copies = []
    for i, (result, place) in enumerate(((dx, to_x), (wd, to_down))):
        n = result.shape[0] // 4
        for k in range(4):
            here = pl.ds(k * n, n)
            copies.append(pltpu.make_async_copy(result.at[here], place.at[here], d_sem.at[i, k]))
    for copy in copies:
        copy.start()

    def store(a, n):
        here = pl.ds(pl.multiple_of(n * tile, tile), tile)
        return pltpu.make_async_copy(done.at[a, here], (to_gate, to_up)[a].at[here], g_sem.at[a, n])

    def column(n, _):
        xt = rows_in[:, pl.ds(pl.multiple_of(n * tile, tile), tile)]
        new = lax.dot_general(xt, d[...], (((0,), (0,)), ((), ())), preferred_element_type=F32)
        for i in range(tile // 128):
            to = pl.ds(pl.multiple_of(n * tile + i * 128, 128), 128)
            for j in range(2 * ni):
                k = (n * (tile // 128) + i) * ni + j % ni
                one = acc[j // ni, k] + new[i * 128 : (i + 1) * 128, j * 128 : (j + 1) * 128]
                done[j // ni, to, j % ni * 128 : (j % ni + 1) * 128] = one.astype(BF16)
        for a in range(2):
            store(a, n).start()
        return 0

    lax.fori_loop(0, depth // tile, column, 0)
    for copy in copies:
        copy.wait()
    for n in range(depth // tile):
        for a in range(2):
            store(a, n).wait()


def solution(mesh):
    def step(x, dy, gate, up, w_gate, w_up, w_down):
        block, depth = dy.shape
        tokens, width = gate.shape
        rows, chips = block // 2, tokens // block // 2
        anywhere, inside = pl.BlockSpec(memory_space=pl.ANY), pl.BlockSpec(memory_space=pltpu.VMEM)
        dma, flops = pltpu.SemaphoreType.DMA, 12 * tokens * depth * width
        outs = pl.pallas_call(
            kernel,
            out_shape=[
                pltpu.VMEM((block, depth), BF16),
                pltpu.VMEM((width, depth), BF16),
                pltpu.VMEM((2, (depth // 128) * (width // 128), 128, 128), F32),
                pltpu.VMEM((rows, 2 * width), BF16),
                pltpu.VMEM((rows, depth), BF16),
                jax.ShapeDtypeStruct((2, 2 * chips, block, depth), BF16),
                jax.ShapeDtypeStruct((4, chips, block, depth), BF16),
            ],
            in_specs=[anywhere] * 7,
            out_specs=[inside] * 5 + [anywhere] * 2,
            scratch_shapes=[
                pltpu.VMEM((depth, 2 * width), BF16),
                pltpu.VMEM((2 * chips, 2 * rows, 2 * width), BF16),
                pltpu.VMEM((2, 2 * rows, depth), BF16),
                pltpu.VMEM((2, 2 * rows, width), BF16),
                pltpu.VMEM((2, 2 * rows, width), BF16),
                pltpu.VMEM((2 * rows, width), F32),
                pltpu.VMEM((rows, depth), F32),
                pltpu.VMEM((4, rows, depth), BF16),
                pltpu.VMEM((3, 2, rows, depth), BF16),
                pltpu.VMEM((rows, depth), BF16),
                dma((2, chips, 4)),
                dma((3,)),
                dma((2, chips, 4)),
                dma((2,)),
                dma((4, chips, 2)),
                dma((3, 2)),
                dma(()),
                dma(()),
                dma((3,)),
                dma((2, 2)),
                dma((2, 2)),
                dma((2, 2)),
                dma((4,)),
            ],
            compiler_params=pltpu.CompilerParams(collective_id=0, has_side_effects=True, vmem_limit_bytes=46900000),
            cost_estimate=pl.CostEstimate(flops=flops, bytes_accessed=12 * tokens * depth, transcendentals=tokens * width),
            name="mlp_backward",
        )(x, dy, gate, up, w_gate, w_up, w_down)
        return pl.pallas_call(
            finish,
            out_shape=[jax.ShapeDtypeStruct(a.shape, BF16) for a in (dy, w_gate, w_up, w_down)],
            in_specs=[inside] * 5,
            out_specs=[anywhere] * 4,
            scratch_shapes=[
                pltpu.VMEM((2, depth, width), BF16),
                dma((2, 4)),
                dma((2, depth // 512)),
            ],
            compiler_params=pltpu.CompilerParams(vmem_limit_bytes=2**24),
            name="finish",
        )(*outs[:5])

    rows_, cols_ = P(("dp", "tp"), None), P("dp", "tp")
    return jax.shard_map(
        step,
        mesh=mesh,
        in_specs=(rows_, rows_, cols_, cols_, P(None, "tp"), P(None, "tp"), P("tp", None)),
        out_specs=(rows_, cols_, cols_, rows_),
        check_vma=False,
    )
```

```python
import jax
import jax.numpy as jnp
from jax import lax
from jax.experimental import pallas as pl
from jax.experimental.pallas import tpu as pltpu
from jax.sharding import PartitionSpec as P

MESH = pl.DeviceIdType.MESH
F32, BF16 = jnp.float32, jnp.bfloat16

LANES = 128
ROOT = 0.7978845608028654
BY_ROWS, BY_COLUMNS = (((0,), (0,)), ((), ())), (((1,), (1,)), ((), ()))
P_, D_, Y_, W_ = 0, 1, 2, 3
DY, X = 0, 1
ROLES = "MC"
LINKS = {"a": ("C", "C", Y_), "b": ("M", "C", P_), "c": ("C", "M", P_), "d": ("M", "M", D_), "e": ("M", "M", Y_)}

START = {
    "a": [
        "d00C1", "d00M0", "d00C0", "d01C0", "d01M1", "d00M1", "d01C1", "s10M0", "d01M0", "s10M2", "x00M1", "x00C0",
        "x00C1", "x01C0", "x01M0", "x01M1", "x00M0",
    ],
    "b": [
        "d00M0", "d00M1", "d01C0", "d01M1", "s10M0", "d01C1", "s10M2", "d01M0", "x01M0", "x00M1", "x00M0", "x01C1",
        "x01C0", "x11C1", "x01M1", "s00C0", "s00C1",
    ],
    "c": [
        "d00C0", "x00C0", "d00C1", "s10C1", "x00C1", "s01C0", "s11C0", "s10C0", "s01C1", "s11C1", "s01M1", "s10M3",
        "s11M1", "s11M0", "x10C7", "s01M0", "s00M0", "s00M1",
    ],
    "d": [
        "d00M1", "d00C0", "d10M0", "d00C1", "d10M1", "x00M0", "d00M0", "s01C0", "x00C0", "x00C1", "x10M0", "s11C0",
        "s01C1", "x00M1", "x10M1", "s01M1", "s01M0",
    ],
    "e": [
        "x00M1", "d00M0", "d00C0", "d00M1", "d00C1", "d01C0", "d01C1", "s10C1", "x00C6", "x00M0", "x01C0", "s11C1",
        "x01C1", "s10C0", "s11M1", "s11M0", "x00C0", "s10M3",
    ],
}
TOKENS = {
    "M": [
        "0d00M0", "1d00M1", "4d00C0", "4d01M1", "6d10M0", "6d01C0", "8d10C0", "8d11M0", "9d00C1", "10d10M1", "10d01C1", "12d10C1",
        "12d11M1", "14d11C0", "16d11C1", "16d01M0", "17x00M0", "17x00M1", "18x10M1", "18x00C0", "19x00C1", "19x01M0", "20x01C0", "21x10M0",
        "22x01C1", "23x11C0", "24x11M0", "27x11C1", "30x01M1", "30x10C1", "32x11M1", "35x10C0",
    ],
    "C": [
        "0d00C0", "1d00C1", "4d10C1", "4d00M0", "6d10M0", "6d00M1", "8d01C0", "8d10C0", "10d11C0", "10d01M1", "12d11M1", "14d01C1",
        "14d10M1", "16d11C1", "18d01M0", "20d11M0", "21x00C0", "21x00C1", "22x01M0", "22x00M1", "24x00M0", "24x10M1", "26x01C1", "26x10C0",
        "28x01C0", "28x10C1", "30x11C0", "30x11C1", "32x01M1", "32x11M0", "34x11M1", "36x10M0",
    ],
}
X_FROM = {"M": 17, "C": 21}
LAST = {"M": (35, 35), "C": (33, 35)}
STEPS = 37


def seen_by_receiver(unit, link):
    flip = {"0": "1", "1": "0"}
    if link == Y_:
        return flip[unit[0]] + unit[1:]
    return unit[0] + flip[unit[1]] + unit[2] if link == D_ else unit


def pack(unit):
    return int(unit[0]) + 2 * int(unit[1]) + 4 * (unit[2] == "M")


def lanes(i):
    return slice(i * LANES, (i + 1) * LANES)


def half_in(code):
    return (code // 8) % 2


def select(key, table):
    out = jnp.int32(0)
    for k, v in table.items():
        out = jnp.where(key == k, jnp.int32(v), out)
    return out


def plan():
    send, recv = ({P_: {}, D_: {}, Y_: {}} for _ in range(2))
    sums, terms, sent = {"M": {}, "C": {}}, {}, {}
    for name, entries in START.items():
        sender, receiver, link = LINKS[name]
        t = 0
        for what in entries:
            if what[0] == "+":
                t += int(what)
                continue
            kind, unit, part = what[0], what[1:4], int(what[4])
            there = seen_by_receiver(unit, link)
            if kind == "s":
                h, part = (1, part - 1) if part > 1 else (part, 0)
                before = sent.setdefault((sender, link), [])
                sums[sender].setdefault(t, []).append((unit, h, part, link, len(before) % 2, before[-2] + 1 if len(before) > 1 else 0, 0))
                before.append(part)
                terms.setdefault((receiver, there, h), []).append((link, part))
                t += 1 if part == 2 else 2
                continue
            for p in (2 * part, 2 * part + 1) if part < 2 else (part - 4,):
                code = 1 + "dx".index(kind) + 16 * p
                send[link][ROLES.index(sender) * 100 + t] = code + 2 * pack(unit)
                recv[link][ROLES.index(receiver) * 100 + t + 2] = code + 2 * pack(there)
                t += 1
    for role in ROLES:
        for h in range(2):
            early = h == (LAST[role][1] >= LAST[role][0])
            sums[role].setdefault(LAST[role][h], []).insert(0, ("00" + role, h, 0, 3, 0, 0, early))
    sum_count, sum_what, tok_count, tok_what = {}, {}, {}, {}
    for r, role in enumerate(ROLES):
        met = set()
        for t, entries in sorted(sums[role].items()):
            sum_count[r * 100 + t] = len(entries)
            for k, (unit, h, part, link, parity, before, early) in enumerate(entries):
                mine = [(i, p) for i, p in terms.get((role, unit, h), []) if part in (0, p)]
                odd = [(i, p) for i, p in mine if p]
                code = pack(unit) + 8 * h + 16 * sum(1 << i for i, _ in mine) + 128 * link + 512 * parity + 1024 * before
                code += 4096 * early + 8192 * part + 2**17 * ((unit, h) in met)
                if odd:
                    code += 2**15 * (odd[0][1] + 0) + 2**18 * odd[0][0]
                met.add((unit, h))
                sum_what[(r * 100 + t) * 10 + k] = code
        for what in TOKENS[role]:
            t, kind, unit, h = int(what[:-5]), what[-5], what[-4:-1], int(what[-1])
            k = tok_count.get(r * 100 + t, 0)
            tok_count[r * 100 + t] = k + 1
            code = pack(unit) + 8 * h + 16 * "dx".index(kind)
            tok_what[(r * 100 + t) * 10 + k] = code + 32 * (what is TOKENS[role][-1])
    return send, recv, sum_count, sum_what, tok_count, tok_what, sent


def last_code(role):
    what = TOKENS[role][-1]
    return pack(what[-4:-1]) + 8 * int(what[-1])


def kernel(
    x, dy, gate, up, w_gate, w_up, w_down,
    dx, wd, acc, d_last, last_rows, full, parts,
    w, d, tok, gb, ub, dh, total, ext, out, outw,
    ag_recv, ag_send, w_recv, w_send, rs_recv, rs_send, p_send, l_send, l_sem, tok_sem, g_sem, u_sem, e_sem,
):
    block, depth = dy.shape
    width = gate.shape[1]
    rows, quarter, blocks = block // 2, block // 4, full.shape[1] // 2
    tile = 512
    nj, ni = depth // LANES, width // LANES
    own_in = {DY: dy, X: x}
    send_what, recv_what, sum_count, sum_what, tok_count, tok_what, sent = plan()

    tp = lax.axis_index("tp")
    core, chip = tp % 2, tp // 2
    y, z = chip // 4, chip % 4
    half = z // 2
    middle = ((z + 1) % 4) // 2
    is_m, is_c = middle == 1, middle == 0
    role = 1 - middle

    def chip_of(yy, hh, mm):
        return yy * 4 + mm + hh * (3 - 2 * mm)

    def chip_packed(code):
        ry, rh, mm = code % 2, (code // 2) % 2, (code // 4) % 2
        return chip_of(y + ry - 2 * y * ry, half + rh - 2 * half * rh, mm)

    partner = tp + 1 - 2 * core
    at_link = {
        P_: chip_of(y, half, 1 - middle) * 2 + core,
        D_: chip_of(y, 1 - half, middle) * 2 + core,
        Y_: chip_of(1 - y, half, middle) * 2 + core,
    }

    def span(h):
        return pl.ds(pl.multiple_of(h * rows, rows), rows)

    def quarter_at(p):
        return pl.ds(pl.multiple_of(p * quarter, quarter), quarter)

    def remote(src, dst, send, recv, to):
        return pltpu.make_async_remote_copy(
            src_ref=src, dst_ref=dst, send_sem=send, recv_sem=recv, device_id={"tp": to}, device_id_type=MESH
        )

    def by_rows(step, n_rows, fn, start=0):
        def body(i, _):
            fn(pl.ds(pl.multiple_of(i * step, step), step))
            return 0

        lax.fori_loop(start // step, n_rows // step, body, 0)

    cut = rows * 3 // 4 // 16 * 16
    part_rows = ((0, rows), (0, cut), (cut, rows - cut))

    def bounds(part):
        return jnp.where(part == 2, cut, 0), jnp.where(part == 1, cut, rows)

    def in_part(part, fn):
        for i in range(3):

            @pl.when(part == i)
            def _(i=i):
                fn(*part_rows[i])


    def on_link(link, code, src=None):
        code = code - 1
        array, c, p = code % 2, chip_packed(code // 2), code // 16
        piece = quarter_at(p)
        to = full.at[array, c * 2 + core, piece]
        return remote(to if src is None else src.at[piece], to, ag_send.at[link], ag_recv.at[array, c, p], at_link[link])

    def to_partner(array, c, p, src=None):
        piece = quarter_at(p)
        to = full.at[array, c * 2 + core, piece]
        return remote(to if src is None else src.at[piece], to, w_send.at[array], w_recv.at[array, c, p], partner)

    last = jnp.where(is_m, last_code("M"), last_code("C"))

    def last_to_partner():
        c, h = chip_packed(last), last // 8
        here = full.at[X, c * 2 + core, span(h)]
        return remote(here, last_rows, l_send, w_recv.at[X, c, 2 * h + 1], partner)

    def from_partner(array, c, h):
        for k in range(2):
            there = full.at[array, c * 2 + 1 - core, quarter_at(2 * h + k)]
            remote(there, there, p_send, w_recv.at[array, c, 2 * h + k], partner).wait_recv()

    def communicate(s):
        key = role * 100 + s
        come = {link: select(key, recv_what[link]) for link in (P_, D_, Y_)}
        for link, code in come.items():

            @pl.when(code > 0)
            def _(link=link, code=code):
                on_link(link, code).wait_recv()

        for link in (P_, D_, Y_):
            code = select(key, send_what[link])
            mine = chip_packed((code - 1) // 2) == chip

            @pl.when((code > 0) & jnp.logical_not(mine))
            def _(link=link, code=code):
                on_link(link, code).start()

            for array in (DY, X):

                @pl.when((code > 0) & mine & ((code - 1) % 2 == array))
                def _(link=link, code=code, array=array):
                    on_link(link, code, own_in[array]).start()

        for link, code in come.items():

            ends = ((code - 1) % 16 == X + 2 * (last % 8)) & ((code - 1) // 32 == last // 8)

            @pl.when((code > 0) & jnp.logical_not(ends))
            def _(code=code):
                to_partner((code - 1) % 2, chip_packed((code - 1) // 2), (code - 1) // 16).start()

            @pl.when(ends & ((code - 1) // 16 % 2 == 1))
            def _():
                last_to_partner().start()

        for array, when in ((DY, 0), (X, 2)):

            @pl.when(s == when)
            def _(array=array):
                for p in range(4):
                    to_partner(array, chip, p, own_in[array]).start()


    def dx_term(code, plane):
        index = chip_packed(code) * 2 + half_in(code)
        here = span(plane)

        def column(n, _):
            cols = pl.ds(pl.multiple_of(n * tile, tile), tile)
            total[:, cols] = lax.dot_general(
                d[index, here, :], w[cols, :], BY_COLUMNS, preferred_element_type=F32
            )
            return 0

        lax.fori_loop(0, depth // tile, column, 0)

    def reduce_one(code):
        c, h = chip_packed(code), half_in(code)
        mask, link, parity, before = (code // 16) % 8, (code // 128) % 4, (code // 512) % 2, (code // 1024) % 4
        early, part, again = (code // 4096) % 2 == 1, (code // 8192) % 4, (code // 2**17) % 2 == 1
        odd_part, odd = (code // 2**15) % 4, code // 2**18
        bits = {P_: mask % 2 == 1, D_: (mask // 2) % 2 == 1, Y_: mask // 4 == 1}
        part_of = {P_: jnp.where(odd == P_, odd_part, 0), D_: jnp.int32(0), Y_: jnp.where(odd == Y_, odd_part, 0), W_: jnp.int32(0)}

        def there(lo, n):
            return pl.ds(pl.multiple_of(h * rows + lo, 16), n)

        def term_in(kind, lo, n):
            return pltpu.make_async_copy(parts.at[kind, c, there(lo, n)], ext.at[kind, pl.ds(lo, n)], e_sem.at[kind])

        def with_term(kind, fn):
            if kind in (P_, Y_):
                in_part(part_of[kind], fn)
            else:
                fn(0, rows)

        def arrived(kind):
            def wait(lo, n):
                here = ext.at[kind, pl.ds(lo, n)]
                remote(here, parts.at[kind, c, there(lo, n)], p_send, rs_recv.at[kind, c, h], partner).wait_recv()

            with_term(kind, wait)

        def fetch(kind):
            with_term(kind, lambda lo, n: term_in(kind, lo, n).start())

        def send_term(to, lo, n):
            return remote(
                out.at[link, parity, pl.ds(lo, n)], parts.at[link, c, there(lo, n)], rs_send.at[link, parity],
                rs_recv.at[link, c, h], to,
            )

        @pl.when(jnp.logical_not(again))
        def _():
            arrived(W_)

        fetch(W_)
        for kind in (P_, D_, Y_):

            @pl.when(bits[kind] & (link != 3))
            def _(kind=kind):
                arrived(kind)
                fetch(kind)

        @pl.when(jnp.logical_not(early))
        def _():
            dx_term(code, core)

        for kind in (P_, D_, Y_):

            @pl.when(bits[kind] & (link == 3))
            def _(kind=kind):
                arrived(kind)
                fetch(kind)

        for kind in (P_, D_, Y_):

            @pl.when(bits[kind])
            def _(kind=kind):
                with_term(kind, lambda lo, n: term_in(kind, lo, n).wait())

                def add(r):
                    total[r, :] += ext[kind, r, :].astype(F32)

                lo, hi = bounds(part_of[kind])
                by_rows(16, hi, add, lo)

        term_in(W_, 0, rows).wait()

        @pl.when(link == 3)
        def _():
            def finish(r):
                to = pl.ds(pl.multiple_of(h * rows + r.start, 16), 16)
                dx[to, :] = (total[r, :] + ext[W_, r, :].astype(F32)).astype(BF16)

            by_rows(16, rows, finish)

        @pl.when(link != 3)
        def _():
            to = jnp.where(link == P_, at_link[P_], jnp.where(link == D_, at_link[D_], at_link[Y_]))
            in_part(before - 1, lambda lo, n: send_term(to, lo, n).wait_send())

            def round_(r):
                out[link, parity, r, :] = (total[r, :] + ext[W_, r, :].astype(F32)).astype(BF16)

            lo, hi = bounds(part)
            by_rows(16, hi, round_, lo)
            in_part(part, lambda lo, n: send_term(to, lo, n).start())

    def term_to_partner(code):
        c, h = chip_packed(code), half_in(code)
        return remote(outw, parts.at[W_, c, span(h)], p_send, rs_recv.at[W_, c, h], partner)

    def partner_one(code, first):
        dx_term(code, 1 - core)

        @pl.when(jnp.logical_not(first))
        def _():
            term_to_partner(code).wait_send()

        def round_(r):
            outw[r, :] = total[r, :].astype(BF16)

        by_rows(16, rows, round_)
        term_to_partner(code).start()


    def tok_in(code, b, start):
        @pl.when(code < 32)
        def _():
            pair_in(code, b, start)

    def pair_in(code, b, start):
        c, h, array = chip_packed(code), half_in(code), (code // 16) % 2
        mine = c == chip
        for plane in range(2):
            blk = c * 2 + plane
            here = slice(plane * rows, (plane + 1) * rows)
            dst, src, sem = tok.at[b, here], full.at[array, blk, span(h)], tok_sem.at[b, plane]
            spread = pl.ds(pl.multiple_of(blk * block + h * rows, rows), rows)
            pair = (
                pltpu.make_async_copy(gate.at[spread], gb.at[b, here], g_sem.at[b, plane]),
                pltpu.make_async_copy(up.at[spread], ub.at[b, here], u_sem.at[b, plane]),
            )
            if not start:
                pltpu.make_async_copy(src, dst, sem).wait()

                @pl.when(array == DY)
                def _(pair=pair):
                    for copy in pair:
                        copy.wait()

                continue

            @pl.when(array == DY)
            def _(pair=pair):
                for copy in pair:
                    copy.start()

            local = mine & (core == plane)

            @pl.when(core != plane)
            def _():
                from_partner(array, c, h)

            @pl.when(jnp.logical_not(local))
            def _(src=src, dst=dst, sem=sem):
                pltpu.make_async_copy(src, dst, sem).start()

            for a in (DY, X):

                @pl.when(local & (array == a))
                def _(a=a, dst=dst, sem=sem):
                    pltpu.make_async_copy(own_in[a].at[span(h)], dst, sem).start()

    def work_dy(code, b):
        index = chip_packed(code) * 2 + half_in(code)
        dh[...] = lax.dot_general(tok[b], wd[...], BY_COLUMNS, preferred_element_type=F32)

        def pointwise(r):
            g, u, dhid = gb[b, r, :].astype(F32), ub[b, r, :].astype(F32), dh[r, :]
            g2 = g * g
            t = jnp.tanh(g * (ROOT + (ROOT * 0.044715) * g2))
            cdf = 0.5 + 0.5 * t
            act = g * cdf
            slope = cdf + (0.5 * g) * (1.0 - t * t) * (ROOT + (3 * ROOT * 0.044715) * g2)
            d[index, r, width:] = (dhid * act).astype(BF16)
            d[index, r, :width] = ((dhid * u) * slope).astype(BF16)
            gb[b, r, :] = (act * u).astype(BF16)

        by_rows(16, 2 * rows, pointwise)

        def column(n, _):
            cols = pl.ds(pl.multiple_of(n * tile, tile), tile)
            new = lax.dot_general(gb[b], tok[b, :, cols], BY_ROWS, preferred_element_type=F32)
            for i in range(ni):
                for j in range(tile // LANES):
                    k = i * nj + n * (tile // LANES) + j
                    acc[0, k] += new[lanes(i), lanes(j)]
            return 0

        lax.fori_loop(0, depth // tile, column, 0)

    def work_x(code, b):
        index = chip_packed(code) * 2 + half_in(code)

        def column(n, _):
            cols = pl.ds(pl.multiple_of(n * tile, tile), tile)
            new = lax.dot_general(tok[b, :, cols], d[index], BY_ROWS, preferred_element_type=F32)
            for i in range(tile // LANES):
                for j in range(2 * ni):
                    k = (n * (tile // LANES) + i) * ni + j % ni
                    acc[j // ni, k] += new[lanes(i), lanes(j)]
            return 0

        lax.fori_loop(0, depth // tile, column, 0)

    def last_x(code):
        c, h = chip_packed(code), half_in(code)
        own = pltpu.make_async_copy(d.at[c * 2 + h, span(core)], parts.at[4, 0, 0:rows, 0 : 2 * width], tok_sem.at[0, 0])
        own.start()

        def keep(r):
            there = pl.ds(pl.multiple_of((1 - core) * rows + r.start, 16), 16)
            d_last[r, :] = d[c * 2 + h, there, :]

        by_rows(16, rows, keep)
        own.wait()
        last_to_partner().wait_recv()

    def finish_down():
        for i in range(ni):
            for j in range(nj):
                wd[lanes(i), lanes(j)] = acc[0, i * nj + j].astype(BF16)
                acc[0, i * nj + j] = jnp.zeros((LANES, LANES), F32)

    def clear(i):
        def body(k, _):
            acc[i, k] = jnp.zeros((LANES, LANES), F32)
            return 0

        lax.fori_loop(0, ni * nj, body, 0)


    pairs = (w_down, wd), (w_gate, w.at[:, :width]), (w_up, w.at[:, width:])
    loads = [pltpu.make_async_copy(s, d, l_sem.at[i]) for i, (s, d) in enumerate(pairs)]
    for load in loads:
        load.start()

    barrier = pltpu.get_barrier_semaphore()
    for to in (at_link[P_], at_link[Y_], partner):
        pl.semaphore_signal(barrier, inc=1, device_id={"tp": to}, device_id_type=MESH)

    @pl.when(is_m)
    def _():
        pl.semaphore_signal(barrier, inc=1, device_id={"tp": at_link[D_]}, device_id_type=MESH)
        pl.semaphore_wait(barrier, 4)

    @pl.when(is_c)
    def _():
        pl.semaphore_wait(barrier, 3)

    x_from = jnp.where(is_m, X_FROM["M"], X_FROM["C"])

    first_sum = jnp.where(is_m, min(k for k in sum_count if k < 100), min(k for k in sum_count if k >= 100) - 100)
    last_sum = jnp.where(is_m, max(LAST["M"]), max(LAST["C"]))

    def step(s, _):
        @pl.when(s == last_sum)
        def _():
            dx_term(select((role * 100 + s) * 10, sum_what), core)

        communicate(s)

        @pl.when(s == x_from)
        def _():
            finish_down()

        key = role * 100 + s
        n_tok = select(key, tok_count)

        @pl.when(n_tok > 0)
        def _():
            tok_in(select(key * 10, tok_what), 0, True)

        @pl.when(s == 0)
        def _():
            clear(0)
            clear(1)
            for load in loads:
                load.wait()

        def sums(k, _):
            reduce_one(select(key * 10 + k, sum_what))
            return 0

        def tokens(k, _):
            code, b = select(key * 10 + k, tok_what), k % 2

            @pl.when(k + 1 < n_tok)
            def _():
                tok_in(select(key * 10 + k + 1, tok_what), 1 - b, True)

            tok_in(code, b, False)

            @pl.when((code // 16) % 2 == DY)
            def _():
                work_dy(code, b)

            @pl.when(code // 16 == X)
            def _():
                work_x(code, b)

            @pl.when(code >= 32)
            def _():
                last_x(code)

            return 0

        n_sum, tokens_first = select(key, sum_count), is_m & (s == last_sum)

        def phase(p, _):
            now = (p == 0) != tokens_first
            lax.fori_loop(0, jnp.where(now, n_sum, 0), sums, 0)
            lax.fori_loop(0, jnp.where(now, 0, n_tok), tokens, 0)
            return 0

        lax.fori_loop(0, 2, phase, 0)

        n_next = select(key + 1, sum_count)

        def partners(k, _):
            code = select((key + 1) * 10 + k, sum_what)

            @pl.when((code // 2**17) % 2 == 0)
            def _():
                partner_one(code, (k == 0) & (s + 1 == first_sum))

            return 0

        lax.fori_loop(0, n_next, partners, 0)

        return 0

    lax.fori_loop(0, STEPS, step, 0)

    def pieces_left(sem, n):
        sizes = [(b, n * quarter // b) for b in range(1, 2 * blocks) if n * quarter % b == 0 and n * quarter // b <= block]
        b, m = min(sizes, key=lambda size: size[1] % 8 > 0)
        some = full.at[0, pl.ds(0, b), pl.ds(0, m)]
        remote(some, some, sem, ag_recv.at[0, 0, 0], partner).wait_send()

    for r, here in enumerate((is_m, is_c)):

        @pl.when(here)
        def _(r=r):
            for link in (P_, D_, Y_):
                n = sum(k // 100 == r for k in send_what[link])
                if n:
                    pieces_left(ag_send.at[link], n)
                    parts_sent = sent[ROLES[r], link]
                    for i in (len(parts_sent) - 2, len(parts_sent) - 1):
                        lo, m = part_rows[parts_sent[i]]
                        here, there = out.at[link, i % 2, pl.ds(lo, m)], parts.at[link, 0, pl.ds(lo, m)]
                        remote(here, there, rs_send.at[link, i % 2], rs_recv.at[link, 0, 0], partner).wait_send()

    for array in (DY, X):
        pieces_left(w_send.at[array], 32 if array == DY else 30)
    last_to_partner().wait_send()
    term_to_partner(0).wait_send()


def finish(
    dx, wd, acc, d, rows_in, full, parts, to_x, to_gate, to_up, to_down, done, d_in, rows_own, o_sem, d_sem, g_sem
):
    depth, width = to_gate.shape
    rows, tile, ni = rows_in.shape[0], 512, width // LANES
    tp = lax.axis_index("tp")
    core, y, z = tp % 2, tp // 8, (tp // 2) % 4
    half, middle = z // 2, ((z + 1) % 4) // 2
    code = jnp.where(middle == 1, last_code("M"), last_code("C"))
    ry, rh, mm, h = code % 2, (code // 2) % 2, (code // 4) % 2, code // 8
    yy, hh = y + ry - 2 * y * ry, half + rh - 2 * half * rh
    block = (yy * 4 + mm + hh * (3 - 2 * mm)) * 2 + core
    loads = (
        pltpu.make_async_copy(full.at[X, block, pl.ds(pl.multiple_of(h * rows, rows), rows)], rows_own, o_sem.at[0]),
        pltpu.make_async_copy(parts.at[4, 0, 0:rows, 0 : 2 * width], d_in, o_sem.at[1]),
    )
    for load in loads:
        load.start()
    copies = []
    for i, (result, place) in enumerate(((dx, to_x), (wd, to_down))):
        n = result.shape[0] // 4
        for k in range(4):
            here = pl.ds(k * n, n)
            copies.append(pltpu.make_async_copy(result.at[here], place.at[here], d_sem.at[i, k]))
    for copy in copies:
        copy.start()

    def store(a, n):
        here = pl.ds(pl.multiple_of(n * tile, tile), tile)
        return pltpu.make_async_copy(done.at[a, here], (to_gate, to_up)[a].at[here], g_sem.at[a, n])

    for load in loads:
        load.wait()

    def column(n, _):
        cols = pl.ds(pl.multiple_of(n * tile, tile), tile)
        new = lax.dot_general(rows_in[:, cols], d[...], BY_ROWS, preferred_element_type=F32)
        new += lax.dot_general(rows_own[:, cols], d_in[...], BY_ROWS, preferred_element_type=F32)
        for i in range(tile // LANES):
            to = pl.ds(pl.multiple_of(n * tile + i * LANES, LANES), LANES)
            for j in range(2 * ni):
                a, k = j // ni, (n * (tile // LANES) + i) * ni + j % ni
                one = acc[a, k] + new[lanes(i), lanes(j)]
                done[a, to, j % ni * LANES : (j % ni + 1) * LANES] = one.astype(BF16)
        for a in range(2):
            store(a, n).start()
        return 0

    lax.fori_loop(0, depth // tile, column, 0)
    for copy in copies:
        copy.wait()
    for n in range(depth // tile):
        for a in range(2):
            store(a, n).wait()


def solution(mesh):
    def step(x, dy, gate, up, w_gate, w_up, w_down):
        block, depth = dy.shape
        tokens, width = gate.shape
        rows, chips = block // 2, tokens // block // 2
        anywhere, inside = pl.BlockSpec(memory_space=pl.ANY), pl.BlockSpec(memory_space=pltpu.VMEM)
        dma, flops = pltpu.SemaphoreType.DMA, 12 * tokens * depth * width
        outs = pl.pallas_call(
            kernel,
            out_shape=[
                pltpu.VMEM((block, depth), BF16),
                pltpu.VMEM((width, depth), BF16),
                pltpu.VMEM((2, (depth // LANES) * (width // LANES), LANES, LANES), F32),
                pltpu.VMEM((rows, 2 * width), BF16),
                pltpu.VMEM((rows, depth), BF16),
                jax.ShapeDtypeStruct((2, 2 * chips, block, depth), BF16),
                jax.ShapeDtypeStruct((5, chips, block, depth), BF16),
            ],
            in_specs=[anywhere] * 7,
            out_specs=[inside] * 5 + [anywhere] * 2,
            scratch_shapes=[
                pltpu.VMEM((depth, 2 * width), BF16),
                pltpu.VMEM((2 * chips, 2 * rows, 2 * width), BF16),
                pltpu.VMEM((2, 2 * rows, depth), BF16),
                pltpu.VMEM((2, 2 * rows, width), BF16),
                pltpu.VMEM((2, 2 * rows, width), BF16),
                pltpu.VMEM((2 * rows, width), F32),
                pltpu.VMEM((rows, depth), F32),
                pltpu.VMEM((4, rows, depth), BF16),
                pltpu.VMEM((3, 2, rows, depth), BF16),
                pltpu.VMEM((rows, depth), BF16),
                dma((2, chips, 4)),
                dma((3,)),
                dma((2, chips, 4)),
                dma((2,)),
                dma((4, chips, 2)),
                dma((3, 2)),
                dma(()),
                dma(()),
                dma((3,)),
                dma((2, 2)),
                dma((2, 2)),
                dma((2, 2)),
                dma((4,)),
            ],
            compiler_params=pltpu.CompilerParams(collective_id=0, has_side_effects=True, vmem_limit_bytes=46900000),
            cost_estimate=pl.CostEstimate(flops=flops, bytes_accessed=12 * tokens * depth, transcendentals=tokens * width),
            name="mlp_backward",
        )(x, dy, gate, up, w_gate, w_up, w_down)
        return pl.pallas_call(
            finish,
            out_shape=[jax.ShapeDtypeStruct(a.shape, BF16) for a in (dy, w_gate, w_up, w_down)],
            in_specs=[inside] * 5 + [anywhere] * 2,
            out_specs=[anywhere] * 4,
            scratch_shapes=[
                pltpu.VMEM((2, depth, width), BF16),
                pltpu.VMEM((rows, 2 * width), BF16),
                pltpu.VMEM((rows, depth), BF16),
                dma((2,)),
                dma((2, 4)),
                dma((2, depth // 512)),
            ],
            compiler_params=pltpu.CompilerParams(vmem_limit_bytes=2**24),
            name="finish",
        )(*outs)

    rows_, cols_ = P(("dp", "tp"), None), P("dp", "tp")
    return jax.shard_map(
        step,
        mesh=mesh,
        in_specs=(rows_, rows_, cols_, cols_, P(None, "tp"), P(None, "tp"), P("tp", None)),
        out_specs=(rows_, cols_, cols_, rows_),
        check_vma=False,
    )
```

```python
import jax
import jax.numpy as jnp
from jax import lax
from jax.experimental import pallas as pl
from jax.experimental.pallas import tpu as pltpu
from jax.sharding import PartitionSpec as P

MESH = pl.DeviceIdType.MESH
F32, BF16 = jnp.float32, jnp.bfloat16

LANES = 128
ROOT = 0.7978845608028654
BY_ROWS, BY_COLUMNS = (((0,), (0,)), ((), ())), (((1,), (1,)), ((), ()))
P_, D_, Y_, W_ = 0, 1, 2, 3
DY, X = 0, 1
ROLES = "MC"
LINKS = {"a": ("C", "C", Y_), "b": ("M", "C", P_), "c": ("C", "M", P_), "d": ("M", "M", D_), "e": ("M", "M", Y_)}

START = {
    "a": [
        "d00C0", "d00M0", "d00M1", "d01C0", "d00C1", "s10M0", "d01M1", "d01C1", "d01M0", "x01M1", "x01C1", "x00M1",
        "x00C1", "x00M0", "s10M2", "x01C0", "x00C0",
    ],
    "b": [
        "d00M0", "d00M1", "d01C0", "s10M0", "d01M1", "s10M2", "d01C1", "d01M0", "x01M1", "x01C1", "x00M1", "x11M0",
        "x00M0", "x01M0", "x01C0", "s00C0", "s00C1",
    ],
    "c": [
        "d00C0", "x00C0", "d00C1", "x00C1", "s10C0", "s01C0", "s11C0", "s00M0", "s10C1", "s11M1", "s11C1", "s11M0",
        "s01C1", "s01M0", "x10C7", "s01M1", "s10M3", "s00M1",
    ],
    "d": [
        "d00M0", "d00C0", "d00M1", "d10M0", "d10M1", "d00C1", "x10M1", "x00M1", "x00C1", "x00M0", "x10M0", "s01C0",
        "s11C1", "x00C0", "s01C1", "s01M0", "s01M1",
    ],
    "e": [
        "d00M0", "d00M1", "d01C0", "d00C1", "d00C0", "x00M1", "d01C1", "s10C0", "s11C0", "x00M0", "x01C1", "s11M1",
        "x00C6", "s11M0", "s10C1", "x01C0", "x00C0", "s10M3",
    ],
}
TOKENS = {
    "M": [
        "0d00M0", "1d00M1", "4d10M0", "4d00C0", "5d01M0", "6d10M1", "6d01C0", "8d11C0", "8d00C1", "9d01M1", "10d11M0", "10d10C1",
        "12d10C0", "12d11M1", "14d01C1", "16d11C1", "17x00M0", "17x00M1", "18x00C0", "18x00C1", "19x10M1", "19x11M1", "20x01M1", "20x01C1",
        "22x01M0", "22x10M0", "24x11C1", "24x11M0", "30x01C0", "31x10C1", "33x11C0", "35x10C0",
    ],
    "C": [
        "0d00C0", "1d00C1", "4d10C0", "4d00M0", "6d10M0", "6d00M1", "8d01C0", "8d10M1", "10d11C0", "12d10C1", "12d01M1", "16d11M1",
        "16d01C1", "18d11C1", "18d01M0", "20d11M0", "21x00C0", "21x00C1", "22x01M1", "22x01C1", "23x11M1", "24x00M1", "24x11C1", "26x10M1",
        "26x11M0", "28x00M0", "28x10C1", "30x01M0", "30x10M0", "32x01C0", "34x11C0", "36x10C0",
    ],
}
X_FROM = {"M": 17, "C": 21}
LAST = {"M": (33, 35), "C": (33, 35)}
STEPS = 37


def seen_by_receiver(unit, link):
    flip = {"0": "1", "1": "0"}
    if link == Y_:
        return flip[unit[0]] + unit[1:]
    return unit[0] + flip[unit[1]] + unit[2] if link == D_ else unit


def pack(unit):
    return int(unit[0]) + 2 * int(unit[1]) + 4 * (unit[2] == "M")


def lanes(i):
    return slice(i * LANES, (i + 1) * LANES)


def half_in(code):
    return (code // 8) % 2


def select(key, table):
    out = jnp.int32(0)
    for k, v in table.items():
        out = jnp.where(key == k, jnp.int32(v), out)
    return out


def plan():
    send, recv = ({P_: {}, D_: {}, Y_: {}} for _ in range(2))
    sums, terms, sent = {"M": {}, "C": {}}, {}, {}
    for name, entries in START.items():
        sender, receiver, link = LINKS[name]
        t = 0
        for what in entries:
            if what[0] == "+":
                t += int(what)
                continue
            kind, unit, part = what[0], what[1:4], int(what[4])
            there = seen_by_receiver(unit, link)
            if kind == "s":
                h, part = (1, part - 1) if part > 1 else (part, 0)
                before = sent.setdefault((sender, link), [])
                sums[sender].setdefault(t, []).append((unit, h, part, link, len(before) % 2, before[-2] + 1 if len(before) > 1 else 0, 0))
                before.append(part)
                terms.setdefault((receiver, there, h), []).append((link, part))
                t += 1 if part == 2 else 2
                continue
            for p in (2 * part, 2 * part + 1) if part < 2 else (part - 4,):
                code = 1 + "dx".index(kind) + 16 * p
                send[link][ROLES.index(sender) * 100 + t] = code + 2 * pack(unit)
                recv[link][ROLES.index(receiver) * 100 + t + 2] = code + 2 * pack(there)
                t += 1
    for role in ROLES:
        for h in range(2):
            early = h == (LAST[role][1] >= LAST[role][0])
            sums[role].setdefault(LAST[role][h], []).insert(0, ("00" + role, h, 0, 3, 0, 0, early))
    sum_count, sum_what, tok_count, tok_what = {}, {}, {}, {}
    for r, role in enumerate(ROLES):
        met = set()
        for t, entries in sorted(sums[role].items()):
            sum_count[r * 100 + t] = len(entries)
            for k, (unit, h, part, link, parity, before, early) in enumerate(entries):
                mine = [(i, p) for i, p in terms.get((role, unit, h), []) if part in (0, p)]
                odd = [(i, p) for i, p in mine if p]
                code = pack(unit) + 8 * h + 16 * sum(1 << i for i, _ in mine) + 128 * link + 512 * parity + 1024 * before
                code += 4096 * early + 8192 * part + 2**17 * ((unit, h) in met)
                if odd:
                    code += 2**15 * (odd[0][1] + 0) + 2**18 * odd[0][0]
                met.add((unit, h))
                sum_what[(r * 100 + t) * 10 + k] = code
        for what in TOKENS[role]:
            t, kind, unit, h = int(what[:-5]), what[-5], what[-4:-1], int(what[-1])
            k = tok_count.get(r * 100 + t, 0)
            tok_count[r * 100 + t] = k + 1
            code = pack(unit) + 8 * h + 16 * "dx".index(kind)
            tok_what[(r * 100 + t) * 10 + k] = code + 32 * (what is TOKENS[role][-1])
    return send, recv, sum_count, sum_what, tok_count, tok_what, sent


def last_code(role):
    what = TOKENS[role][-1]
    return pack(what[-4:-1]) + 8 * int(what[-1])


def kernel(
    x, dy, gate, up, w_gate, w_up, w_down,
    dx, wd, acc, d_last, last_rows, full, parts,
    w, d, tok, gb, ub, dh, total, ext, out, outw,
    ag_recv, ag_send, w_recv, w_send, rs_recv, rs_send, p_send, l_send, l_sem, tok_sem, g_sem, u_sem, e_sem,
):
    block, depth = dy.shape
    width = gate.shape[1]
    rows, quarter, blocks = block // 2, block // 4, full.shape[1] // 2
    tile = 512
    nj, ni = depth // LANES, width // LANES
    own_in = {DY: dy, X: x}
    send_what, recv_what, sum_count, sum_what, tok_count, tok_what, sent = plan()

    tp = lax.axis_index("tp")
    core, chip = tp % 2, tp // 2
    y, z = chip // 4, chip % 4
    half = z // 2
    middle = ((z + 1) % 4) // 2
    is_m, is_c = middle == 1, middle == 0
    role = 1 - middle

    def chip_of(yy, hh, mm):
        return yy * 4 + mm + hh * (3 - 2 * mm)

    def chip_packed(code):
        ry, rh, mm = code % 2, (code // 2) % 2, (code // 4) % 2
        return chip_of(y + ry - 2 * y * ry, half + rh - 2 * half * rh, mm)

    partner = tp + 1 - 2 * core
    at_link = {
        P_: chip_of(y, half, 1 - middle) * 2 + core,
        D_: chip_of(y, 1 - half, middle) * 2 + core,
        Y_: chip_of(1 - y, half, middle) * 2 + core,
    }

    def span(h):
        return pl.ds(pl.multiple_of(h * rows, rows), rows)

    def quarter_at(p):
        return pl.ds(pl.multiple_of(p * quarter, quarter), quarter)

    def remote(src, dst, send, recv, to):
        return pltpu.make_async_remote_copy(
            src_ref=src, dst_ref=dst, send_sem=send, recv_sem=recv, device_id={"tp": to}, device_id_type=MESH
        )

    def by_rows(step, n_rows, fn, start=0):
        def body(i, _):
            fn(pl.ds(pl.multiple_of(i * step, step), step))
            return 0

        lax.fori_loop(start // step, n_rows // step, body, 0)

    cut = rows * 3 // 4 // 16 * 16
    part_rows = ((0, rows), (0, cut), (cut, rows - cut))

    def bounds(part):
        return jnp.where(part == 2, cut, 0), jnp.where(part == 1, cut, rows)

    def in_part(part, fn):
        for i in range(3):

            @pl.when(part == i)
            def _(i=i):
                fn(*part_rows[i])


    def on_link(link, code, src=None):
        code = code - 1
        array, c, p = code % 2, chip_packed(code // 2), code // 16
        piece = quarter_at(p)
        to = full.at[array, c * 2 + core, piece]
        return remote(to if src is None else src.at[piece], to, ag_send.at[link], ag_recv.at[array, c, p], at_link[link])

    def to_partner(array, c, p, src=None):
        piece = quarter_at(p)
        to = full.at[array, c * 2 + core, piece]
        return remote(to if src is None else src.at[piece], to, w_send.at[array], w_recv.at[array, c, p], partner)

    last = jnp.where(is_m, last_code("M"), last_code("C"))

    def last_to_partner():
        c, h = chip_packed(last), last // 8
        here = full.at[X, c * 2 + core, span(h)]
        return remote(here, last_rows, l_send, w_recv.at[X, c, 2 * h + 1], partner)

    def from_partner(array, c, h):
        for k in range(2):
            there = full.at[array, c * 2 + 1 - core, quarter_at(2 * h + k)]
            remote(there, there, p_send, w_recv.at[array, c, 2 * h + k], partner).wait_recv()

    def communicate(s):
        key = role * 100 + s
        come = {link: select(key, recv_what[link]) for link in (P_, D_, Y_)}
        for link, code in come.items():

            @pl.when(code > 0)
            def _(link=link, code=code):
                on_link(link, code).wait_recv()

        for link in (P_, D_, Y_):
            code = select(key, send_what[link])
            mine = chip_packed((code - 1) // 2) == chip

            @pl.when((code > 0) & jnp.logical_not(mine))
            def _(link=link, code=code):
                on_link(link, code).start()

            for array in (DY, X):

                @pl.when((code > 0) & mine & ((code - 1) % 2 == array))
                def _(link=link, code=code, array=array):
                    on_link(link, code, own_in[array]).start()

        for link, code in come.items():

            ends = ((code - 1) % 16 == X + 2 * (last % 8)) & ((code - 1) // 32 == last // 8)

            @pl.when((code > 0) & jnp.logical_not(ends))
            def _(code=code):
                to_partner((code - 1) % 2, chip_packed((code - 1) // 2), (code - 1) // 16).start()

            @pl.when(ends & ((code - 1) // 16 % 2 == 1))
            def _():
                last_to_partner().start()

        for array, when in ((DY, 0), (X, 2)):

            @pl.when(s == when)
            def _(array=array):
                for p in range(4):
                    to_partner(array, chip, p, own_in[array]).start()


    def dx_term(code, plane):
        index = chip_packed(code) * 2 + half_in(code)
        here = span(plane)

        def column(n, _):
            cols = pl.ds(pl.multiple_of(n * tile, tile), tile)
            total[:, cols] = lax.dot_general(
                d[index, here, :], w[cols, :], BY_COLUMNS, preferred_element_type=F32
            )
            return 0

        lax.fori_loop(0, depth // tile, column, 0)

    def reduce_one(code):
        c, h = chip_packed(code), half_in(code)
        mask, link, parity, before = (code // 16) % 8, (code // 128) % 4, (code // 512) % 2, (code // 1024) % 4
        early, part, again = (code // 4096) % 2 == 1, (code // 8192) % 4, (code // 2**17) % 2 == 1
        odd_part, odd = (code // 2**15) % 4, code // 2**18
        bits = {P_: mask % 2 == 1, D_: (mask // 2) % 2 == 1, Y_: mask // 4 == 1}
        part_of = {P_: jnp.where(odd == P_, odd_part, 0), D_: jnp.int32(0), Y_: jnp.where(odd == Y_, odd_part, 0), W_: jnp.int32(0)}

        def there(lo, n):
            return pl.ds(pl.multiple_of(h * rows + lo, 16), n)

        def term_in(kind, lo, n):
            return pltpu.make_async_copy(parts.at[kind, c, there(lo, n)], ext.at[kind, pl.ds(lo, n)], e_sem.at[kind])

        def with_term(kind, fn):
            if kind in (P_, Y_):
                in_part(part_of[kind], fn)
            else:
                fn(0, rows)

        def arrived(kind):
            def wait(lo, n):
                here = ext.at[kind, pl.ds(lo, n)]
                remote(here, parts.at[kind, c, there(lo, n)], p_send, rs_recv.at[kind, c, h], partner).wait_recv()

            with_term(kind, wait)

        def fetch(kind):
            with_term(kind, lambda lo, n: term_in(kind, lo, n).start())

        def send_term(to, lo, n):
            return remote(
                out.at[link, parity, pl.ds(lo, n)], parts.at[link, c, there(lo, n)], rs_send.at[link, parity],
                rs_recv.at[link, c, h], to,
            )

        @pl.when(jnp.logical_not(again))
        def _():
            arrived(W_)

        fetch(W_)
        for kind in (P_, D_, Y_):

            @pl.when(bits[kind] & (link != 3))
            def _(kind=kind):
                arrived(kind)
                fetch(kind)

        @pl.when(jnp.logical_not(early))
        def _():
            dx_term(code, core)

        for kind in (P_, D_, Y_):

            @pl.when(bits[kind] & (link == 3))
            def _(kind=kind):
                arrived(kind)
                fetch(kind)

        for kind in (P_, D_, Y_):

            @pl.when(bits[kind])
            def _(kind=kind):
                with_term(kind, lambda lo, n: term_in(kind, lo, n).wait())

                def add(r):
                    total[r, :] += ext[kind, r, :].astype(F32)

                lo, hi = bounds(part_of[kind])
                by_rows(16, hi, add, lo)

        term_in(W_, 0, rows).wait()

        @pl.when(link == 3)
        def _():
            def finish(r):
                to = pl.ds(pl.multiple_of(h * rows + r.start, 16), 16)
                dx[to, :] = (total[r, :] + ext[W_, r, :].astype(F32)).astype(BF16)

            by_rows(16, rows, finish)

        @pl.when(link != 3)
        def _():
            to = jnp.where(link == P_, at_link[P_], jnp.where(link == D_, at_link[D_], at_link[Y_]))
            in_part(before - 1, lambda lo, n: send_term(to, lo, n).wait_send())

            def round_(r):
                out[link, parity, r, :] = (total[r, :] + ext[W_, r, :].astype(F32)).astype(BF16)

            lo, hi = bounds(part)
            by_rows(16, hi, round_, lo)
            in_part(part, lambda lo, n: send_term(to, lo, n).start())

    def term_to_partner(code):
        c, h = chip_packed(code), half_in(code)
        return remote(outw, parts.at[W_, c, span(h)], p_send, rs_recv.at[W_, c, h], partner)

    def partner_one(code, first):
        dx_term(code, 1 - core)

        @pl.when(jnp.logical_not(first))
        def _():
            term_to_partner(code).wait_send()

        def round_(r):
            outw[r, :] = total[r, :].astype(BF16)

        by_rows(16, rows, round_)
        term_to_partner(code).start()


    def last_in(code, b):
        c, h = chip_packed(code), half_in(code)
        src = full.at[X, c * 2 + core, span(h)]
        return pltpu.make_async_copy(src, tok.at[b, span(core)], tok_sem.at[b, core])

    def tok_in(code, b, start):
        @pl.when(code < 32)
        def _():
            pair_in(code, b, start)

        @pl.when(code >= 32)
        def _():
            copy = last_in(code, b)
            copy.start() if start else copy.wait()

    def pair_in(code, b, start):
        c, h, array = chip_packed(code), half_in(code), (code // 16) % 2
        mine = c == chip
        for plane in range(2):
            blk = c * 2 + plane
            here = slice(plane * rows, (plane + 1) * rows)
            dst, src, sem = tok.at[b, here], full.at[array, blk, span(h)], tok_sem.at[b, plane]
            spread = pl.ds(pl.multiple_of(blk * block + h * rows, rows), rows)
            pair = (
                pltpu.make_async_copy(gate.at[spread], gb.at[b, here], g_sem.at[b, plane]),
                pltpu.make_async_copy(up.at[spread], ub.at[b, here], u_sem.at[b, plane]),
            )
            if not start:
                pltpu.make_async_copy(src, dst, sem).wait()

                @pl.when(array == DY)
                def _(pair=pair):
                    for copy in pair:
                        copy.wait()

                continue

            @pl.when(array == DY)
            def _(pair=pair):
                for copy in pair:
                    copy.start()

            local = mine & (core == plane)

            @pl.when(core != plane)
            def _():
                from_partner(array, c, h)

            @pl.when(jnp.logical_not(local))
            def _(src=src, dst=dst, sem=sem):
                pltpu.make_async_copy(src, dst, sem).start()

            for a in (DY, X):

                @pl.when(local & (array == a))
                def _(a=a, dst=dst, sem=sem):
                    pltpu.make_async_copy(own_in[a].at[span(h)], dst, sem).start()

    def work_dy(code, b):
        index = chip_packed(code) * 2 + half_in(code)
        dh[...] = lax.dot_general(tok[b], wd[...], BY_COLUMNS, preferred_element_type=F32)

        def pointwise(r):
            g, u, dhid = gb[b, r, :].astype(F32), ub[b, r, :].astype(F32), dh[r, :]
            g2 = g * g
            t = jnp.tanh(g * (ROOT + (ROOT * 0.044715) * g2))
            cdf = 0.5 + 0.5 * t
            act = g * cdf
            slope = cdf + (0.5 * g) * (1.0 - t * t) * (ROOT + (3 * ROOT * 0.044715) * g2)
            d[index, r, width:] = (dhid * act).astype(BF16)
            d[index, r, :width] = ((dhid * u) * slope).astype(BF16)
            gb[b, r, :] = (act * u).astype(BF16)

        by_rows(16, 2 * rows, pointwise)

        def column(n, _):
            cols = pl.ds(pl.multiple_of(n * tile, tile), tile)
            new = lax.dot_general(gb[b], tok[b, :, cols], BY_ROWS, preferred_element_type=F32)
            for i in range(ni):
                for j in range(tile // LANES):
                    k = i * nj + n * (tile // LANES) + j
                    acc[0, k] += new[lanes(i), lanes(j)]
            return 0

        lax.fori_loop(0, depth // tile, column, 0)

    def x_columns(index, b, here):
        def column(n, _):
            cols = pl.ds(pl.multiple_of(n * tile, tile), tile)
            xt = tok[b, here, cols]
            new = lax.dot_general(xt, d[index, here, :], BY_ROWS, preferred_element_type=F32)
            for i in range(tile // LANES):
                for j in range(2 * ni):
                    k = (n * (tile // LANES) + i) * ni + j % ni
                    acc[j // ni, k] += new[lanes(i), lanes(j)]
            return 0

        lax.fori_loop(0, depth // tile, column, 0)

    def work_x(code, b):
        x_columns(chip_packed(code) * 2 + half_in(code), b, slice(None))

    def last_x(code, b):
        c, h = chip_packed(code), half_in(code)
        x_columns(c * 2 + h, b, span(core))

        def keep(r):
            there = pl.ds(pl.multiple_of((1 - core) * rows + r.start, 16), 16)
            d_last[r, :] = d[c * 2 + h, there, :]

        by_rows(16, rows, keep)
        last_to_partner().wait_recv()

    def finish_down():
        for i in range(ni):
            for j in range(nj):
                wd[lanes(i), lanes(j)] = acc[0, i * nj + j].astype(BF16)
                acc[0, i * nj + j] = jnp.zeros((LANES, LANES), F32)

    def clear(i):
        def body(k, _):
            acc[i, k] = jnp.zeros((LANES, LANES), F32)
            return 0

        lax.fori_loop(0, ni * nj, body, 0)


    pairs = (w_down, wd), (w_gate, w.at[:, :width]), (w_up, w.at[:, width:])
    loads = [pltpu.make_async_copy(s, d, l_sem.at[i]) for i, (s, d) in enumerate(pairs)]
    for load in loads:
        load.start()

    barrier = pltpu.get_barrier_semaphore()
    for to in (at_link[P_], at_link[Y_], partner):
        pl.semaphore_signal(barrier, inc=1, device_id={"tp": to}, device_id_type=MESH)

    @pl.when(is_m)
    def _():
        pl.semaphore_signal(barrier, inc=1, device_id={"tp": at_link[D_]}, device_id_type=MESH)
        pl.semaphore_wait(barrier, 4)

    @pl.when(is_c)
    def _():
        pl.semaphore_wait(barrier, 3)

    x_from = jnp.where(is_m, X_FROM["M"], X_FROM["C"])

    first_sum = jnp.where(is_m, min(k for k in sum_count if k < 100), min(k for k in sum_count if k >= 100) - 100)
    last_sum = jnp.where(is_m, max(LAST["M"]), max(LAST["C"]))

    def step(s, _):
        @pl.when(s == last_sum)
        def _():
            dx_term(select((role * 100 + s) * 10, sum_what), core)

        communicate(s)

        @pl.when(s == x_from)
        def _():
            finish_down()

        key = role * 100 + s
        n_tok = select(key, tok_count)

        @pl.when(n_tok > 0)
        def _():
            tok_in(select(key * 10, tok_what), 0, True)

        @pl.when(s == 0)
        def _():
            clear(0)
            clear(1)
            for load in loads:
                load.wait()

        def sums(k, _):
            reduce_one(select(key * 10 + k, sum_what))
            return 0

        def tokens(k, _):
            code, b = select(key * 10 + k, tok_what), k % 2

            @pl.when(k + 1 < n_tok)
            def _():
                tok_in(select(key * 10 + k + 1, tok_what), 1 - b, True)

            tok_in(code, b, False)

            @pl.when((code // 16) % 2 == DY)
            def _():
                work_dy(code, b)

            @pl.when(code // 16 == X)
            def _():
                work_x(code, b)

            @pl.when(code >= 32)
            def _():
                last_x(code, b)

            return 0

        n_sum, tokens_first = select(key, sum_count), is_m & (s == last_sum)

        def phase(p, _):
            now = (p == 0) != tokens_first
            lax.fori_loop(0, jnp.where(now, n_sum, 0), sums, 0)
            lax.fori_loop(0, jnp.where(now, 0, n_tok), tokens, 0)
            return 0

        lax.fori_loop(0, 2, phase, 0)

        n_next = select(key + 1, sum_count)

        def partners(k, _):
            code = select((key + 1) * 10 + k, sum_what)

            @pl.when((code // 2**17) % 2 == 0)
            def _():
                partner_one(code, (k == 0) & (s + 1 == first_sum))

            return 0

        lax.fori_loop(0, n_next, partners, 0)

        return 0

    lax.fori_loop(0, STEPS, step, 0)

    def pieces_left(sem, n):
        sizes = [(b, n * quarter // b) for b in range(1, 2 * blocks) if n * quarter % b == 0 and n * quarter // b <= block]
        b, m = min(sizes, key=lambda size: size[1] % 8 > 0)
        some = full.at[0, pl.ds(0, b), pl.ds(0, m)]
        remote(some, some, sem, ag_recv.at[0, 0, 0], partner).wait_send()

    for r, here in enumerate((is_m, is_c)):

        @pl.when(here)
        def _(r=r):
            for link in (P_, D_, Y_):
                n = sum(k // 100 == r for k in send_what[link])
                if n:
                    pieces_left(ag_send.at[link], n)
                    parts_sent = sent[ROLES[r], link]
                    for i in (len(parts_sent) - 2, len(parts_sent) - 1):
                        lo, m = part_rows[parts_sent[i]]
                        here, there = out.at[link, i % 2, pl.ds(lo, m)], parts.at[link, 0, pl.ds(lo, m)]
                        remote(here, there, rs_send.at[link, i % 2], rs_recv.at[link, 0, 0], partner).wait_send()

    for array in (DY, X):
        pieces_left(w_send.at[array], 32 if array == DY else 30)
    last_to_partner().wait_send()
    term_to_partner(0).wait_send()


def finish(dx, wd, acc, d, rows_in, to_x, to_gate, to_up, to_down, done, d_sem, g_sem):
    depth, width = to_gate.shape
    tile, ni = 512, width // LANES
    copies = []
    for i, (result, place) in enumerate(((dx, to_x), (wd, to_down))):
        n = result.shape[0] // 4
        for k in range(4):
            here = pl.ds(k * n, n)
            copies.append(pltpu.make_async_copy(result.at[here], place.at[here], d_sem.at[i, k]))
    for copy in copies:
        copy.start()

    def store(a, n):
        here = pl.ds(pl.multiple_of(n * tile, tile), tile)
        return pltpu.make_async_copy(done.at[a, here], (to_gate, to_up)[a].at[here], g_sem.at[a, n])

    def column(n, _):
        xt = rows_in[:, pl.ds(pl.multiple_of(n * tile, tile), tile)]
        new = lax.dot_general(xt, d[...], BY_ROWS, preferred_element_type=F32)
        for i in range(tile // LANES):
            to = pl.ds(pl.multiple_of(n * tile + i * LANES, LANES), LANES)
            for j in range(2 * ni):
                k = (n * (tile // LANES) + i) * ni + j % ni
                one = acc[j // ni, k] + new[lanes(i), lanes(j)]
                done[j // ni, to, j % ni * LANES : (j % ni + 1) * LANES] = one.astype(BF16)
        for a in range(2):
            store(a, n).start()
        return 0

    lax.fori_loop(0, depth // tile, column, 0)
    for copy in copies:
        copy.wait()
    for n in range(depth // tile):
        for a in range(2):
            store(a, n).wait()


def solution(mesh):
    def step(x, dy, gate, up, w_gate, w_up, w_down):
        block, depth = dy.shape
        tokens, width = gate.shape
        rows, chips = block // 2, tokens // block // 2
        anywhere, inside = pl.BlockSpec(memory_space=pl.ANY), pl.BlockSpec(memory_space=pltpu.VMEM)
        dma, flops = pltpu.SemaphoreType.DMA, 12 * tokens * depth * width
        outs = pl.pallas_call(
            kernel,
            out_shape=[
                pltpu.VMEM((block, depth), BF16),
                pltpu.VMEM((width, depth), BF16),
                pltpu.VMEM((2, (depth // LANES) * (width // LANES), LANES, LANES), F32),
                pltpu.VMEM((rows, 2 * width), BF16),
                pltpu.VMEM((rows, depth), BF16),
                jax.ShapeDtypeStruct((2, 2 * chips, block, depth), BF16),
                jax.ShapeDtypeStruct((4, chips, block, depth), BF16),
            ],
            in_specs=[anywhere] * 7,
            out_specs=[inside] * 5 + [anywhere] * 2,
            scratch_shapes=[
                pltpu.VMEM((depth, 2 * width), BF16),
                pltpu.VMEM((2 * chips, 2 * rows, 2 * width), BF16),
                pltpu.VMEM((2, 2 * rows, depth), BF16),
                pltpu.VMEM((2, 2 * rows, width), BF16),
                pltpu.VMEM((2, 2 * rows, width), BF16),
                pltpu.VMEM((2 * rows, width), F32),
                pltpu.VMEM((rows, depth), F32),
                pltpu.VMEM((4, rows, depth), BF16),
                pltpu.VMEM((3, 2, rows, depth), BF16),
                pltpu.VMEM((rows, depth), BF16),
                dma((2, chips, 4)),
                dma((3,)),
                dma((2, chips, 4)),
                dma((2,)),
                dma((4, chips, 2)),
                dma((3, 2)),
                dma(()),
                dma(()),
                dma((3,)),
                dma((2, 2)),
                dma((2, 2)),
                dma((2, 2)),
                dma((4,)),
            ],
            compiler_params=pltpu.CompilerParams(collective_id=0, has_side_effects=True, vmem_limit_bytes=46900000),
            cost_estimate=pl.CostEstimate(flops=flops, bytes_accessed=12 * tokens * depth, transcendentals=tokens * width),
            name="mlp_backward",
        )(x, dy, gate, up, w_gate, w_up, w_down)
        return pl.pallas_call(
            finish,
            out_shape=[jax.ShapeDtypeStruct(a.shape, BF16) for a in (dy, w_gate, w_up, w_down)],
            in_specs=[inside] * 5,
            out_specs=[anywhere] * 4,
            scratch_shapes=[
                pltpu.VMEM((2, depth, width), BF16),
                dma((2, 4)),
                dma((2, depth // 512)),
            ],
            compiler_params=pltpu.CompilerParams(vmem_limit_bytes=2**24),
            name="finish",
        )(*outs[:5])

    rows_, cols_ = P(("dp", "tp"), None), P("dp", "tp")
    return jax.shard_map(
        step,
        mesh=mesh,
        in_specs=(rows_, rows_, cols_, cols_, P(None, "tp"), P(None, "tp"), P("tp", None)),
        out_specs=(rows_, cols_, cols_, rows_),
        check_vma=False,
    )
```

```python
import jax
import jax.numpy as jnp
from jax import lax
from jax.experimental import pallas as pl
from jax.experimental.pallas import tpu as pltpu
from jax.sharding import PartitionSpec as P

MESH = pl.DeviceIdType.MESH
F32, BF16 = jnp.float32, jnp.bfloat16

LANES = 128
ROOT = 0.7978845608028654
BY_ROWS, BY_COLUMNS = (((0,), (0,)), ((), ())), (((1,), (1,)), ((), ()))
P_, D_, Y_, W_ = 0, 1, 2, 3
DY, X = 0, 1
ROLES = "MC"
LINKS = {"a": ("C", "C", Y_), "b": ("M", "C", P_), "c": ("C", "M", P_), "d": ("M", "M", D_), "e": ("M", "M", Y_)}

START = {
    "a": [
        "d00C1", "d00M0", "d00C0", "d01C0", "d01M1", "d00M1", "d01C1", "s10M0", "d01M0", "s10M2", "x00M1", "x00C0",
        "x00C1", "x01C0", "x01M0", "x01M1", "x00M0",
    ],
    "b": [
        "d00M0", "d00M1", "d01C0", "d01M1", "s10M0", "d01C1", "s10M2", "d01M0", "x01M0", "x00M1", "x00M0", "x01C1",
        "x01C0", "x11C1", "x01M1", "s00C0", "s00C1",
    ],
    "c": [
        "d00C0", "x00C0", "d00C1", "s10C1", "x00C1", "s01C0", "s11C0", "s10C0", "s01C1", "s11C1", "s01M1", "s10M3",
        "s11M1", "s11M0", "x10C7", "s01M0", "s00M0", "s00M1",
    ],
    "d": [
        "d00M1", "d00C0", "d10M0", "d00C1", "d10M1", "x00M0", "d00M0", "s01C0", "x00C0", "x00C1", "x10M0", "s11C0",
        "s01C1", "x00M1", "x10M1", "s01M1", "s01M0",
    ],
    "e": [
        "x00M1", "d00M0", "d00C0", "d00M1", "d00C1", "d01C0", "d01C1", "s10C1", "x00C6", "x00M0", "x01C0", "s11C1",
        "x01C1", "s10C0", "s11M1", "s11M0", "x00C0", "s10M3",
    ],
}
TOKENS = {
    "M": [
        "0d00M0", "1d00M1", "4d00C0", "4d01M1", "6d10M0", "6d01C0", "8d10C0", "8d11M0", "9d00C1", "10d10M1", "10d01C1", "12d10C1",
        "12d11M1", "14d11C0", "16d11C1", "16d01M0", "17x00M0", "17x00M1", "18x10M1", "18x00C0", "19x00C1", "19x01M0", "20x01C0", "21x10M0",
        "22x01C1", "23x11C0", "24x11M0", "27x11C1", "30x01M1", "30x10C1", "32x11M1", "35x10C0",
    ],
    "C": [
        "0d00C0", "1d00C1", "4d10C1", "4d00M0", "6d10M0", "6d00M1", "8d01C0", "8d10C0", "10d11C0", "10d01M1", "12d11M1", "14d01C1",
        "14d10M1", "16d11C1", "18d01M0", "20d11M0", "21x00C0", "21x00C1", "22x01M0", "22x00M1", "24x00M0", "24x10M1", "26x01C1", "26x10C0",
        "28x01C0", "28x10C1", "30x11C0", "30x11C1", "32x01M1", "32x11M0", "34x11M1", "36x10M0",
    ],
}
X_FROM = {"M": 17, "C": 21}
LAST = {"M": (35, 35), "C": (33, 35)}
STEPS = 37


def seen_by_receiver(unit, link):
    flip = {"0": "1", "1": "0"}
    if link == Y_:
        return flip[unit[0]] + unit[1:]
    return unit[0] + flip[unit[1]] + unit[2] if link == D_ else unit


def pack(unit):
    return int(unit[0]) + 2 * int(unit[1]) + 4 * (unit[2] == "M")


def lanes(i):
    return slice(i * LANES, (i + 1) * LANES)


def half_in(code):
    return (code // 8) % 2


def select(key, table):
    out = jnp.int32(0)
    for k, v in table.items():
        out = jnp.where(key == k, jnp.int32(v), out)
    return out


def plan():
    send, recv = ({P_: {}, D_: {}, Y_: {}} for _ in range(2))
    sums, terms, sent = {"M": {}, "C": {}}, {}, {}
    for name, entries in START.items():
        sender, receiver, link = LINKS[name]
        t = 0
        for what in entries:
            if what[0] == "+":
                t += int(what)
                continue
            kind, unit, part = what[0], what[1:4], int(what[4])
            there = seen_by_receiver(unit, link)
            if kind == "s":
                h, part = (1, part - 1) if part > 1 else (part, 0)
                before = sent.setdefault((sender, link), [])
                sums[sender].setdefault(t, []).append((unit, h, part, link, len(before) % 2, before[-2] + 1 if len(before) > 1 else 0, 0))
                before.append(part)
                terms.setdefault((receiver, there, h), []).append((link, part))
                t += 1 if part == 2 else 2
                continue
            for p in (2 * part, 2 * part + 1) if part < 2 else (part - 4,):
                code = 1 + "dx".index(kind) + 16 * p
                send[link][ROLES.index(sender) * 100 + t] = code + 2 * pack(unit)
                recv[link][ROLES.index(receiver) * 100 + t + 2] = code + 2 * pack(there)
                t += 1
    for role in ROLES:
        for h in range(2):
            early = h == (LAST[role][1] >= LAST[role][0])
            sums[role].setdefault(LAST[role][h], []).insert(0, ("00" + role, h, 0, 3, 0, 0, early))
    sum_count, sum_what, tok_count, tok_what = {}, {}, {}, {}
    for r, role in enumerate(ROLES):
        met = set()
        for t, entries in sorted(sums[role].items()):
            sum_count[r * 100 + t] = len(entries)
            for k, (unit, h, part, link, parity, before, early) in enumerate(entries):
                mine = [(i, p) for i, p in terms.get((role, unit, h), []) if part in (0, p)]
                odd = [(i, p) for i, p in mine if p]
                code = pack(unit) + 8 * h + 16 * sum(1 << i for i, _ in mine) + 128 * link + 512 * parity + 1024 * before
                code += 4096 * early + 8192 * part + 2**17 * ((unit, h) in met)
                if odd:
                    code += 2**15 * (odd[0][1] + 0) + 2**18 * odd[0][0]
                met.add((unit, h))
                sum_what[(r * 100 + t) * 10 + k] = code
        for what in TOKENS[role]:
            t, kind, unit, h = int(what[:-5]), what[-5], what[-4:-1], int(what[-1])
            k = tok_count.get(r * 100 + t, 0)
            tok_count[r * 100 + t] = k + 1
            code = pack(unit) + 8 * h + 16 * "dx".index(kind)
            tok_what[(r * 100 + t) * 10 + k] = code + 32 * (what is TOKENS[role][-1])
    return send, recv, sum_count, sum_what, tok_count, tok_what, sent


def last_code(role):
    what = TOKENS[role][-1]
    return pack(what[-4:-1]) + 8 * int(what[-1])


def kernel(
    x, dy, gate, up, w_gate, w_up, w_down,
    dx, wd, acc, d_last, last_rows, full, parts,
    w, d, tok, gb, ub, dh, total, ext, out, outw,
    ag_recv, ag_send, w_recv, w_send, rs_recv, rs_send, p_send, l_send, l_sem, tok_sem, g_sem, u_sem, e_sem,
):
    block, depth = dy.shape
    width = gate.shape[1]
    rows, quarter, blocks = block // 2, block // 4, full.shape[1] // 2
    tile = 512
    nj, ni = depth // LANES, width // LANES
    own_in = {DY: dy, X: x}
    send_what, recv_what, sum_count, sum_what, tok_count, tok_what, sent = plan()

    tp = lax.axis_index("tp")
    core, chip = tp % 2, tp // 2
    y, z = chip // 4, chip % 4
    half = z // 2
    middle = ((z + 1) % 4) // 2
    is_m, is_c = middle == 1, middle == 0
    role = 1 - middle

    def chip_of(yy, hh, mm):
        return yy * 4 + mm + hh * (3 - 2 * mm)

    def chip_packed(code):
        ry, rh, mm = code % 2, (code // 2) % 2, (code // 4) % 2
        return chip_of(y + ry - 2 * y * ry, half + rh - 2 * half * rh, mm)

    partner = tp + 1 - 2 * core
    at_link = {
        P_: chip_of(y, half, 1 - middle) * 2 + core,
        D_: chip_of(y, 1 - half, middle) * 2 + core,
        Y_: chip_of(1 - y, half, middle) * 2 + core,
    }

    def span(h):
        return pl.ds(pl.multiple_of(h * rows, rows), rows)

    def quarter_at(p):
        return pl.ds(pl.multiple_of(p * quarter, quarter), quarter)

    def remote(src, dst, send, recv, to):
        return pltpu.make_async_remote_copy(
            src_ref=src, dst_ref=dst, send_sem=send, recv_sem=recv, device_id={"tp": to}, device_id_type=MESH
        )

    def by_rows(step, n_rows, fn, start=0):
        def body(i, _):
            fn(pl.ds(pl.multiple_of(i * step, step), step))
            return 0

        lax.fori_loop(start // step, n_rows // step, body, 0)

    cut = rows * 3 // 4 // 16 * 16
    part_rows = ((0, rows), (0, cut), (cut, rows - cut))

    def bounds(part):
        return jnp.where(part == 2, cut, 0), jnp.where(part == 1, cut, rows)

    def in_part(part, fn):
        for i in range(3):

            @pl.when(part == i)
            def _(i=i):
                fn(*part_rows[i])


    def on_link(link, code, src=None):
        code = code - 1
        array, c, p = code % 2, chip_packed(code // 2), code // 16
        piece = quarter_at(p)
        to = full.at[array, c * 2 + core, piece]
        return remote(to if src is None else src.at[piece], to, ag_send.at[link], ag_recv.at[array, c, p], at_link[link])

    def to_partner(array, c, p, src=None):
        piece = quarter_at(p)
        to = full.at[array, c * 2 + core, piece]
        return remote(to if src is None else src.at[piece], to, w_send.at[array], w_recv.at[array, c, p], partner)

    last = jnp.where(is_m, last_code("M"), last_code("C"))

    def last_to_partner():
        c, h = chip_packed(last), last // 8
        here = full.at[X, c * 2 + core, span(h)]
        return remote(here, last_rows, l_send, w_recv.at[X, c, 2 * h + 1], partner)

    def from_partner(array, c, h):
        for k in range(2):
            there = full.at[array, c * 2 + 1 - core, quarter_at(2 * h + k)]
            remote(there, there, p_send, w_recv.at[array, c, 2 * h + k], partner).wait_recv()

    def communicate(s):
        key = role * 100 + s
        come = {link: select(key, recv_what[link]) for link in (P_, D_, Y_)}
        for link, code in come.items():

            @pl.when(code > 0)
            def _(link=link, code=code):
                on_link(link, code).wait_recv()

        for link in (P_, D_, Y_):
            code = select(key, send_what[link])
            mine = chip_packed((code - 1) // 2) == chip

            @pl.when((code > 0) & jnp.logical_not(mine))
            def _(link=link, code=code):
                on_link(link, code).start()

            for array in (DY, X):

                @pl.when((code > 0) & mine & ((code - 1) % 2 == array))
                def _(link=link, code=code, array=array):
                    on_link(link, code, own_in[array]).start()

        for link, code in come.items():

            ends = ((code - 1) % 16 == X + 2 * (last % 8)) & ((code - 1) // 32 == last // 8)

            @pl.when((code > 0) & jnp.logical_not(ends))
            def _(code=code):
                to_partner((code - 1) % 2, chip_packed((code - 1) // 2), (code - 1) // 16).start()

            @pl.when(ends & ((code - 1) // 16 % 2 == 1))
            def _():
                last_to_partner().start()

        for array, when in ((DY, 0), (X, 2)):

            @pl.when(s == when)
            def _(array=array):
                for p in range(4):
                    to_partner(array, chip, p, own_in[array]).start()


    def dx_term(code, plane):
        index = chip_packed(code) * 2 + half_in(code)
        here = span(plane)

        def column(n, _):
            cols = pl.ds(pl.multiple_of(n * tile, tile), tile)
            total[:, cols] = lax.dot_general(
                d[index, here, :], w[cols, :], BY_COLUMNS, preferred_element_type=F32
            )
            return 0

        lax.fori_loop(0, depth // tile, column, 0)

    def reduce_one(code):
        c, h = chip_packed(code), half_in(code)
        mask, link, parity, before = (code // 16) % 8, (code // 128) % 4, (code // 512) % 2, (code // 1024) % 4
        early, part, again = (code // 4096) % 2 == 1, (code // 8192) % 4, (code // 2**17) % 2 == 1
        odd_part, odd = (code // 2**15) % 4, code // 2**18
        bits = {P_: mask % 2 == 1, D_: (mask // 2) % 2 == 1, Y_: mask // 4 == 1}
        part_of = {P_: jnp.where(odd == P_, odd_part, 0), D_: jnp.int32(0), Y_: jnp.where(odd == Y_, odd_part, 0), W_: jnp.int32(0)}

        def there(lo, n):
            return pl.ds(pl.multiple_of(h * rows + lo, 16), n)

        def term_in(kind, lo, n):
            return pltpu.make_async_copy(parts.at[kind, c, there(lo, n)], ext.at[kind, pl.ds(lo, n)], e_sem.at[kind])

        def with_term(kind, fn):
            if kind in (P_, Y_):
                in_part(part_of[kind], fn)
            else:
                fn(0, rows)

        def arrived(kind):
            def wait(lo, n):
                here = ext.at[kind, pl.ds(lo, n)]
                remote(here, parts.at[kind, c, there(lo, n)], p_send, rs_recv.at[kind, c, h], partner).wait_recv()

            with_term(kind, wait)

        def fetch(kind):
            with_term(kind, lambda lo, n: term_in(kind, lo, n).start())

        def send_term(to, lo, n):
            return remote(
                out.at[link, parity, pl.ds(lo, n)], parts.at[link, c, there(lo, n)], rs_send.at[link, parity],
                rs_recv.at[link, c, h], to,
            )

        @pl.when(jnp.logical_not(again))
        def _():
            arrived(W_)

        fetch(W_)
        for kind in (P_, D_, Y_):

            @pl.when(bits[kind] & (link != 3))
            def _(kind=kind):
                arrived(kind)
                fetch(kind)

        @pl.when(jnp.logical_not(early))
        def _():
            dx_term(code, core)

        for kind in (P_, D_, Y_):

            @pl.when(bits[kind] & (link == 3))
            def _(kind=kind):
                arrived(kind)
                fetch(kind)

        for kind in (P_, D_, Y_):

            @pl.when(bits[kind])
            def _(kind=kind):
                with_term(kind, lambda lo, n: term_in(kind, lo, n).wait())

                def add(r):
                    total[r, :] += ext[kind, r, :].astype(F32)

                lo, hi = bounds(part_of[kind])
                by_rows(16, hi, add, lo)

        term_in(W_, 0, rows).wait()

        @pl.when(link == 3)
        def _():
            def finish(r):
                to = pl.ds(pl.multiple_of(h * rows + r.start, 16), 16)
                dx[to, :] = (total[r, :] + ext[W_, r, :].astype(F32)).astype(BF16)

            by_rows(16, rows, finish)

        @pl.when(link != 3)
        def _():
            to = jnp.where(link == P_, at_link[P_], jnp.where(link == D_, at_link[D_], at_link[Y_]))
            in_part(before - 1, lambda lo, n: send_term(to, lo, n).wait_send())

            def round_(r):
                out[link, parity, r, :] = (total[r, :] + ext[W_, r, :].astype(F32)).astype(BF16)

            lo, hi = bounds(part)
            by_rows(16, hi, round_, lo)
            in_part(part, lambda lo, n: send_term(to, lo, n).start())

    def term_to_partner(code):
        c, h = chip_packed(code), half_in(code)
        return remote(outw, parts.at[W_, c, span(h)], p_send, rs_recv.at[W_, c, h], partner)

    def partner_one(code, first):
        dx_term(code, 1 - core)

        @pl.when(jnp.logical_not(first))
        def _():
            term_to_partner(code).wait_send()

        def round_(r):
            outw[r, :] = total[r, :].astype(BF16)

        by_rows(16, rows, round_)
        term_to_partner(code).start()


    def last_in(code, b):
        c, h = chip_packed(code), half_in(code)
        src = full.at[X, c * 2 + core, span(h)]
        return pltpu.make_async_copy(src, tok.at[b, span(core)], tok_sem.at[b, core])

    def tok_in(code, b, start):
        @pl.when(code < 32)
        def _():
            pair_in(code, b, start)

        @pl.when(code >= 32)
        def _():
            copy = last_in(code, b)
            copy.start() if start else copy.wait()

    def pair_in(code, b, start):
        c, h, array = chip_packed(code), half_in(code), (code // 16) % 2
        mine = c == chip
        for plane in range(2):
            blk = c * 2 + plane
            here = slice(plane * rows, (plane + 1) * rows)
            dst, src, sem = tok.at[b, here], full.at[array, blk, span(h)], tok_sem.at[b, plane]
            spread = pl.ds(pl.multiple_of(blk * block + h * rows, rows), rows)
            pair = (
                pltpu.make_async_copy(gate.at[spread], gb.at[b, here], g_sem.at[b, plane]),
                pltpu.make_async_copy(up.at[spread], ub.at[b, here], u_sem.at[b, plane]),
            )
            if not start:
                pltpu.make_async_copy(src, dst, sem).wait()

                @pl.when(array == DY)
                def _(pair=pair):
                    for copy in pair:
                        copy.wait()

                continue

            @pl.when(array == DY)
            def _(pair=pair):
                for copy in pair:
                    copy.start()

            local = mine & (core == plane)

            @pl.when(core != plane)
            def _():
                from_partner(array, c, h)

            @pl.when(jnp.logical_not(local))
            def _(src=src, dst=dst, sem=sem):
                pltpu.make_async_copy(src, dst, sem).start()

            for a in (DY, X):

                @pl.when(local & (array == a))
                def _(a=a, dst=dst, sem=sem):
                    pltpu.make_async_copy(own_in[a].at[span(h)], dst, sem).start()

    def work_dy(code, b):
        index = chip_packed(code) * 2 + half_in(code)
        dh[...] = lax.dot_general(tok[b], wd[...], BY_COLUMNS, preferred_element_type=F32)

        def pointwise(r):
            g, u, dhid = gb[b, r, :].astype(F32), ub[b, r, :].astype(F32), dh[r, :]
            g2 = g * g
            t = jnp.tanh(g * (ROOT + (ROOT * 0.044715) * g2))
            cdf = 0.5 + 0.5 * t
            act = g * cdf
            slope = cdf + (0.5 * g) * (1.0 - t * t) * (ROOT + (3 * ROOT * 0.044715) * g2)
            d[index, r, width:] = (dhid * act).astype(BF16)
            d[index, r, :width] = ((dhid * u) * slope).astype(BF16)
            gb[b, r, :] = (act * u).astype(BF16)

        by_rows(16, 2 * rows, pointwise)

        def column(n, _):
            cols = pl.ds(pl.multiple_of(n * tile, tile), tile)
            new = lax.dot_general(gb[b], tok[b, :, cols], BY_ROWS, preferred_element_type=F32)
            for i in range(ni):
                for j in range(tile // LANES):
                    k = i * nj + n * (tile // LANES) + j
                    acc[0, k] += new[lanes(i), lanes(j)]
            return 0

        lax.fori_loop(0, depth // tile, column, 0)

    def x_columns(index, b, here):
        def column(n, _):
            cols = pl.ds(pl.multiple_of(n * tile, tile), tile)
            xt = tok[b, here, cols]
            new = lax.dot_general(xt, d[index, here, :], BY_ROWS, preferred_element_type=F32)
            for i in range(tile // LANES):
                for j in range(2 * ni):
                    k = (n * (tile // LANES) + i) * ni + j % ni
                    acc[j // ni, k] += new[lanes(i), lanes(j)]
            return 0

        lax.fori_loop(0, depth // tile, column, 0)

    def work_x(code, b):
        x_columns(chip_packed(code) * 2 + half_in(code), b, slice(None))

    def last_x(code, b):
        c, h = chip_packed(code), half_in(code)
        x_columns(c * 2 + h, b, span(core))

        def keep(r):
            there = pl.ds(pl.multiple_of((1 - core) * rows + r.start, 16), 16)
            d_last[r, :] = d[c * 2 + h, there, :]

        by_rows(16, rows, keep)
        last_to_partner().wait_recv()

    def finish_down():
        for i in range(ni):
            for j in range(nj):
                wd[lanes(i), lanes(j)] = acc[0, i * nj + j].astype(BF16)
                acc[0, i * nj + j] = jnp.zeros((LANES, LANES), F32)

    def clear(i):
        def body(k, _):
            acc[i, k] = jnp.zeros((LANES, LANES), F32)
            return 0

        lax.fori_loop(0, ni * nj, body, 0)


    pairs = (w_down, wd), (w_gate, w.at[:, :width]), (w_up, w.at[:, width:])
    loads = [pltpu.make_async_copy(s, d, l_sem.at[i]) for i, (s, d) in enumerate(pairs)]
    for load in loads:
        load.start()

    barrier = pltpu.get_barrier_semaphore()
    for to in (at_link[P_], at_link[Y_], partner):
        pl.semaphore_signal(barrier, inc=1, device_id={"tp": to}, device_id_type=MESH)

    @pl.when(is_m)
    def _():
        pl.semaphore_signal(barrier, inc=1, device_id={"tp": at_link[D_]}, device_id_type=MESH)
        pl.semaphore_wait(barrier, 4)

    @pl.when(is_c)
    def _():
        pl.semaphore_wait(barrier, 3)

    x_from = jnp.where(is_m, X_FROM["M"], X_FROM["C"])

    first_sum = jnp.where(is_m, min(k for k in sum_count if k < 100), min(k for k in sum_count if k >= 100) - 100)
    last_sum = jnp.where(is_m, max(LAST["M"]), max(LAST["C"]))

    def step(s, _):
        @pl.when(s == last_sum)
        def _():
            dx_term(select((role * 100 + s) * 10, sum_what), core)

        communicate(s)

        @pl.when(s == x_from)
        def _():
            finish_down()

        key = role * 100 + s
        n_tok = select(key, tok_count)

        @pl.when(n_tok > 0)
        def _():
            tok_in(select(key * 10, tok_what), 0, True)

        @pl.when(s == 0)
        def _():
            clear(0)
            clear(1)
            for load in loads:
                load.wait()

        def sums(k, _):
            reduce_one(select(key * 10 + k, sum_what))
            return 0

        def tokens(k, _):
            code, b = select(key * 10 + k, tok_what), k % 2

            @pl.when(k + 1 < n_tok)
            def _():
                tok_in(select(key * 10 + k + 1, tok_what), 1 - b, True)

            tok_in(code, b, False)

            @pl.when((code // 16) % 2 == DY)
            def _():
                work_dy(code, b)

            @pl.when(code // 16 == X)
            def _():
                work_x(code, b)

            @pl.when(code >= 32)
            def _():
                last_x(code, b)

            return 0

        n_sum, tokens_first = select(key, sum_count), is_m & (s == last_sum)

        def phase(p, _):
            now = (p == 0) != tokens_first
            lax.fori_loop(0, jnp.where(now, n_sum, 0), sums, 0)
            lax.fori_loop(0, jnp.where(now, 0, n_tok), tokens, 0)
            return 0

        lax.fori_loop(0, 2, phase, 0)

        n_next = select(key + 1, sum_count)

        def partners(k, _):
            code = select((key + 1) * 10 + k, sum_what)

            @pl.when((code // 2**17) % 2 == 0)
            def _():
                partner_one(code, (k == 0) & (s + 1 == first_sum))

            return 0

        lax.fori_loop(0, n_next, partners, 0)

        return 0

    lax.fori_loop(0, STEPS, step, 0)

    def pieces_left(sem, n):
        sizes = [(b, n * quarter // b) for b in range(1, 2 * blocks) if n * quarter % b == 0 and n * quarter // b <= block]
        b, m = min(sizes, key=lambda size: size[1] % 8 > 0)
        some = full.at[0, pl.ds(0, b), pl.ds(0, m)]
        remote(some, some, sem, ag_recv.at[0, 0, 0], partner).wait_send()

    for r, here in enumerate((is_m, is_c)):

        @pl.when(here)
        def _(r=r):
            for link in (P_, D_, Y_):
                n = sum(k // 100 == r for k in send_what[link])
                if n:
                    pieces_left(ag_send.at[link], n)
                    parts_sent = sent[ROLES[r], link]
                    for i in (len(parts_sent) - 2, len(parts_sent) - 1):
                        lo, m = part_rows[parts_sent[i]]
                        here, there = out.at[link, i % 2, pl.ds(lo, m)], parts.at[link, 0, pl.ds(lo, m)]
                        remote(here, there, rs_send.at[link, i % 2], rs_recv.at[link, 0, 0], partner).wait_send()

    for array in (DY, X):
        pieces_left(w_send.at[array], 32 if array == DY else 30)
    last_to_partner().wait_send()
    term_to_partner(0).wait_send()


def finish(dx, wd, acc, d, rows_in, to_x, to_gate, to_up, to_down, done, d_sem, g_sem):
    depth, width = to_gate.shape
    tile, ni = 512, width // LANES
    copies = []
    for i, (result, place) in enumerate(((dx, to_x), (wd, to_down))):
        n = result.shape[0] // 4
        for k in range(4):
            here = pl.ds(k * n, n)
            copies.append(pltpu.make_async_copy(result.at[here], place.at[here], d_sem.at[i, k]))
    for copy in copies:
        copy.start()

    def store(a, n):
        here = pl.ds(pl.multiple_of(n * tile, tile), tile)
        return pltpu.make_async_copy(done.at[a, here], (to_gate, to_up)[a].at[here], g_sem.at[a, n])

    def column(n, _):
        xt = rows_in[:, pl.ds(pl.multiple_of(n * tile, tile), tile)]
        new = lax.dot_general(xt, d[...], BY_ROWS, preferred_element_type=F32)
        for i in range(tile // LANES):
            to = pl.ds(pl.multiple_of(n * tile + i * LANES, LANES), LANES)
            for j in range(2 * ni):
                k = (n * (tile // LANES) + i) * ni + j % ni
                one = acc[j // ni, k] + new[lanes(i), lanes(j)]
                done[j // ni, to, j % ni * LANES : (j % ni + 1) * LANES] = one.astype(BF16)
        for a in range(2):
            store(a, n).start()
        return 0

    lax.fori_loop(0, depth // tile, column, 0)
    for copy in copies:
        copy.wait()
    for n in range(depth // tile):
        for a in range(2):
            store(a, n).wait()


def solution(mesh):
    def step(x, dy, gate, up, w_gate, w_up, w_down):
        block, depth = dy.shape
        tokens, width = gate.shape
        rows, chips = block // 2, tokens // block // 2
        anywhere, inside = pl.BlockSpec(memory_space=pl.ANY), pl.BlockSpec(memory_space=pltpu.VMEM)
        dma, flops = pltpu.SemaphoreType.DMA, 12 * tokens * depth * width
        outs = pl.pallas_call(
            kernel,
            out_shape=[
                pltpu.VMEM((block, depth), BF16),
                pltpu.VMEM((width, depth), BF16),
                pltpu.VMEM((2, (depth // LANES) * (width // LANES), LANES, LANES), F32),
                pltpu.VMEM((rows, 2 * width), BF16),
                pltpu.VMEM((rows, depth), BF16),
                jax.ShapeDtypeStruct((2, 2 * chips, block, depth), BF16),
                jax.ShapeDtypeStruct((4, chips, block, depth), BF16),
            ],
            in_specs=[anywhere] * 7,
            out_specs=[inside] * 5 + [anywhere] * 2,
            scratch_shapes=[
                pltpu.VMEM((depth, 2 * width), BF16),
                pltpu.VMEM((2 * chips, 2 * rows, 2 * width), BF16),
                pltpu.VMEM((2, 2 * rows, depth), BF16),
                pltpu.VMEM((2, 2 * rows, width), BF16),
                pltpu.VMEM((2, 2 * rows, width), BF16),
                pltpu.VMEM((2 * rows, width), F32),
                pltpu.VMEM((rows, depth), F32),
                pltpu.VMEM((4, rows, depth), BF16),
                pltpu.VMEM((3, 2, rows, depth), BF16),
                pltpu.VMEM((rows, depth), BF16),
                dma((2, chips, 4)),
                dma((3,)),
                dma((2, chips, 4)),
                dma((2,)),
                dma((4, chips, 2)),
                dma((3, 2)),
                dma(()),
                dma(()),
                dma((3,)),
                dma((2, 2)),
                dma((2, 2)),
                dma((2, 2)),
                dma((4,)),
            ],
            compiler_params=pltpu.CompilerParams(collective_id=0, has_side_effects=True, vmem_limit_bytes=46900000),
            cost_estimate=pl.CostEstimate(flops=flops, bytes_accessed=12 * tokens * depth, transcendentals=tokens * width),
            name="mlp_backward",
        )(x, dy, gate, up, w_gate, w_up, w_down)
        return pl.pallas_call(
            finish,
            out_shape=[jax.ShapeDtypeStruct(a.shape, BF16) for a in (dy, w_gate, w_up, w_down)],
            in_specs=[inside] * 5,
            out_specs=[anywhere] * 4,
            scratch_shapes=[
                pltpu.VMEM((2, depth, width), BF16),
                dma((2, 4)),
                dma((2, depth // 512)),
            ],
            compiler_params=pltpu.CompilerParams(vmem_limit_bytes=2**24),
            name="finish",
        )(*outs[:5])

    rows_, cols_ = P(("dp", "tp"), None), P("dp", "tp")
    return jax.shard_map(
        step,
        mesh=mesh,
        in_specs=(rows_, rows_, cols_, cols_, P(None, "tp"), P(None, "tp"), P("tp", None)),
        out_specs=(rows_, cols_, cols_, rows_),
        check_vma=False,
    )
```
